8 devices in a mesh: dp: 1 (over z), tp: 2 (over y), sp: 4 (over x, core).
Axes of the slice: x: 2, y: 2, z: 1, core: 2. Of those that a mesh axis runs over, the one named last changes fastest.
Arguments:
- encoded: bfloat16 [64, 384, 1280], P('dp', 'sp')
- enc_gain: float32 [1280], replicated
- enc_bias: float32 [1280], replicated
- probe: float32 [1280], replicated
- w_query: bfloat16 [1280, 16, 80], P(None, 'tp')
- b_query: float32 [16, 80], P('tp')
- w_key: bfloat16 [1280, 16, 80], P(None, 'tp')
- w_value: bfloat16 [1280, 16, 80], P(None, 'tp')
- b_value: float32 [16, 80], P('tp')
- w_out: bfloat16 [16, 80, 1280], P('tp')
- b_out: float32 [1280], replicated
- head_gain: float32 [1280], replicated
- head_bias: float32 [1280], replicated
- w_up: bfloat16 [1280, 5120], P(None, 'tp')
- b_up: float32 [5120], P('tp')
- w_down: bfloat16 [5120, 1280], P('tp')
- b_down: float32 [1280], replicated
- out_grad: bfloat16 [64, 1280], P('dp')
Outputs:
- output 1: bfloat16 [64, 1280], P('dp')
- output 2: bfloat16 [64, 384, 1280], P('dp', 'sp')
- output 3: float32 [1280], P('dp')
- output 4: float32 [1280, 16, 80], P('dp', 'tp')
- output 5: float32 [1280, 16, 80], P('dp', 'tp')
- output 6: float32 [1280, 16, 80], P('dp', 'tp')
- output 7: float32 [16, 80, 1280], P(('dp', 'tp'))
- output 8: float32 [1280, 5120], P('dp', 'tp')
- output 9: float32 [5120, 1280], P(('dp', 'tp'))
All inputs are finite; a program needn't handle non-finite values.
Results may differ from the reference program's by a relative error of at most 0.0187281.
Values sent between devices are 32-bit elements.
A program may use at most 1 GiB of HBM per device.

```python
import jax
import jax.numpy as jnp
from jax import lax

IMAGES = 64
TOKENS = 384
MODEL_WIDTH = 1280
NUM_HEADS = 16
MLP_WIDTH = 5120
HEAD_DIM = MODEL_WIDTH // NUM_HEADS
NORM_EPS = 1e-6


def normal_weight(key_in, shape_in, fan_in):
    return (jax.random.normal(key_in, shape_in, jnp.float32) * fan_in ** -0.5).astype(jnp.bfloat16)


def normal_vector(key_in, shape_in, center, spread):
    return center + spread * jax.random.normal(key_in, shape_in, jnp.float32)


def setup_inputs(seed: int = 0, part: int = 0) -> dict:
    base_key = jax.random.key(seed)
    shared_keys = jax.random.split(base_key, 16)
    part_keys = jax.random.split(jax.random.fold_in(base_key, part), 4)
    head_shape = (MODEL_WIDTH, NUM_HEADS, HEAD_DIM)
    positions = jnp.linspace(-1.5, 1.5, TOKENS, dtype=jnp.float32)
    token_noise = jax.random.normal(part_keys[0], (IMAGES, TOKENS, MODEL_WIDTH), jnp.float32)
    common = jax.random.normal(part_keys[1], (IMAGES, 1, MODEL_WIDTH), jnp.float32)
    trend_dir = jax.random.normal(part_keys[2], (IMAGES, 1, MODEL_WIDTH), jnp.float32)
    encoded = (token_noise + common + positions[None, :, None] * trend_dir).astype(jnp.bfloat16)
    out_grad = jax.random.normal(part_keys[3], (IMAGES, MODEL_WIDTH), jnp.float32).astype(jnp.bfloat16)
    return {
        'encoded': encoded,
        'enc_gain': normal_vector(shared_keys[0], (MODEL_WIDTH,), 1.0, 0.3),
        'enc_bias': normal_vector(shared_keys[1], (MODEL_WIDTH,), 0.0, 0.5),
        'probe': normal_vector(shared_keys[2], (MODEL_WIDTH,), 0.0, 1.0),
        'w_query': normal_weight(shared_keys[3], head_shape, MODEL_WIDTH),
        'b_query': normal_vector(shared_keys[4], (NUM_HEADS, HEAD_DIM), 0.0, 0.5),
        'w_key': normal_weight(shared_keys[5], head_shape, MODEL_WIDTH),
        'w_value': normal_weight(shared_keys[6], head_shape, MODEL_WIDTH),
        'b_value': normal_vector(shared_keys[7], (NUM_HEADS, HEAD_DIM), 0.0, 0.5),
        'w_out': normal_weight(shared_keys[8], (NUM_HEADS, HEAD_DIM, MODEL_WIDTH), MODEL_WIDTH),
        'b_out': normal_vector(shared_keys[9], (MODEL_WIDTH,), 0.0, 0.5),
        'head_gain': normal_vector(shared_keys[10], (MODEL_WIDTH,), 1.0, 0.3),
        'head_bias': normal_vector(shared_keys[11], (MODEL_WIDTH,), 0.0, 0.5),
        'w_up': normal_weight(shared_keys[12], (MODEL_WIDTH, MLP_WIDTH), MODEL_WIDTH),
        'b_up': normal_vector(shared_keys[13], (MLP_WIDTH,), 0.0, 0.5),
        'w_down': normal_weight(shared_keys[14], (MLP_WIDTH, MODEL_WIDTH), MLP_WIDTH),
        'b_down': normal_vector(shared_keys[15], (MODEL_WIDTH,), 0.0, 0.5),
        'out_grad': out_grad,
    }


def layer_norm(rows_in, norm_gain, norm_bias):
    row_mean = jnp.mean(rows_in, axis=-1, keepdims=True)
    centred = rows_in - row_mean
    inv_std = lax.rsqrt(jnp.mean(centred * centred, axis=-1, keepdims=True) + NORM_EPS)
    return centred * inv_std * norm_gain + norm_bias


def keep_exact(array_in):
    return array_in


def store_bf16(array_in):
    return array_in.astype(jnp.bfloat16).astype(jnp.float32)


def head_forward(store, encoded, enc_gain, enc_bias, probe, w_query, b_query, w_key, w_value, b_value, w_out, b_out, head_gain, head_bias, w_up, b_up, w_down, b_down):
    normed = store(layer_norm(encoded, enc_gain, enc_bias))
    query_heads = store(jnp.einsum('w,whd->hd', store(probe), w_query) + b_query)
    key_heads = store(jnp.einsum('bnw,whd->bnhd', normed, w_key))
    value_heads = store(jnp.einsum('bnw,whd->bnhd', normed, w_value) + b_value)
    scores = jnp.einsum('bnhd,hd->bhn', key_heads, query_heads) * HEAD_DIM ** -0.5
    weights = jax.nn.softmax(scores, axis=-1)
    pooled_heads = store(jnp.einsum('bhn,bnhd->bhd', weights, value_heads))
    attn_out = jnp.einsum('bhd,hdw->bw', pooled_heads, w_out) + b_out
    normed_out = store(layer_norm(attn_out, head_gain, head_bias))
    hidden = store(jax.nn.gelu(jnp.dot(normed_out, w_up) + b_up, approximate=True))
    return attn_out + jnp.dot(hidden, w_down) + b_down


def reference(encoded, enc_gain, enc_bias, probe, w_query, b_query, w_key, w_value, b_value, w_out, b_out, head_gain, head_bias, w_up, b_up, w_down, b_down, out_grad):
    exact_args = [array_in.astype(jnp.float32) for array_in in (encoded, enc_gain, enc_bias, probe, w_query, b_query, w_key, w_value, b_value, w_out, b_out, head_gain, head_bias, w_up, b_up, w_down, b_down)]
    pooled = head_forward(store_bf16, *exact_args).astype(jnp.bfloat16)

    def grad_target(enc_in, probe_in, query_in, key_in, value_in, out_in, up_in, down_in):
        return head_forward(keep_exact, enc_in, exact_args[1], exact_args[2], probe_in, query_in, exact_args[5], key_in, value_in, exact_args[8], out_in, exact_args[10], exact_args[11], exact_args[12], up_in, exact_args[14], down_in, exact_args[16])

    pull_back = jax.vjp(grad_target, exact_args[0], exact_args[3], exact_args[4], exact_args[6], exact_args[7], exact_args[9], exact_args[13], exact_args[15])[1]
    grad_list = pull_back(out_grad.astype(jnp.float32))
    return (pooled, grad_list[0].astype(jnp.bfloat16), grad_list[1], grad_list[2], grad_list[3], grad_list[4], grad_list[5], grad_list[6], grad_list[7])
```

```python
import jax
import jax.numpy as jnp
from jax import lax
from jax.sharding import PartitionSpec as P

NORM_EPS = 1e-6
F32 = jnp.float32
BF16 = jnp.bfloat16
IN_SPECS = (P('dp', 'sp', None), P(), P(), P(), P(None, 'tp', None), P('tp', None), P(None, 'tp', None), P(None, 'tp', None), P('tp', None), P('tp', None, None), P(), P(), P(), P(None, 'tp'), P('tp'), P('tp', None), P(), P('dp', None))
OUT_SPECS = (P('dp', None), P('dp', 'sp', None), P('dp'), P('dp', 'tp', None), P('dp', 'tp', None), P('dp', 'tp', None), P(('dp', 'tp'), None, None), P('dp', 'tp'), P(('dp', 'tp'), None))


def dot(spec, a, b):
    return jnp.einsum(spec, a, b, preferred_element_type=F32)


def split(a):
    hi = lax.reduce_precision(a, 8, 7)
    return hi.astype(BF16), (a - hi).astype(BF16)


def stats(rows):
    mean = jnp.mean(rows, axis=-1, keepdims=True)
    cen = rows - mean
    return cen, lax.rsqrt(jnp.mean(cen * cen, axis=-1, keepdims=True) + NORM_EPS)


def local_head(encoded, enc_gain, enc_bias, probe, w_query, b_query, w_key, w_value, b_value, w_out, b_out, head_gain, head_bias, w_up, b_up, w_down, b_down, out_grad):
    hd = b_query.shape[1]
    nh = b_query.shape[0]
    width = probe.shape[0]
    scale = hd ** -0.5
    tp_i = lax.axis_index('tp')
    q = (dot('w,whd->hd', probe.astype(BF16), w_query) + b_query).astype(BF16)
    u_own = dot('hd,whd->hw', q, w_key)
    u = lax.all_gather(u_own, 'tp', axis=0, tiled=True)
    gu = u * enc_gain * scale
    bu = jnp.sum(u * enc_bias, axis=-1) * scale
    gu_hi, gu_lo = split(gu)
    cen, rstd = stats(encoded.astype(F32))
    xh = (cen * rstd).astype(BF16)
    s2 = dot('bnw,kw->bkn', xh, jnp.concatenate([gu_hi, gu_lo], 0))
    nk = 2 * nh
    s_x = s2[:, :nk] + s2[:, nk:]
    s = s_x + bu[None, :, None]
    m = jnp.max(s, axis=-1)
    e = jnp.exp(s - m[..., None])
    l = jnp.sum(e, axis=-1)
    e_own = lax.dynamic_slice_in_dim(e, tp_i * nh, nh, 1)
    l_own = lax.dynamic_slice_in_dim(l, tp_i * nh, nh, 1)
    r_raw = dot('bhn,bnw->bhw', e_own.astype(BF16), xh)
    r = r_raw * enc_gain + l_own[..., None] * enc_bias
    o_loc = dot('bhw,whd->bhd', r.astype(BF16), w_value) + l_own[..., None] * b_value
    nb = o_loc.shape[0]
    pack = jnp.concatenate([o_loc.reshape(nb, nh * hd), m, l], axis=1)
    allp = lax.all_gather(pack, 'sp', axis=0)
    ms = allp[:, :, nh * hd:nh * hd + nk]
    ls = allp[:, :, nh * hd + nk:]
    os_ = allp[:, :, :nh * hd].reshape(-1, nb, nh, hd)
    mg = jnp.max(ms, axis=0)
    fs = jnp.exp(ms - mg)
    lg = jnp.sum(fs * ls, axis=0)
    fs_own = lax.dynamic_slice_in_dim(fs, tp_i * nh, nh, 2)
    lg_own = lax.dynamic_slice_in_dim(lg, tp_i * nh, nh, 1)
    o = jnp.sum(fs_own[..., None] * os_, axis=0) / lg_own[..., None]
    w_loc = jnp.exp(m - mg) / lg
    p = e * w_loc[..., None]
    w_own = lax.dynamic_slice_in_dim(w_loc, tp_i * nh, nh, 1)
    r_full = lax.psum(r_raw * w_own[..., None], 'sp') * enc_gain + enc_bias
    o_bf = o.astype(BF16)
    r_bf = r_full.astype(BF16)
    a = lax.psum(dot('bhd,hdw->bw', o_bf, w_out), 'tp') + b_out
    acen, arstd = stats(a)
    ahat = acen * arstd
    y = (ahat * head_gain + head_bias).astype(BF16)
    pre = jnp.dot(y, w_up, preferred_element_type=F32) + b_up
    g32, gelu_pb = jax.vjp(lambda t: jax.nn.gelu(t, approximate=True), pre)
    g = g32.astype(BF16)
    dg = dot('bw,fw->bf', out_grad, w_down)
    dpre = gelu_pb(dg)[0].astype(BF16)
    both = lax.psum((dot('bf,wf->bw', dpre, w_up), jnp.dot(g, w_down, preferred_element_type=F32)), 'tp')
    dy, mlp = both
    pooled = (a + mlp + b_down).astype(BF16)
    grad_w_down = dot('bf,bw->fw', g, out_grad)
    grad_w_up = dot('bw,bf->wf', y, dpre)
    dah = dy * head_gain
    da = arstd * (dah - jnp.mean(dah, -1, keepdims=True) - ahat * jnp.mean(dah * ahat, -1, keepdims=True))
    da = (out_grad.astype(F32) + da).astype(BF16)
    grad_w_out = dot('bhd,bw->hdw', o_bf, da)
    do = dot('bw,hdw->bhd', da, w_out).astype(BF16)
    do32 = do.astype(F32)
    d_own = jnp.sum(do32 * o, axis=-1)
    c_own = jnp.sum(do32 * b_value, axis=-1)
    t_own = dot('bhd,whd->bhw', do, w_value)
    t, d_all, c_all = lax.all_gather((t_own, d_own, c_own), 'tp', axis=1, tiled=True)
    gt32 = t * enc_gain
    gt = gt32.astype(BF16)
    bt = jnp.sum(t * enc_bias, axis=-1) + c_all
    dp_x = dot('bnw,bkw->bkn', xh, gt)
    dsu = p * (dp_x + bt[..., None] - d_all[..., None])
    dsu_own = lax.dynamic_slice_in_dim(dsu, tp_i * nh, nh, 1)
    z = dot('bhn,bnw->hw', dsu_own.astype(BF16), xh)
    z, dl = lax.psum((z, jnp.sum(dsu_own, axis=2)), 'sp')
    z = (z * enc_gain - dot('bh,bhw->hw', dl.astype(BF16), r_bf) + jnp.sum(dl, 0)[:, None] * enc_bias) * scale
    q32 = q.astype(F32)
    grad_w_key = z.T[:, :, None] * q32[None]
    dq = dot('hw,whd->hd', z.astype(BF16), w_key)
    grad_w_query = probe[:, None, None] * dq[None]
    grad_probe = lax.psum(dot('whd,hd->w', w_query, dq.astype(BF16)), 'tp')
    grad_w_value = dot('bhw,bhd->whd', r_bf, do)
    c1 = (jnp.sum(dsu * jnp.sum(gu, -1)[None, :, None], 1) + jnp.sum(p * jnp.sum(gt32, -1)[..., None], 1)) / width
    c2 = (jnp.sum(dsu * s_x, 1) + jnp.sum(p * dp_x, 1)) / width
    coef = jnp.concatenate([dsu, p], axis=1).astype(BF16)
    basis = jnp.concatenate([jnp.broadcast_to(gu_hi[None], (nb,) + gu_hi.shape), gt], axis=1)
    dxh = dot('bkn,bkw->bnw', coef, basis)
    grad_encoded = (rstd * (dxh - c1[..., None] - xh.astype(F32) * c2[..., None])).astype(BF16)
    return (pooled, grad_encoded, grad_probe, grad_w_query, grad_w_key, grad_w_value, grad_w_out, grad_w_up, grad_w_down)


def solution(mesh):
    return jax.shard_map(local_head, mesh=mesh, in_specs=IN_SPECS, out_specs=OUT_SPECS, check_vma=False)
```

```python
import functools
import jax
import jax.numpy as jnp
from jax import lax
from jax.experimental import pallas as pl
from jax.experimental.pallas import tpu as pltpu
from jax.sharding import PartitionSpec as P

NORM_EPS = 1e-6
F32 = jnp.float32
BF16 = jnp.bfloat16
IN_SPECS = (P('dp', 'sp', None), P(), P(), P(), P(None, 'tp', None), P('tp', None), P(None, 'tp', None), P(None, 'tp', None), P('tp', None), P('tp', None, None), P(), P(), P(), P(None, 'tp'), P('tp'), P('tp', None), P(), P('dp', None))
OUT_SPECS = (P('dp', None), P('dp', 'sp', None), P('dp'), P('dp', 'tp', None), P('dp', 'tp', None), P('dp', 'tp', None), P(('dp', 'tp'), None, None), P('dp', 'tp'), P(('dp', 'tp'), None))
NN = (((1,), (0,)), ((), ()))
NT = (((1,), (1,)), ((), ()))
TN = (((0,), (0,)), ((), ()))
FWD_IMAGES = 4
BWD_IMAGES = 4


def mm(a, b, dims=NN):
    return lax.dot_general(a, b, dims, preferred_element_type=F32)


def dot(spec, a, b):
    return jnp.einsum(spec, a, b, preferred_element_type=F32)


def split(a):
    hi = lax.reduce_precision(a, 8, 7)
    return hi.astype(BF16), (a - hi).astype(BF16)


def stats(rows):
    mean = jnp.mean(rows, axis=-1, keepdims=True)
    cen = rows - mean
    return cen, lax.rsqrt(jnp.mean(cen * cen, axis=-1, keepdims=True) + NORM_EPS)


def fwd_body(nk, x_ref, gu_ref, bu_ref, xh_ref, sx_ref, r_ref, ml_ref):
    step = pl.program_id(0)
    images, tokens, width = x_ref.shape
    nh = nk // 2

    @pl.when(step == 0)
    def _():
        ml_ref[...] = jnp.zeros_like(ml_ref)

    lane = lax.broadcasted_iota(jnp.int32, (nk, ml_ref.shape[1]), 1)
    for i in range(images):
        rs = []
        for j in range(0, tokens, 16):
            xs = x_ref[i, j:j + 16, :].astype(F32)
            cen, rstd = stats(xs)
            xh_ref[i, j:j + 16, :] = (cen * rstd).astype(BF16)
            rs.append(rstd)
        rcol = jnp.broadcast_to(jnp.concatenate(rs, 0), (tokens, 128))
        xh = xh_ref[i]
        s2 = mm(gu_ref[...], xh, NT)
        sx = s2[:nk] + s2[nk:]
        s = sx + bu_ref[:, :1]
        m = jnp.max(s, axis=1, keepdims=True)
        e = jnp.exp(s - m)
        l = jnp.sum(e, axis=1, keepdims=True)
        r_ref[i * nh:(i + 1) * nh, :] = mm(e[:nh].astype(BF16), xh)
        sx_ref[i, :nk, :] = sx
        sx_ref[i, nk:, :] = jnp.transpose(rcol)[:8]
        sel = lane == step * images + i
        ml_ref[:nk] = jnp.where(sel, m, ml_ref[:nk])
        ml_ref[nk:] = jnp.where(sel, l, ml_ref[nk:])


def run_fwd(x, gu2, bu):
    nb, tokens, width = x.shape
    nk = bu.shape[0]
    bi = FWD_IMAGES
    return pl.pallas_call(
        functools.partial(fwd_body, nk),
        grid=(nb // bi,),
        in_specs=[
            pl.BlockSpec((bi, tokens, width), lambda i: (i, 0, 0)),
            pl.BlockSpec(gu2.shape, lambda i: (0, 0)),
            pl.BlockSpec(bu.shape, lambda i: (0, 0)),
        ],
        out_specs=[
            pl.BlockSpec((bi, tokens, width), lambda i: (i, 0, 0)),
            pl.BlockSpec((bi, nk + 8, tokens), lambda i: (i, 0, 0)),
            pl.BlockSpec((bi * nk // 2, width), lambda i: (i, 0)),
            pl.BlockSpec((2 * nk, 128), lambda i: (0, 0)),
        ],
        out_shape=[
            jax.ShapeDtypeStruct((nb, tokens, width), BF16),
            jax.ShapeDtypeStruct((nb, nk + 8, tokens), F32),
            jax.ShapeDtypeStruct((nb * nk // 2, width), F32),
            jax.ShapeDtypeStruct((2 * nk, 128), F32),
        ],
        cost_estimate=pl.CostEstimate(flops=8_000_000_000, bytes_accessed=40_000_000, transcendentals=0),
        name='fwd_tokens',
    )(x, gu2, bu)


def bwd_body(nk, xh_ref, sx_ref, gt_ref, gu_ref, aux_ref, dx_ref, z_ref, dl_ref, bas_ref, zacc_ref):
    step = pl.program_id(0)
    images, tokens, width = xh_ref.shape
    nh = nk // 2

    @pl.when(step == 0)
    def _():
        dl_ref[...] = jnp.zeros_like(dl_ref)
        zacc_ref[...] = jnp.zeros_like(zacc_ref)
        row = lax.broadcasted_iota(jnp.int32, (16, width), 0)
        for i in range(images):
            bas_ref[i, :nk, :] = gu_ref[...]
            bas_ref[i, 2 * nk:, :] = jnp.where(row < 2, 1.0, 0.0).astype(BF16)

    lane = lax.broadcasted_iota(jnp.int32, (nh, dl_ref.shape[1]), 1)
    row = lax.broadcasted_iota(jnp.int32, (16, tokens), 0)
    inv_w = 1.0 / width
    z = zacc_ref[...]
    for i in range(images):
        xh = xh_ref[i]
        gt = gt_ref[i]
        bas_ref[i, nk:2 * nk, :] = gt
        aux = aux_ref[i]
        sx = sx_ref[i, :nk, :]
        rstd = sx_ref[i, nk:nk + 1, :]
        p = jnp.exp(sx - aux[:, 0:1]) * aux[:, 1:2]
        dpx = mm(gt, xh, NT)
        ds = p * (dpx + aux[:, 2:3])
        z = z + mm(ds[:nh].astype(BF16), xh)
        dl_ref[...] = jnp.where(lane == step * images + i, jnp.sum(ds[:nh], axis=1, keepdims=True), dl_ref[...])
        c1 = jnp.sum(ds * aux[:, 4:5] + p * aux[:, 3:4], axis=0, keepdims=True) * (-inv_w * rstd)
        c2 = jnp.sum(ds * sx + p * dpx, axis=0, keepdims=True) * (inv_w * rstd)
        c1h = c1.astype(BF16).astype(F32)
        tail = jnp.where(row == 0, c1h, jnp.where(row == 1, c1 - c1h, 0.0))
        coef = jnp.concatenate([ds * rstd, p * rstd, tail], axis=0).astype(BF16)
        c2col = jnp.transpose(jnp.broadcast_to(c2, (8, tokens)))[:, :1]
        dxh = mm(coef, bas_ref[i], TN)
        dx_ref[i] = (dxh - c2col * xh.astype(F32)).astype(BF16)
    zacc_ref[...] = z
    z_ref[...] = z


def run_bwd(xh, sx, gt, gu_hi, aux):
    nb, tokens, width = xh.shape
    nk = gu_hi.shape[0]
    bi = BWD_IMAGES
    return pl.pallas_call(
        functools.partial(bwd_body, nk),
        grid=(nb // bi,),
        in_specs=[
            pl.BlockSpec((bi, tokens, width), lambda i: (i, 0, 0)),
            pl.BlockSpec((bi, nk + 8, tokens), lambda i: (i, 0, 0)),
            pl.BlockSpec((bi, nk, width), lambda i: (i, 0, 0)),
            pl.BlockSpec((nk, width), lambda i: (0, 0)),
            pl.BlockSpec((bi, nk, aux.shape[2]), lambda i: (i, 0, 0)),
        ],
        out_specs=[
            pl.BlockSpec((bi, tokens, width), lambda i: (i, 0, 0)),
            pl.BlockSpec((nk // 2, width), lambda i: (0, 0)),
            pl.BlockSpec((nk // 2, 128), lambda i: (0, 0)),
        ],
        out_shape=[
            jax.ShapeDtypeStruct((nb, tokens, width), BF16),
            jax.ShapeDtypeStruct((nk // 2, width), F32),
            jax.ShapeDtypeStruct((nk // 2, 128), F32),
        ],
        scratch_shapes=[pltpu.VMEM((bi, 2 * nk + 16, width), BF16), pltpu.VMEM((nk // 2, width), F32)],
        cost_estimate=pl.CostEstimate(flops=12_000_000_000, bytes_accessed=40_000_000, transcendentals=0),
        name='bwd_tokens',
    )(xh, sx, gt, gu_hi, aux)


def t_body(nh, do_ref, dother_ref, wv_ref, wvo_ref, gain_ref, gt_ref, sg_ref):
    hd = wv_ref.shape[0] // nh
    gain = gain_ref[...]
    for k in range(2):
        for h in range(nh):
            w = (wv_ref, wvo_ref)[k][h * hd:(h + 1) * hd, :].astype(BF16)
            d = (do_ref, dother_ref)[k][:, h, :].astype(BF16)
            gt = mm(d, w) * gain
            gt_ref[:, k * nh + h, :] = gt
            sg_ref[k * nh + h] = jnp.sum(gt, axis=1, keepdims=True)


def run_t(do, do_other, wv_t, wv_other, gain):
    nb, nh, _ = do.shape
    width = wv_t.shape[1]
    return pl.pallas_call(
        functools.partial(t_body, nh),
        out_shape=[
            jax.ShapeDtypeStruct((nb, 2 * nh, width), F32),
            jax.ShapeDtypeStruct((2 * nh, nb, 1), F32),
        ],
        cost_estimate=pl.CostEstimate(flops=200_000_000, bytes_accessed=8_000_000, transcendentals=0),
        name='value_back',
    )(do, do_other, wv_t, wv_other, gain)


def swap(a):
    return lax.ppermute(a, 'tp', [(0, 1), (1, 0)])


def local_head(encoded, enc_gain, enc_bias, probe, w_query, b_query, w_key, w_value, b_value, w_out, b_out, head_gain, head_bias, w_up, b_up, w_down, b_down, out_grad):
    nh, hd = b_query.shape
    width = probe.shape[0]
    nb = encoded.shape[0]
    scale = hd ** -0.5
    nk = 2 * nh
    wv_t = jnp.transpose(w_value, (1, 2, 0)).reshape(nh * hd, width)
    wv_other = swap(wv_t.astype(F32))
    q = (dot('w,whd->hd', probe.astype(BF16), w_query) + b_query).astype(BF16)
    u_own = dot('hd,whd->hw', q, w_key)
    u = jnp.concatenate([u_own, swap(u_own)], 0)
    gu = u * enc_gain * scale
    bu = jnp.sum(u * enc_bias, axis=-1) * scale
    gu_hi, gu_lo = split(gu)
    xh, sx, r_raw, ml = run_fwd(encoded, jnp.concatenate([gu_hi, gu_lo], 0), jnp.broadcast_to(bu[:, None], (nk, 128)))
    r_raw = r_raw.reshape(nb, nh, width)
    m, l = ml[:nk, :nb].T, ml[nk:, :nb].T
    l_own = l[:, :nh]
    r = r_raw * enc_gain + l_own[..., None] * enc_bias
    o_loc = dot('bhw,whd->bhd', r.astype(BF16), w_value) + l_own[..., None] * b_value
    pack = jnp.concatenate([o_loc.reshape(nb, nh * hd), m, l], axis=1)
    allp = lax.all_gather(pack, 'sp', axis=0)
    ms = allp[:, :, nh * hd:nh * hd + nk]
    ls = allp[:, :, nh * hd + nk:]
    os_ = allp[:, :, :nh * hd].reshape(-1, nb, nh, hd)
    mg = jnp.max(ms, axis=0)
    fs = jnp.exp(ms - mg)
    lg = jnp.sum(fs * ls, axis=0)
    o = jnp.sum(fs[..., :nh, None] * os_, axis=0) / lg[:, :nh, None]
    w_own = jnp.exp(m - mg)[:, :nh] / lg[:, :nh]
    r_full = lax.psum(r_raw * w_own[..., None], 'sp') * enc_gain + enc_bias
    o_bf = o.astype(BF16)
    r_bf = r_full.astype(BF16)
    a = lax.psum(dot('bhd,hdw->bw', o_bf, w_out), 'tp') + b_out
    acen, arstd = stats(a)
    ahat = acen * arstd
    y = (ahat * head_gain + head_bias).astype(BF16)
    pre = jnp.dot(y, w_up, preferred_element_type=F32) + b_up
    g32, gelu_pb = jax.vjp(lambda t: jax.nn.gelu(t, approximate=True), pre)
    g = g32.astype(BF16)
    dg = dot('bw,fw->bf', out_grad, w_down)
    dpre = gelu_pb(dg)[0].astype(BF16)
    both = lax.psum((dot('bf,wf->bw', dpre, w_up), jnp.dot(g, w_down, preferred_element_type=F32)), 'tp')
    dy, mlp = both
    pooled = (a + mlp + b_down).astype(BF16)
    grad_w_down = dot('bf,bw->fw', g, out_grad)
    grad_w_up = dot('bw,bf->wf', y, dpre)
    dah = dy * head_gain
    da = arstd * (dah - jnp.mean(dah, -1, keepdims=True) - ahat * jnp.mean(dah * ahat, -1, keepdims=True))
    da = (out_grad.astype(F32) + da).astype(BF16)
    grad_w_out = dot('bhd,bw->hdw', o_bf, da)
    do32 = lax.reduce_precision(dot('bw,hdw->bhd', da, w_out), 8, 7)
    do = do32.astype(BF16)
    cb = dot('w,whd->hd', split(enc_bias)[0], w_value) + dot('w,whd->hd', split(enc_bias)[1], w_value) + b_value
    kap_own = jnp.sum(do32 * (cb - o), axis=-1)
    do_other = swap(do32)
    kap = jnp.concatenate([kap_own, swap(kap_own)], axis=1)
    gt32, sg = run_t(do32, do_other, wv_t, wv_other, enc_gain[None])
    gt = gt32.astype(BF16)
    aux = jnp.stack([mg - bu, 1.0 / lg, kap, sg[..., 0].T, jnp.broadcast_to(jnp.sum(gu, -1), (nb, nk))] + [jnp.zeros((nb, nk), F32)] * 3, axis=-1)
    grad_encoded, z, dl = run_bwd(xh, sx, gt, gu_hi, aux)
    z, dl = lax.psum((z, dl[:, :nb]), 'sp')
    z = (z * enc_gain - dot('hb,bhw->hw', dl.astype(BF16), r_bf) + jnp.sum(dl, 1)[:, None] * enc_bias) * scale
    q32 = q.astype(F32)
    grad_w_key = z.T[:, :, None] * q32[None]
    dq = dot('hw,whd->hd', z.astype(BF16), w_key)
    grad_w_query = probe[:, None, None] * dq[None]
    grad_probe = lax.psum(dot('whd,hd->w', w_query, dq.astype(BF16)), 'tp')
    grad_w_value = dot('bhw,bhd->whd', r_bf, do)
    return (pooled, grad_encoded, grad_probe, grad_w_query, grad_w_key, grad_w_value, grad_w_out, grad_w_up, grad_w_down)


def solution(mesh):
    return jax.shard_map(local_head, mesh=mesh, in_specs=IN_SPECS, out_specs=OUT_SPECS, check_vma=False)
```

```python
import functools
import jax
import jax.numpy as jnp
from jax import lax
from jax.experimental import pallas as pl
from jax.experimental.pallas import tpu as pltpu
from jax.sharding import PartitionSpec as P

NORM_EPS = 1e-6
F32 = jnp.float32
BF16 = jnp.bfloat16
IN_SPECS = (P('dp', 'sp', None), P(), P(), P(), P(None, 'tp', None), P('tp', None), P(None, 'tp', None), P(None, 'tp', None), P('tp', None), P('tp', None, None), P(), P(), P(), P(None, 'tp'), P('tp'), P('tp', None), P(), P('dp', None))
OUT_SPECS = (P('dp', None), P('dp', 'sp', None), P('dp'), P('dp', 'tp', None), P('dp', 'tp', None), P('dp', 'tp', None), P(('dp', 'tp'), None, None), P('dp', 'tp'), P(('dp', 'tp'), None))
NN = (((1,), (0,)), ((), ()))
NT = (((1,), (1,)), ((), ()))
TN = (((0,), (0,)), ((), ()))


def mm(a, b, dims=NN):
    return lax.dot_general(a, b, dims, preferred_element_type=F32)


def dot(spec, a, b):
    return jnp.einsum(spec, a, b, preferred_element_type=F32)


def row_stats(xs):
    mean = jnp.mean(xs, axis=-1, keepdims=True)
    cen = xs - mean
    return cen, lax.rsqrt(jnp.mean(cen * cen, axis=-1, keepdims=True) + NORM_EPS)


def fwd_body(nk, x_ref, gu_ref, bu_ref, xh_ref, sx_ref, rs_ref, r_ref, ml_ref):
    images, tokens, width = x_ref.shape
    nh = nk // 2
    strip = 16
    for i in range(images):
        for j in range(0, tokens, strip):
            cen, rstd = row_stats(x_ref[i, j:j + strip, :].astype(F32))
            xh_ref[i, j:j + strip, :] = (cen * rstd).astype(BF16)
            rs_ref[0, j:j + strip, i * nk:(i + 1) * nk] = jnp.broadcast_to(rstd, (strip, nk))
    parts = []
    for i in range(images):
        s2 = mm(xh_ref[i], gu_ref[...], NT)
        parts.append(s2[:, :nk] + s2[:, nk:])
    sx = jnp.concatenate(parts, axis=1)
    sx_ref[0] = sx
    s = sx + bu_ref[...]
    m = jnp.max(s, axis=0, keepdims=True)
    e = jnp.exp(s - m)
    l = jnp.sum(e, axis=0, keepdims=True)
    row = lax.broadcasted_iota(jnp.int32, (8, m.shape[1]), 0)
    ml_ref[0] = jnp.where(row == 0, m, l)
    et = jnp.transpose(e.astype(BF16))
    for i in range(images):
        r_ref[:, i, :] = mm(et[i * nk:i * nk + nh], xh_ref[i])


def run_fwd(x, gu2, bu):
    nb, tokens, width = x.shape
    nk = gu2.shape[0] // 2
    bi = 128 // nk
    ng = nb // bi
    return pl.pallas_call(
        functools.partial(fwd_body, nk),
        grid=(ng,),
        in_specs=[
            pl.BlockSpec((bi, tokens, width), lambda i: (i, 0, 0)),
            pl.BlockSpec(gu2.shape, lambda i: (0, 0)),
            pl.BlockSpec(bu.shape, lambda i: (0, 0)),
        ],
        out_specs=[
            pl.BlockSpec((bi, tokens, width), lambda i: (i, 0, 0)),
            pl.BlockSpec((1, tokens, 128), lambda i: (i, 0, 0)),
            pl.BlockSpec((1, tokens, 128), lambda i: (i, 0, 0)),
            pl.BlockSpec((nk // 2, bi, width), lambda i: (0, i, 0)),
            pl.BlockSpec((1, 8, 128), lambda i: (i, 0, 0)),
        ],
        out_shape=[
            jax.ShapeDtypeStruct((nb, tokens, width), BF16),
            jax.ShapeDtypeStruct((ng, tokens, 128), F32),
            jax.ShapeDtypeStruct((ng, tokens, 128), F32),
            jax.ShapeDtypeStruct((nk // 2, nb, width), F32),
            jax.ShapeDtypeStruct((ng, 8, 128), F32),
        ],
        cost_estimate=pl.CostEstimate(flops=8_000_000_000, bytes_accessed=40_000_000, transcendentals=0),
        name='fwd_tokens',
    )(x, gu2, bu)


def bwd_body(nk, xh_ref, sx_ref, rs_ref, gt_ref, gu_ref, aux_ref, dx_ref, z_ref, dl_ref, zacc_ref):
    step = pl.program_id(0)
    images, tokens, width = xh_ref.shape
    nh = nk // 2

    @pl.when(step == 0)
    def _():
        zacc_ref[...] = jnp.zeros_like(zacc_ref)

    sx = sx_ref[0]
    rstd = rs_ref[0]
    dpx = jnp.concatenate([mm(xh_ref[i], gt_ref[i], NT) for i in range(images)], axis=1)
    p = jnp.exp(sx - aux_ref[0, 0:1]) * aux_ref[0, 1:2]
    ds = p * (dpx + aux_ref[0, 2:3])
    dl_ref[0] = jnp.broadcast_to(jnp.sum(ds, axis=0, keepdims=True), dl_ref.shape[1:])
    prod = (ds * sx + p * dpx) * rstd * (1.0 / width)
    ph = prod.astype(BF16)
    po = (prod - ph.astype(F32)).astype(BF16)
    g0 = lax.broadcasted_iota(jnp.int32, (128, 128), 0) // nk
    g1 = lax.broadcasted_iota(jnp.int32, (128, 128), 1) // nk
    ind = jnp.where(g0 == g1, 1.0, 0.0).astype(BF16)
    c2 = mm(ph, ind) + mm(po, ind)
    dst = jnp.transpose(ds.astype(BF16))
    ca = (ds * rstd).astype(BF16)
    cb = (p * rstd).astype(BF16)
    z = zacc_ref[...]
    for i in range(images):
        xh = xh_ref[i]
        z = z + mm(dst[i * nk:i * nk + nh], xh)
        coef = jnp.concatenate([ca[:, i * nk:(i + 1) * nk], cb[:, i * nk:(i + 1) * nk]], axis=1)
        dxh = mm(coef, jnp.concatenate([gu_ref[...], gt_ref[i]], axis=0))
        dx_ref[i] = (dxh - c2[:, i * nk:i * nk + 1] * xh.astype(F32)).astype(BF16)
    zacc_ref[...] = z
    z_ref[...] = z


def run_bwd(xh, sx, rs, gt, gu_hi, aux):
    nb, tokens, width = xh.shape
    nk = gu_hi.shape[0]
    bi = 128 // nk
    ng = nb // bi
    return pl.pallas_call(
        functools.partial(bwd_body, nk),
        grid=(ng,),
        in_specs=[
            pl.BlockSpec((bi, tokens, width), lambda i: (i, 0, 0)),
            pl.BlockSpec((1, tokens, 128), lambda i: (i, 0, 0)),
            pl.BlockSpec((1, tokens, 128), lambda i: (i, 0, 0)),
            pl.BlockSpec((bi, nk, width), lambda i: (i, 0, 0)),
            pl.BlockSpec((nk, width), lambda i: (0, 0)),
            pl.BlockSpec((1, 8, 128), lambda i: (i, 0, 0)),
        ],
        out_specs=[
            pl.BlockSpec((bi, tokens, width), lambda i: (i, 0, 0)),
            pl.BlockSpec((nk // 2, width), lambda i: (0, 0)),
            pl.BlockSpec((1, 8, 128), lambda i: (i, 0, 0)),
        ],
        out_shape=[
            jax.ShapeDtypeStruct((nb, tokens, width), BF16),
            jax.ShapeDtypeStruct((nk // 2, width), F32),
            jax.ShapeDtypeStruct((ng, 8, 128), F32),
        ],
        scratch_shapes=[pltpu.VMEM((nk // 2, width), F32)],
        cost_estimate=pl.CostEstimate(flops=12_000_000_000, bytes_accessed=40_000_000, transcendentals=0),
        name='bwd_tokens',
    )(xh, sx, rs, gt, gu_hi, aux)


MESH = pl.DeviceIdType.MESH
VM = pl.BlockSpec(memory_space=pltpu.VMEM)
ANY = pl.BlockSpec(memory_space=pl.ANY)


def send(src, dst, sems, k, where):
    copy = pltpu.make_async_remote_copy(src_ref=src, dst_ref=dst, send_sem=sems.at[0, k], recv_sem=sems.at[1, k], device_id=where, device_id_type=MESH)
    copy.start()
    return copy


def greet(places):
    barrier = pltpu.get_barrier_semaphore()
    for where in places:
        pl.semaphore_signal(barrier, inc=1, device_id=where, device_id_type=MESH)
    pl.semaphore_wait(barrier, len(places))


def places():
    tp = lax.axis_index('tp')
    sp = lax.axis_index('sp')
    core = lax.rem(sp, 2)
    return {'tp': 1 - tp}, {'sp': sp + 1 - 2 * core}, {'sp': lax.rem(sp + 2, 4)}, core


def two(a):
    hi = a.astype(BF16)
    return hi, (a - hi.astype(F32)).astype(BF16)


def three(a):
    hi, rest = a.astype(BF16), a
    rest = rest - hi.astype(F32)
    mid = rest.astype(BF16)
    return hi, mid, (rest - mid.astype(F32)).astype(BF16)


def head_mask(rows, nh, hd):
    lane = lax.broadcasted_iota(jnp.int32, (rows, nh * hd), 1)
    row = lax.broadcasted_iota(jnp.int32, (rows, nh * hd), 0)
    return jnp.logical_and(lane >= row * hd, lane < (row + 1) * hd)


def unpack(packed, nk):
    groups, lanes = packed.shape
    per = lanes // nk
    rows = jnp.concatenate([jnp.broadcast_to(packed[g:g + 1], (per, lanes)) for g in range(groups)], axis=0)
    keep = own_lanes(rows.shape, nk, per)
    rows = jnp.where(keep, rows, 0.0)
    shift = nk
    while shift < lanes:
        rows = rows + pltpu.roll(rows, shift, 1)
        shift *= 2
    return rows


def own_lanes(shape, nk, per):
    lane = lax.broadcasted_iota(jnp.int32, shape, 1)
    row = lax.rem(lax.broadcasted_iota(jnp.int32, shape, 0), per)
    return jnp.logical_and(lane >= row * nk, lane < (row + 1) * nk)


def pack(rows, nk):
    images, lanes = rows.shape
    per = lanes // nk
    shift = nk
    while shift < lanes:
        rows = rows + pltpu.roll(rows, shift, 1)
        shift *= 2
    rows = jnp.where(own_lanes(rows.shape, nk, per), rows, 0.0)
    return jnp.concatenate([jnp.sum(rows[g * per:(g + 1) * per], axis=0, keepdims=True) for g in range(images // per)], axis=0)


def query_body(nh, hd, probe_ref, wq_ref, bq_ref, wk_ref, wv_ref, bv_ref, gain_ref, bias_ref, gu_ref, bu_ref, q_ref, cb_ref, us_ref, ur_ref, sems):
    tp_peer, _, _, _ = places()
    greet([tp_peer])
    width = probe_ref.shape[1]
    nk = 2 * nh
    q = (mm(jnp.broadcast_to(probe_ref[...], (8, width)).astype(BF16), wq_ref[...], NT)[:1] + bq_ref[...]).astype(BF16)
    q_ref[...] = q.astype(F32)
    qd = jnp.where(head_mask(nh, nh, hd), jnp.broadcast_to(q.astype(F32), (nh, nh * hd)), 0.0).astype(BF16)
    u = mm(qd, wk_ref[...])
    us_ref[...] = u
    copy = send(us_ref, ur_ref, sems, 0, tp_peer)
    bias = bias_ref[...]
    bh, bl = two(bias)
    row = lax.broadcasted_iota(jnp.int32, (8, width), 0)
    b2 = jnp.where(row == 0, bh.astype(F32), jnp.where(row == 1, bl.astype(F32), 0.0)).astype(BF16)
    cb_ref[...] = jnp.sum(mm(b2, wv_ref[...], NT), axis=0, keepdims=True) + bv_ref[...]
    copy.wait()
    scale = hd ** -0.5
    ua = jnp.concatenate([u, ur_ref[...]], axis=0) * scale
    gu = ua * gain_ref[...]
    gu = gu - jnp.mean(gu, axis=1, keepdims=True)
    gh, gl = two(gu)
    gu_ref[:nk] = gh
    gu_ref[nk:] = gl
    bu = jnp.broadcast_to(jnp.sum(ua * bias, axis=1, keepdims=True), (nk, 128))
    bu_ref[...] = jnp.transpose(jnp.concatenate([bu] * (128 // nk), axis=0))[:1]


def run_query(nh, hd, probe, wq, bq, wk, wv, bv, gain, bias):
    width = probe.shape[1]
    return pl.pallas_call(
        functools.partial(query_body, nh, hd),
        in_specs=[VM] * 8,
        out_specs=[VM] * 4,
        out_shape=[
            jax.ShapeDtypeStruct((4 * nh, width), BF16),
            jax.ShapeDtypeStruct((1, 128), F32),
            jax.ShapeDtypeStruct((1, nh * hd), F32),
            jax.ShapeDtypeStruct((1, nh * hd), F32),
        ],
        scratch_shapes=[pltpu.VMEM((nh, width), F32), pltpu.VMEM((nh, width), F32), pltpu.SemaphoreType.DMA((2, 1))],
        compiler_params=pltpu.CompilerParams(collective_id=0, has_side_effects=True),
        cost_estimate=pl.CostEstimate(flops=50_000_000, bytes_accessed=6_000_000, transcendentals=0),
        name='query_fold',
    )(probe, wq, bq, wk, wv, bv, gain, bias)


def swap_halves(src, buf, sems, k, tp_peer, core):
    half = src.shape[0] // 2
    rows = pl.ds(pl.multiple_of(core * half, half), half)
    return send(src.at[rows], buf.at[rows], sems, k, tp_peer)


def pass_on(buf, sems, k, sib, core):
    half = buf.shape[0] // 2
    rows = pl.ds(pl.multiple_of(core * half, half), half)
    return send(buf.at[rows], buf.at[rows], sems, k, sib)


def head_body(nh, hd, r_ref, ml_ref, wv_ref, wvh_ref, wo_ref, wup_hbm, wdn_hbm, gain_ref, bu_ref, cb_ref, bo_ref, hg_ref, hb_ref, bup_ref, bdn_ref, og_ref,
              y_out, g_out, dpre_out, o_out, da_out, pooled_out, do_out, gt_out, aux_out, rf_out,
              wup, wdn, wvs, osd, mls, ora, mra, osd2, mls2, orb, mrb, aps, apr, rs, ra, rb, rc, rd, re, dys, dyr, mps, mpr, dor, kps, kpr, dg_s, lsem, sems):
    tp_peer, sib, xp, core = places()
    nk = 2 * nh
    nb = og_ref.shape[0]
    width = og_ref.shape[1]
    load_up = pltpu.make_async_copy(wup_hbm, wup, lsem.at[0])
    load_dn = pltpu.make_async_copy(wdn_hbm, wdn, lsem.at[1])
    load_dn.start()
    load_up.start()
    gain = gain_ref[...]
    groups = ml_ref.shape[0]
    for h in range(nh):
        rh = (r_ref[h] * gain).astype(BF16)
        osd[:, h * hd:(h + 1) * hd] = mm(rh, wv_ref[h * hd:(h + 1) * hd, :], NT)
    m0 = jnp.concatenate([ml_ref[g, 0:1] for g in range(groups)], axis=0)
    l0 = jnp.concatenate([ml_ref[g, 1:2] for g in range(groups)], axis=0)
    mls[:groups] = m0
    mls[groups:] = l0
    greet([tp_peer, sib, xp])
    c_wv = send(wvh_ref, wvs, sems, 0, sib)
    c1 = send(osd, ora, sems, 1, sib)
    c2 = send(mls, mra, sems, 2, sib)
    onehot = jnp.where(head_mask(128, nh, hd), 1.0, 0.0).astype(BF16)

    def spread(rows):
        return sum(mm(part, onehot) for part in three(rows))

    def join(oa, ma, la, ob, mb, lb):
        mn = jnp.maximum(ma, mb)
        fa, fb = jnp.exp(ma - mn), jnp.exp(mb - mn)
        o = oa * spread(unpack(fa, nk)) + ob * spread(unpack(fb, nk))
        return o, mn, fa * la + fb * lb

    c1.wait()
    c2.wait()
    o1, m1, l1 = join(osd[...], m0, l0, ora[...], mra[:groups], mra[groups:])
    osd2[...] = o1
    mls2[:groups] = m1
    mls2[groups:] = l1
    c3 = send(osd2, orb, sems, 3, xp)
    c4 = send(mls2, mrb, sems, 4, xp)
    load_dn.wait()
    dg_s[...] = mm(og_ref[...], wdn[...], NT)
    c3.wait()
    c4.wait()
    o, m, l = join(o1, m1, l1, orb[...], mrb[:groups], mrb[groups:])
    inv_l = 1.0 / l
    o = o * spread(unpack(inv_l, nk)) + cb_ref[...]
    o_bf = o.astype(BF16)
    o_out[...] = o_bf
    ap = mm(o_bf, wo_ref[...])
    aps[...] = ap
    c5 = swap_halves(aps, apr, sems, 5, tp_peer, core)
    wr = unpack(jnp.exp(m0 - m) * inv_l, nk)
    for h in range(nh):
        rs[h] = r_ref[h] * wr[:, h:h + 1]
    nq = nh // 2
    mine = pl.ds(core * nq, nq)
    theirs = pl.ds((1 - core) * nq, nq)
    r1 = send(rs.at[theirs], ra, sems, 6, sib)
    c5.wait()
    c6 = pass_on(apr, sems, 7, sib, core)
    r1.wait()
    rb[...] = rs[mine] + ra[...]
    r2 = send(rb, rc, sems, 8, xp)
    c6.wait()
    a = ap + apr[...] + bo_ref[...]
    acen, arstd = row_stats(a)
    ahat = acen * arstd
    y = (ahat * hg_ref[...] + hb_ref[...]).astype(BF16)
    y_out[...] = y
    load_up.wait()
    pre = mm(y, wup[...]) + bup_ref[...]
    k0 = 0.7978845608028654
    k1 = 0.044715
    sq = pre * pre
    th = jnp.tanh(k0 * (pre + k1 * (pre * sq)))
    half = 0.5 * (1.0 + th)
    g = (pre * half).astype(BF16)
    g_out[...] = g
    dgelu = half + 0.5 * pre * (1.0 - th * th) * (k0 * (1.0 + 3.0 * k1 * sq))
    dpre = (dg_s[...] * dgelu).astype(BF16)
    dpre_out[...] = dpre
    dyp = mm(dpre, wup[...], NT)
    dys[...] = dyp
    c7 = swap_halves(dys, dyr, sems, 9, tp_peer, core)
    mp = mm(g, wdn[...])
    mps[...] = mp
    c8 = swap_halves(mps, mpr, sems, 10, tp_peer, core)
    c_wv.wait()
    c7.wait()
    c9 = pass_on(dyr, sems, 11, sib, core)
    c9.wait()
    dah = (dyp + dyr[...]) * hg_ref[...]
    da = arstd * (dah - jnp.mean(dah, axis=1, keepdims=True) - ahat * jnp.mean(dah * ahat, axis=1, keepdims=True))
    da = (og_ref[...].astype(F32) + da).astype(BF16)
    da_out[...] = da
    do_bf = mm(da, wo_ref[...], NT).astype(BF16)
    do = do_bf.astype(F32)
    do_out[...] = do
    kap = sum(mm(part, onehot, NT) for part in two(do * (cb_ref[...] - o)))
    kps[...] = kap
    c10 = swap_halves(do_out, dor, sems, 12, tp_peer, core)
    c11 = send(kps, kpr, sems, 13, tp_peer)

    def back(k, h, d, w):
        t = mm(d, w) * gain
        t = t - jnp.mean(t, axis=1, keepdims=True)
        gt_out[:, k * nh + h, :] = t

    for h in range(nh):
        back(0, h, do_bf[:, h * hd:(h + 1) * hd], wv_ref[h * hd:(h + 1) * hd, :])
    c10.wait()
    c12 = pass_on(dor, sems, 14, sib, core)
    c8.wait()
    c13 = pass_on(mpr, sems, 15, sib, core)
    c11.wait()
    kall = kap + pltpu.roll(kpr[...], nh, 1)
    kpk = pack(kall, nk)
    mb = m - bu_ref[...]
    for g_ in range(groups):
        aux_out[g_, 0:1] = mb[g_:g_ + 1]
        aux_out[g_, 1:2] = inv_l[g_:g_ + 1]
        aux_out[g_, 2:3] = kpk[g_:g_ + 1]
    c12.wait()
    dob = dor[...].astype(BF16)
    first = core == 0
    for h in range(nh):
        lo = (h % nq) * hd
        mine_w = wvh_ref[lo:lo + hd, :]
        sib_w = wvs[lo:lo + hd, :]
        pick = first if h < nq else jnp.logical_not(first)
        w = jnp.where(pick, mine_w, sib_w).astype(BF16)
        back(1, h, dob[:, h * hd:(h + 1) * hd], w)
    c13.wait()
    pooled_out[...] = (a + mp + mpr[...] + bdn_ref[...]).astype(BF16)
    r2.wait()
    rd[...] = rb[...] + rc[...]
    r3 = send(rd, re, sems, 16, sib)
    rf_out[mine] = rd[...]
    r3.wait()
    rf_out[theirs] = re[...]


def run_head(nh, hd, r_raw, ml, wv, wvh, wo, w_up, w_down, gain, bu, cb, b_out, hgain, hbias, b_up, b_down, out_grad):
    nb, width = out_grad.shape
    ff = w_up.shape[1]
    nd = nh * hd
    groups = ml.shape[0]
    full = pltpu.VMEM((nb, width), F32)
    heads = pltpu.VMEM((nb, nd), F32)
    stat = pltpu.VMEM((2 * groups, 128), F32)
    rhalf = pltpu.VMEM((nh // 2, nb, width), F32)
    return pl.pallas_call(
        functools.partial(head_body, nh, hd),
        in_specs=[VM] * 5 + [ANY] * 2 + [VM] * 9,
        out_specs=[VM] * 10,
        out_shape=[
            jax.ShapeDtypeStruct((nb, width), BF16),
            jax.ShapeDtypeStruct((nb, ff), BF16),
            jax.ShapeDtypeStruct((nb, ff), BF16),
            jax.ShapeDtypeStruct((nb, nd), BF16),
            jax.ShapeDtypeStruct((nb, width), BF16),
            jax.ShapeDtypeStruct((nb, width), BF16),
            jax.ShapeDtypeStruct((nb, nd), F32),
            jax.ShapeDtypeStruct((nb, 2 * nh, width), F32),
            jax.ShapeDtypeStruct((groups, 8, 128), F32),
            jax.ShapeDtypeStruct((nh, nb, width), F32),
        ],
        scratch_shapes=[
            pltpu.VMEM(w_up.shape, BF16), pltpu.VMEM(w_down.shape, BF16), pltpu.VMEM(wvh.shape, F32),
            heads, stat, heads, stat, heads, stat, heads, stat,
            full, full, pltpu.VMEM((nh, nb, width), F32), rhalf, rhalf, rhalf, rhalf, rhalf,
            full, full, full, full, heads, pltpu.VMEM((nb, 128), F32), pltpu.VMEM((nb, 128), F32),
            pltpu.VMEM((nb, ff), F32),
            pltpu.SemaphoreType.DMA((2,)), pltpu.SemaphoreType.DMA((2, 17)),
        ],
        compiler_params=pltpu.CompilerParams(collective_id=1, has_side_effects=True, vmem_limit_bytes=60 * 1024 * 1024),
        cost_estimate=pl.CostEstimate(flops=3_000_000_000, bytes_accessed=30_000_000, transcendentals=0),
        name='pool_head',
    )(r_raw, ml, wv, wvh, wo, w_up, w_down, gain, bu, cb, b_out, hgain, hbias, b_up, b_down, out_grad)


def tail_body(nh, hd, z_ref, dl_ref, rf_ref, wk_ref, wq_ref, gain_ref, z_out, dq_out, gp_out, zs, za, zs2, zb, ps, pr, sems):
    tp_peer, sib, xp, core = places()
    nk = 2 * nh
    groups = dl_ref.shape[0]
    nb = rf_ref.shape[1]
    width = z_ref.shape[1]
    cols = 128
    zs[:nh] = z_ref[...]
    zs[nh:, :cols] = jnp.concatenate([dl_ref[g, 0:1] for g in range(groups)], axis=0)
    greet([tp_peer, sib, xp])
    c1 = send(zs, za, sems, 0, sib)
    c1.wait()
    zs2[...] = zs[...] + za[...]
    c2 = send(zs2, zb, sems, 1, xp)
    c2.wait()
    z = zs2[:nh] + zb[:nh]
    dl = unpack(zs2[nh:, :cols] + zb[nh:, :cols], nk)
    fix = jnp.concatenate([jnp.sum(rf_ref[h] * dl[:, h:h + 1], axis=0, keepdims=True) for h in range(nh)], axis=0)
    z = (z - fix) * gain_ref[...] * (hd ** -0.5)
    z_out[...] = z
    dqm = mm(z.astype(BF16), wk_ref[...], NT)
    dq = jnp.sum(jnp.where(head_mask(nh, nh, hd), dqm, 0.0), axis=0, keepdims=True)
    dq_out[...] = dq
    gp = mm(jnp.broadcast_to(dq, (8, nh * hd)).astype(BF16), wq_ref[...])
    ps[...] = gp
    c3 = send(ps, pr, sems, 2, tp_peer)
    c3.wait()
    gp_out[...] = gp[:1] + pr[:1]


def run_tail(nh, hd, z, dl, rf, wk, wq, gain):
    width = z.shape[1]
    zz = pltpu.VMEM((nh + dl.shape[0], width), F32)
    pp = pltpu.VMEM((8, width), F32)
    return pl.pallas_call(
        functools.partial(tail_body, nh, hd),
        in_specs=[VM] * 6,
        out_specs=[VM] * 3,
        out_shape=[
            jax.ShapeDtypeStruct((nh, width), F32),
            jax.ShapeDtypeStruct((1, nh * hd), F32),
            jax.ShapeDtypeStruct((1, width), F32),
        ],
        scratch_shapes=[zz, zz, zz, zz, pp, pp, pltpu.SemaphoreType.DMA((2, 3))],
        compiler_params=pltpu.CompilerParams(collective_id=2, has_side_effects=True),
        cost_estimate=pl.CostEstimate(flops=50_000_000, bytes_accessed=6_000_000, transcendentals=0),
        name='query_back',
    )(z, dl, rf, wk, wq, gain)


def local_head(encoded, enc_gain, enc_bias, probe, w_query, b_query, w_key, w_value, b_value, w_out, b_out, head_gain, head_bias, w_up, b_up, w_down, b_down, out_grad):
    nh, hd = b_query.shape
    width = probe.shape[0]
    nd = nh * hd

    def flat(w):
        return jnp.transpose(w, (1, 2, 0)).reshape(nd, width)

    def heads(g):
        return jnp.transpose(g.reshape(nh, hd, width), (2, 0, 1))

    wq, wk, wv, wo = flat(w_query), flat(w_key), flat(w_value), w_out.reshape(nd, width)
    core = lax.rem(lax.axis_index('sp'), 2)
    wvh = lax.dynamic_slice_in_dim(wv, core * (nd // 2), nd // 2, 0).astype(F32)
    wvh = lax.ppermute(wvh, 'tp', [(0, 1), (1, 0)])
    gain, bias = enc_gain[None], enc_bias[None]
    gu2, bu, q, cb = run_query(nh, hd, probe[None], wq, b_query.reshape(1, nd), wk, wv, b_value.reshape(1, nd), gain, bias)
    xh, sx, rs, r_raw, ml = run_fwd(encoded, gu2, bu)
    y, g, dpre, o_bf, da, pooled, do, gt, aux, rf = run_head(nh, hd, r_raw, ml, wv, wvh, wo, w_up, w_down, gain, bu, cb, b_out[None], head_gain[None], head_bias[None], b_up[None], b_down[None], out_grad)
    grad_w_down = mm(g, out_grad, TN)
    grad_w_up = mm(y, dpre, TN)
    grad_w_out = mm(o_bf, da, TN).reshape(nh, hd, width)
    grad_encoded, z, dl = run_bwd(xh, sx, rs, gt.astype(BF16), gu2[:2 * nh], aux)
    z, dq, gp = run_tail(nh, hd, z, dl, rf, wk, wq, gain)
    r_bf = (rf * gain + bias).astype(BF16)
    do3 = do.astype(BF16).reshape(-1, nh, hd)
    grad_w_value = heads(dot('bhd,hbw->hdw', do3, r_bf))
    grad_w_key = heads(q.reshape(nh, hd, 1) * z[:, None, :])
    grad_w_query = heads(dq.reshape(nd, 1) * probe[None])
    return (pooled, grad_encoded, gp[0], grad_w_query, grad_w_key, grad_w_value, grad_w_out, grad_w_up, grad_w_down)


def solution(mesh):
    return jax.shard_map(local_head, mesh=mesh, in_specs=IN_SPECS, out_specs=OUT_SPECS, check_vma=False)
```

```python
import functools
import jax
import jax.numpy as jnp
from jax import lax
from jax.experimental import pallas as pl
from jax.experimental.pallas import tpu as pltpu
from jax.sharding import PartitionSpec as P

NORM_EPS = 1e-6
F32 = jnp.float32
BF16 = jnp.bfloat16
IN_SPECS = (P('dp', 'sp', None), P(), P(), P(), P(None, 'tp', None), P('tp', None), P(None, 'tp', None), P(None, 'tp', None), P('tp', None), P('tp', None, None), P(), P(), P(), P(None, 'tp'), P('tp'), P('tp', None), P(), P('dp', None))
OUT_SPECS = (P('dp', None), P('dp', 'sp', None), P('dp'), P('dp', 'tp', None), P('dp', 'tp', None), P('dp', 'tp', None), P(('dp', 'tp'), None, None), P('dp', 'tp'), P(('dp', 'tp'), None))
NN = (((1,), (0,)), ((), ()))
NT = (((1,), (1,)), ((), ()))
TN = (((0,), (0,)), ((), ()))


def mm(a, b, dims=NN):
    return lax.dot_general(a, b, dims, preferred_element_type=F32)


def dot(spec, a, b):
    return jnp.einsum(spec, a, b, preferred_element_type=F32)


def row_stats(xs):
    mean = jnp.mean(xs, axis=-1, keepdims=True)
    cen = xs - mean
    return cen, lax.rsqrt(jnp.mean(cen * cen, axis=-1, keepdims=True) + NORM_EPS)


def fwd_body(nk, x_ref, gu_ref, bu_ref, xh_ref, sx_ref, rs_ref, r_ref, ml_ref):
    images, tokens, width = x_ref.shape
    nh = nk // 2
    strip = 16
    for i in range(images):
        for j in range(0, tokens, strip):
            cen, rstd = row_stats(x_ref[i, j:j + strip, :].astype(F32))
            xh_ref[i, j:j + strip, :] = (cen * rstd).astype(BF16)
            rs_ref[0, j:j + strip, i * nk:(i + 1) * nk] = jnp.broadcast_to(rstd, (strip, nk))
    parts = []
    for i in range(images):
        s2 = mm(xh_ref[i], gu_ref[...], NT)
        parts.append(s2[:, :nk] + s2[:, nk:])
    sx = jnp.concatenate(parts, axis=1)
    sx_ref[0] = sx
    s = sx + bu_ref[...]
    m = jnp.max(s, axis=0, keepdims=True)
    e = jnp.exp(s - m)
    l = jnp.sum(e, axis=0, keepdims=True)
    row = lax.broadcasted_iota(jnp.int32, (8, m.shape[1]), 0)
    ml_ref[0] = jnp.where(row == 0, m, l)
    et = jnp.transpose(e.astype(BF16))
    for i in range(images):
        r_ref[:, i, :] = mm(et[i * nk:i * nk + nh], xh_ref[i])


def run_fwd(x, gu2, bu):
    nb, tokens, width = x.shape
    nk = gu2.shape[0] // 2
    bi = 128 // nk
    ng = nb // bi
    return pl.pallas_call(
        functools.partial(fwd_body, nk),
        grid=(ng,),
        in_specs=[
            pl.BlockSpec((bi, tokens, width), lambda i: (i, 0, 0)),
            pl.BlockSpec(gu2.shape, lambda i: (0, 0)),
            pl.BlockSpec(bu.shape, lambda i: (0, 0)),
        ],
        out_specs=[
            pl.BlockSpec((bi, tokens, width), lambda i: (i, 0, 0)),
            pl.BlockSpec((1, tokens, 128), lambda i: (i, 0, 0)),
            pl.BlockSpec((1, tokens, 128), lambda i: (i, 0, 0)),
            pl.BlockSpec((nk // 2, bi, width), lambda i: (0, i, 0)),
            pl.BlockSpec((1, 8, 128), lambda i: (i, 0, 0)),
        ],
        out_shape=[
            jax.ShapeDtypeStruct((nb, tokens, width), BF16),
            jax.ShapeDtypeStruct((ng, tokens, 128), F32),
            jax.ShapeDtypeStruct((ng, tokens, 128), F32),
            jax.ShapeDtypeStruct((nk // 2, nb, width), F32),
            jax.ShapeDtypeStruct((ng, 8, 128), F32),
        ],
        cost_estimate=pl.CostEstimate(flops=8_000_000_000, bytes_accessed=40_000_000, transcendentals=0),
        name='fwd_tokens',
    )(x, gu2, bu)


def bwd_body(nk, xh_ref, sx_ref, rs_ref, gt_ref, gu_ref, aux_ref, yt_ref, dpre_ref, ht_ref, og_ref, ot_ref, da_ref, dx_ref, z_ref, dl_ref, gup_ref, gdn_ref, gwo_ref, zacc_ref):
    step = pl.program_id(0)
    images, tokens, width = xh_ref.shape
    nh = nk // 2

    @pl.when(step == 0)
    def _():
        zacc_ref[...] = jnp.zeros_like(zacc_ref)

    gup_ref[...] = mm(yt_ref[...], dpre_ref[...])
    gdn_ref[...] = mm(ht_ref[...], og_ref[...])
    gwo_ref[...] = mm(ot_ref[...], da_ref[...])
    sx = sx_ref[0]
    rstd = rs_ref[0]
    gts = [gt_ref[:, i, :].astype(BF16) for i in range(images)]
    dpx = jnp.concatenate([mm(xh_ref[i], gts[i], NT) for i in range(images)], axis=1)
    p = jnp.exp(sx - aux_ref[0, 0:1]) * aux_ref[0, 1:2]
    ds = p * (dpx + aux_ref[0, 2:3])
    dl_ref[0] = jnp.broadcast_to(jnp.sum(ds, axis=0, keepdims=True), dl_ref.shape[1:])
    prod = (ds * sx + p * dpx) * rstd * (1.0 / width)
    ph = prod.astype(BF16)
    po = (prod - ph.astype(F32)).astype(BF16)
    g0 = lax.broadcasted_iota(jnp.int32, (128, 128), 0) // nk
    g1 = lax.broadcasted_iota(jnp.int32, (128, 128), 1) // nk
    ind = jnp.where(g0 == g1, 1.0, 0.0).astype(BF16)
    c2 = mm(ph, ind) + mm(po, ind)
    dst = jnp.transpose(ds.astype(BF16))
    ca = (ds * rstd).astype(BF16)
    cb = (p * rstd).astype(BF16)
    z = zacc_ref[...]
    for i in range(images):
        xh = xh_ref[i]
        z = z + mm(dst[i * nk:i * nk + nh], xh)
        coef = jnp.concatenate([ca[:, i * nk:(i + 1) * nk], cb[:, i * nk:(i + 1) * nk]], axis=1)
        dxh = mm(coef, jnp.concatenate([gu_ref[...], gts[i]], axis=0))
        dx_ref[i] = (dxh - c2[:, i * nk:i * nk + 1] * xh.astype(F32)).astype(BF16)
    zacc_ref[...] = z
    z_ref[...] = z


def run_bwd(xh, sx, rs, gt, gu2, aux, yt, dpre, ht, out_grad, ot, da):
    nb, tokens, width = xh.shape
    nk = gu2.shape[0] // 2
    bi = 128 // nk
    ng = nb // bi
    ff, nd = ht.shape[0], ot.shape[0]
    return pl.pallas_call(
        functools.partial(bwd_body, nk),
        grid=(ng,),
        in_specs=[
            pl.BlockSpec((bi, tokens, width), lambda i: (i, 0, 0)),
            pl.BlockSpec((1, tokens, 128), lambda i: (i, 0, 0)),
            pl.BlockSpec((1, tokens, 128), lambda i: (i, 0, 0)),
            pl.BlockSpec((nk, bi, width), lambda i: (0, i, 0)),
            pl.BlockSpec((nk, width), lambda i: (0, 0)),
            pl.BlockSpec((1, 8, 128), lambda i: (i, 0, 0)),
            pl.BlockSpec((width // ng, nb), lambda i: (i, 0)),
            pl.BlockSpec((nb, ff), lambda i: (0, 0)),
            pl.BlockSpec((ff // ng, nb), lambda i: (i, 0)),
            pl.BlockSpec((nb, width), lambda i: (0, 0)),
            pl.BlockSpec((nd // ng, nb), lambda i: (i, 0)),
            pl.BlockSpec((nb, width), lambda i: (0, 0)),
        ],
        out_specs=[
            pl.BlockSpec((bi, tokens, width), lambda i: (i, 0, 0)),
            pl.BlockSpec((nk // 2, width), lambda i: (0, 0)),
            pl.BlockSpec((1, 8, 128), lambda i: (i, 0, 0)),
            pl.BlockSpec((width // ng, ff), lambda i: (i, 0)),
            pl.BlockSpec((ff // ng, width), lambda i: (i, 0)),
            pl.BlockSpec((nd // ng, width), lambda i: (i, 0)),
        ],
        out_shape=[
            jax.ShapeDtypeStruct((nb, tokens, width), BF16),
            jax.ShapeDtypeStruct((nk // 2, width), F32),
            jax.ShapeDtypeStruct((ng, 8, 128), F32),
            jax.ShapeDtypeStruct((width, ff), F32),
            jax.ShapeDtypeStruct((ff, width), F32),
            jax.ShapeDtypeStruct((nd, width), F32),
        ],
        scratch_shapes=[pltpu.VMEM((nk // 2, width), F32)],
        cost_estimate=pl.CostEstimate(flops=12_000_000_000, bytes_accessed=40_000_000, transcendentals=0),
        name='bwd_tokens',
    )(xh, sx, rs, gt, gu2, aux, yt, dpre, ht, out_grad, ot, da)


MESH = pl.DeviceIdType.MESH
VM = pl.BlockSpec(memory_space=pltpu.VMEM)
ANY = pl.BlockSpec(memory_space=pl.ANY)


def send(src, dst, sems, k, where):
    copy = pltpu.make_async_remote_copy(src_ref=src, dst_ref=dst, send_sem=sems.at[0, k], recv_sem=sems.at[1, k], device_id=where, device_id_type=MESH)
    copy.start()
    return copy


def greet(places):
    barrier = pltpu.get_barrier_semaphore()
    for where in places:
        pl.semaphore_signal(barrier, inc=1, device_id=where, device_id_type=MESH)
    pl.semaphore_wait(barrier, len(places))


def places():
    tp = lax.axis_index('tp')
    sp = lax.axis_index('sp')
    core = lax.rem(sp, 2)
    return {'tp': 1 - tp}, {'sp': sp + 1 - 2 * core}, {'sp': lax.rem(sp + 2, 4)}, core


def two(a):
    hi = a.astype(BF16)
    return hi, (a - hi.astype(F32)).astype(BF16)


def three(a):
    hi, rest = a.astype(BF16), a
    rest = rest - hi.astype(F32)
    mid = rest.astype(BF16)
    return hi, mid, (rest - mid.astype(F32)).astype(BF16)


def head_mask(rows, nh, hd):
    lane = lax.broadcasted_iota(jnp.int32, (rows, nh * hd), 1)
    row = lax.broadcasted_iota(jnp.int32, (rows, nh * hd), 0)
    return jnp.logical_and(lane >= row * hd, lane < (row + 1) * hd)


def unpack(packed, nk):
    groups, lanes = packed.shape
    per = lanes // nk
    rows = jnp.concatenate([jnp.broadcast_to(packed[g:g + 1], (per, lanes)) for g in range(groups)], axis=0)
    keep = own_lanes(rows.shape, nk, per)
    rows = jnp.where(keep, rows, 0.0)
    shift = nk
    while shift < lanes:
        rows = rows + pltpu.roll(rows, shift, 1)
        shift *= 2
    return rows


def own_lanes(shape, nk, per):
    lane = lax.broadcasted_iota(jnp.int32, shape, 1)
    row = lax.rem(lax.broadcasted_iota(jnp.int32, shape, 0), per)
    return jnp.logical_and(lane >= row * nk, lane < (row + 1) * nk)


def pack(rows, nk):
    images, lanes = rows.shape
    per = lanes // nk
    shift = nk
    while shift < lanes:
        rows = rows + pltpu.roll(rows, shift, 1)
        shift *= 2
    rows = jnp.where(own_lanes(rows.shape, nk, per), rows, 0.0)
    return jnp.concatenate([jnp.sum(rows[g * per:(g + 1) * per], axis=0, keepdims=True) for g in range(images // per)], axis=0)


def row_of(ref):
    return ref[...].reshape(1, ref.shape[0])


def flat_heads(ref):
    return jnp.concatenate([ref[h:h + 1, :] for h in range(ref.shape[0])], axis=1)


def query_body(nh, hd, probe_ref, wq_ref, bq_ref, wk_ref, wv_ref, bv_ref, gain_ref, bias_ref, gu_ref, bu_ref, q_ref, cb_ref, wvq_ref, us_ref, ur_ref, sems):
    tp_peer, _, _, _ = places()
    greet([tp_peer])
    width = probe_ref.shape[0]
    nk = 2 * nh
    q = (mm(jnp.broadcast_to(row_of(probe_ref), (8, width)).astype(BF16), wq_ref[...], NT)[:1] + flat_heads(bq_ref)).astype(BF16)
    q_ref[...] = q.astype(F32)
    qd = jnp.where(head_mask(nh, nh, hd), jnp.broadcast_to(q.astype(F32), (nh, nh * hd)), 0.0).astype(BF16)
    u = mm(qd, wk_ref[...])
    us_ref[...] = u
    copy = send(us_ref, ur_ref, sems, 0, tp_peer)
    bias = row_of(bias_ref)
    bh, bl = two(bias)
    row = lax.broadcasted_iota(jnp.int32, (8, width), 0)
    b2 = jnp.where(row == 0, bh.astype(F32), jnp.where(row == 1, bl.astype(F32), 0.0)).astype(BF16)
    cb_ref[...] = jnp.sum(mm(b2, wv_ref[...], NT), axis=0, keepdims=True) + flat_heads(bv_ref)
    quarter = wvq_ref.shape[0]
    wvq_ref[...] = wv_ref[pl.ds(pl.multiple_of(lax.axis_index('sp') * quarter, quarter), quarter), :].astype(F32)
    copy.wait()
    scale = hd ** -0.5
    ua = jnp.concatenate([u, ur_ref[...]], axis=0) * scale
    gu = ua * row_of(gain_ref)
    gu = gu - jnp.mean(gu, axis=1, keepdims=True)
    gh, gl = two(gu)
    gu_ref[:nk] = gh
    gu_ref[nk:] = gl
    bu = jnp.broadcast_to(jnp.sum(ua * bias, axis=1, keepdims=True), (nk, 128))
    bu_ref[...] = jnp.transpose(jnp.concatenate([bu] * (128 // nk), axis=0))[:1]


def run_query(nh, hd, probe, wq, bq, wk, wv, bv, gain, bias):
    width = probe.shape[0]
    return pl.pallas_call(
        functools.partial(query_body, nh, hd),
        in_specs=[VM] * 8,
        out_specs=[VM] * 5,
        out_shape=[
            jax.ShapeDtypeStruct((4 * nh, width), BF16),
            jax.ShapeDtypeStruct((1, 128), F32),
            jax.ShapeDtypeStruct((1, nh * hd), F32),
            jax.ShapeDtypeStruct((1, nh * hd), F32),
            jax.ShapeDtypeStruct((nh * hd // 4, width), F32),
        ],
        scratch_shapes=[pltpu.VMEM((nh, width), F32), pltpu.VMEM((nh, width), F32), pltpu.SemaphoreType.DMA((2, 1))],
        compiler_params=pltpu.CompilerParams(collective_id=0, has_side_effects=True),
        cost_estimate=pl.CostEstimate(flops=50_000_000, bytes_accessed=6_000_000, transcendentals=0),
        name='query_fold',
    )(probe, wq, bq, wk, wv, bv, gain, bias)


def swap_halves(src, buf, sems, k, tp_peer, core):
    half = src.shape[0] // 2
    rows = pl.ds(pl.multiple_of(core * half, half), half)
    return send(src.at[rows], buf.at[rows], sems, k, tp_peer)


def pass_on(buf, sems, k, sib, core):
    half = buf.shape[0] // 2
    rows = pl.ds(pl.multiple_of(core * half, half), half)
    return send(buf.at[rows], buf.at[rows], sems, k, sib)


def head_body(nh, hd, r_ref, ml_ref, wv_ref, wvh_ref, wo_ref, wup_hbm, wdn_hbm, gain_ref, bu_ref, cb_ref, bo_ref, hg_ref, hb_ref, bup_ref, bdn_ref, og_ref,
              yt_out, gt_t_out, dpre_out, ot_out, da_out, pooled_out, do_out, gt_out, aux_out, rb_out,
              wup, wdn, wall, osd, mls, ora, mra, osd2, mls2, orb, mrb, aps, apr, rs, ra, dys, dyr, mps, mpr, dor, kps, kpr, dg_s, lsem, sems):
    tp_peer, sib, xp, core = places()
    sp = lax.axis_index('sp')
    nk = 2 * nh
    nb = og_ref.shape[0]
    width = og_ref.shape[1]
    load_up = pltpu.make_async_copy(wup_hbm, wup, lsem.at[0])
    load_dn = pltpu.make_async_copy(wdn_hbm, wdn, lsem.at[1])
    load_dn.start()
    load_up.start()
    gain = row_of(gain_ref)
    groups = ml_ref.shape[0]
    for h in range(nh):
        rh = (r_ref[h] * gain).astype(BF16)
        osd[:, h * hd:(h + 1) * hd] = mm(rh, wv_ref[h * hd:(h + 1) * hd, :], NT)
    m0 = jnp.concatenate([ml_ref[g, 0:1] for g in range(groups)], axis=0)
    l0 = jnp.concatenate([ml_ref[g, 1:2] for g in range(groups)], axis=0)
    mls[:groups] = m0
    mls[groups:] = l0
    greet([tp_peer, sib, xp])
    c1 = send(osd, ora, sems, 1, sib)
    c2 = send(mls, mra, sems, 2, sib)
    wall[sp] = wvh_ref[...]
    w1 = send(wvh_ref, wall.at[sp], sems, 0, sib)
    onehot = jnp.where(head_mask(128, nh, hd), 1.0, 0.0).astype(BF16)

    def spread(rows):
        return sum(mm(part, onehot) for part in three(rows))

    def join(oa, ma, la, ob, mb, lb):
        mn = jnp.maximum(ma, mb)
        fa, fb = jnp.exp(ma - mn), jnp.exp(mb - mn)
        o = oa * spread(unpack(fa, nk)) + ob * spread(unpack(fb, nk))
        return o, mn, fa * la + fb * lb

    c1.wait()
    c2.wait()
    o1, m1, l1 = join(osd[...], m0, l0, ora[...], mra[:groups], mra[groups:])
    osd2[...] = o1
    mls2[:groups] = m1
    mls2[groups:] = l1
    c3 = send(osd2, orb, sems, 3, xp)
    c4 = send(mls2, mrb, sems, 4, xp)
    w2 = send(wvh_ref, wall.at[sp], sems, 8, xp)
    load_dn.wait()
    dg_s[...] = mm(og_ref[...], wdn[...], NT)
    c3.wait()
    c4.wait()
    o, m, l = join(o1, m1, l1, orb[...], mrb[:groups], mrb[groups:])
    inv_l = 1.0 / l
    o = o * spread(unpack(inv_l, nk)) + cb_ref[...]
    o_bf = o.astype(BF16)
    ap = mm(o_bf, wo_ref[...])
    aps[...] = ap
    c5 = swap_halves(aps, apr, sems, 5, tp_peer, core)
    wr = unpack(jnp.exp(m0 - m) * inv_l, nk)
    for h in range(nh):
        rs[h] = r_ref[h] * wr[:, h:h + 1]
    nq = nh // 2
    mine = pl.ds(core * nq, nq)
    theirs = pl.ds((1 - core) * nq, nq)
    r1 = send(rs.at[theirs], ra, sems, 6, sib)
    c5.wait()
    c6 = pass_on(apr, sems, 7, sib, core)
    r1.wait()
    rb_out[...] = rs[mine] + ra[...]
    c6.wait()
    a = ap + apr[...] + row_of(bo_ref)
    acen, arstd = row_stats(a)
    ahat = acen * arstd
    hgain = row_of(hg_ref)
    y = (ahat * hgain + row_of(hb_ref)).astype(BF16)
    load_up.wait()
    pre = mm(y, wup[...]) + row_of(bup_ref)
    k0 = 0.7978845608028654
    k1 = 0.044715
    sq = pre * pre
    th = jnp.tanh(k0 * (pre + k1 * (pre * sq)))
    half = 0.5 * (1.0 + th)
    g = (pre * half).astype(BF16)
    dgelu = half + 0.5 * pre * (1.0 - th * th) * (k0 * (1.0 + 3.0 * k1 * sq))
    dpre = (dg_s[...] * dgelu).astype(BF16)
    dpre_out[...] = dpre
    dyp = mm(dpre, wup[...], NT)
    dys[...] = dyp
    c7 = swap_halves(dys, dyr, sems, 9, tp_peer, core)
    mp = mm(g, wdn[...])
    mps[...] = mp
    c8 = swap_halves(mps, mpr, sems, 10, tp_peer, core)
    yt_out[...] = jnp.transpose(y)
    gt_t_out[...] = jnp.transpose(g)
    ot_out[...] = jnp.transpose(o_bf)
    c7.wait()
    c9 = pass_on(dyr, sems, 11, sib, core)
    c9.wait()
    dah = (dyp + dyr[...]) * hgain
    da = arstd * (dah - jnp.mean(dah, axis=1, keepdims=True) - ahat * jnp.mean(dah * ahat, axis=1, keepdims=True))
    da = (og_ref[...].astype(F32) + da).astype(BF16)
    da_out[...] = da
    do_bf = mm(da, wo_ref[...], NT).astype(BF16)
    do = do_bf.astype(F32)
    do_out[...] = do
    kap = sum(mm(part, onehot, NT) for part in two(do * (cb_ref[...] - o)))
    kps[...] = kap
    c10 = swap_halves(do_out, dor, sems, 12, tp_peer, core)
    c11 = send(kps, kpr, sems, 13, tp_peer)

    def back(k, h, d, w):
        t = mm(d, w) * gain
        t = t - jnp.mean(t, axis=1, keepdims=True)
        gt_out[k * nh + h] = t

    for h in range(nh):
        back(0, h, do_bf[:, h * hd:(h + 1) * hd], wv_ref[h * hd:(h + 1) * hd, :])
    c10.wait()
    c12 = pass_on(dor, sems, 14, sib, core)
    w1.wait()
    w2.wait()
    from_x = lax.rem(sp + 2, 4)
    w3 = send(wall.at[from_x], wall.at[from_x], sems, 16, sib)
    c8.wait()
    c13 = pass_on(mpr, sems, 15, sib, core)
    c11.wait()
    kall = kap + pltpu.roll(kpr[...], nh, 1)
    kpk = pack(kall, nk)
    mb = m - bu_ref[...]
    for g_ in range(groups):
        aux_out[g_, 0:1] = mb[g_:g_ + 1]
        aux_out[g_, 1:2] = inv_l[g_:g_ + 1]
        aux_out[g_, 2:3] = kpk[g_:g_ + 1]
    c12.wait()
    dob = dor[...].astype(BF16)
    w3.wait()
    for h in range(nh):
        lo = (h % 2) * hd
        back(1, h, dob[:, h * hd:(h + 1) * hd], wall[h // 2, lo:lo + hd, :].astype(BF16))
    c13.wait()
    pooled_out[...] = (a + mp + mpr[...] + row_of(bdn_ref)).astype(BF16)


def run_head(nh, hd, r_raw, ml, wv, wvh, wo, w_up, w_down, gain, bu, cb, b_out, hgain, hbias, b_up, b_down, out_grad):
    nb, width = out_grad.shape
    ff = w_up.shape[1]
    nd = nh * hd
    groups = ml.shape[0]
    full = pltpu.VMEM((nb, width), F32)
    heads = pltpu.VMEM((nb, nd), F32)
    stat = pltpu.VMEM((2 * groups, 128), F32)
    rhalf = pltpu.VMEM((nh // 2, nb, width), F32)
    return pl.pallas_call(
        functools.partial(head_body, nh, hd),
        in_specs=[VM] * 5 + [ANY] * 2 + [VM] * 9,
        out_specs=[VM] * 10,
        out_shape=[
            jax.ShapeDtypeStruct((width, nb), BF16),
            jax.ShapeDtypeStruct((ff, nb), BF16),
            jax.ShapeDtypeStruct((nb, ff), BF16),
            jax.ShapeDtypeStruct((nd, nb), BF16),
            jax.ShapeDtypeStruct((nb, width), BF16),
            jax.ShapeDtypeStruct((nb, width), BF16),
            jax.ShapeDtypeStruct((nb, nd), F32),
            jax.ShapeDtypeStruct((2 * nh, nb, width), F32),
            jax.ShapeDtypeStruct((groups, 8, 128), F32),
            jax.ShapeDtypeStruct((nh // 2, nb, width), F32),
        ],
        scratch_shapes=[
            pltpu.VMEM(w_up.shape, BF16), pltpu.VMEM(w_down.shape, BF16), pltpu.VMEM((4,) + wvh.shape, F32),
            heads, stat, heads, stat, heads, stat, heads, stat,
            full, full, pltpu.VMEM((nh, nb, width), F32), rhalf,
            full, full, full, full, heads, pltpu.VMEM((nb, 128), F32), pltpu.VMEM((nb, 128), F32),
            pltpu.VMEM((nb, ff), F32),
            pltpu.SemaphoreType.DMA((2,)), pltpu.SemaphoreType.DMA((2, 17)),
        ],
        compiler_params=pltpu.CompilerParams(collective_id=1, has_side_effects=True, vmem_limit_bytes=60 * 1024 * 1024),
        cost_estimate=pl.CostEstimate(flops=3_000_000_000, bytes_accessed=30_000_000, transcendentals=0),
        name='pool_head',
    )(r_raw, ml, wv, wvh, wo, w_up, w_down, gain, bu, cb, b_out, hgain, hbias, b_up, b_down, out_grad)


def tail_body(nh, hd, z_ref, dl_ref, rb_ref, rc_ref, wk_ref, wq_ref, gain_ref, z_out, dq_out, gp_out, rf_out, zs, za, zs2, zb, ps, pr, rd, re, sems):
    tp_peer, sib, xp, core = places()
    nk = 2 * nh
    groups = dl_ref.shape[0]
    width = z_ref.shape[1]
    nq = nh // 2
    mine = pl.ds(core * nq, nq)
    theirs = pl.ds((1 - core) * nq, nq)
    cols = 128
    zs[:nh] = z_ref[...]
    zs[nh:, :cols] = jnp.concatenate([dl_ref[g, 0:1] for g in range(groups)], axis=0)
    greet([tp_peer, sib, xp])
    c1 = send(zs, za, sems, 0, sib)
    rd[...] = rb_ref[...] + rc_ref[...]
    r1 = send(rd, re, sems, 3, sib)
    c1.wait()
    zs2[...] = zs[...] + za[...]
    c2 = send(zs2, zb, sems, 1, xp)
    rf_out[mine] = rd[...]
    r1.wait()
    rf_out[theirs] = re[...]
    c2.wait()
    z = zs2[:nh] + zb[:nh]
    dl = unpack(zs2[nh:, :cols] + zb[nh:, :cols], nk)
    fix = jnp.concatenate([jnp.sum(rf_out[h] * dl[:, h:h + 1], axis=0, keepdims=True) for h in range(nh)], axis=0)
    z = (z - fix) * row_of(gain_ref) * (hd ** -0.5)
    z_out[...] = z
    dqm = mm(z.astype(BF16), wk_ref[...], NT)
    dq = jnp.sum(jnp.where(head_mask(nh, nh, hd), dqm, 0.0), axis=0, keepdims=True)
    dq_out[...] = dq
    gp = mm(jnp.broadcast_to(dq, (8, nh * hd)).astype(BF16), wq_ref[...])
    ps[...] = gp
    c3 = send(ps, pr, sems, 2, tp_peer)
    c3.wait()
    gp_out[...] = (gp[:1] + pr[:1]).reshape(width)


def run_tail(nh, hd, z, dl, rb, rc, wk, wq, gain):
    width = z.shape[1]
    zz = pltpu.VMEM((nh + dl.shape[0], width), F32)
    pp = pltpu.VMEM((8, width), F32)
    return pl.pallas_call(
        functools.partial(tail_body, nh, hd),
        in_specs=[VM] * 7,
        out_specs=[VM] * 4,
        out_shape=[
            jax.ShapeDtypeStruct((nh, width), F32),
            jax.ShapeDtypeStruct((1, nh * hd), F32),
            jax.ShapeDtypeStruct((width,), F32),
            jax.ShapeDtypeStruct((nh,) + rb.shape[1:], F32),
        ],
        scratch_shapes=[zz, zz, zz, zz, pp, pp, pltpu.VMEM(rb.shape, F32), pltpu.VMEM(rb.shape, F32), pltpu.SemaphoreType.DMA((2, 4))],
        compiler_params=pltpu.CompilerParams(collective_id=2, has_side_effects=True),
        cost_estimate=pl.CostEstimate(flops=50_000_000, bytes_accessed=6_000_000, transcendentals=0),
        name='query_back',
    )(z, dl, rb, rc, wk, wq, gain)


def local_head(encoded, enc_gain, enc_bias, probe, w_query, b_query, w_key, w_value, b_value, w_out, b_out, head_gain, head_bias, w_up, b_up, w_down, b_down, out_grad):
    nh, hd = b_query.shape
    width = probe.shape[0]
    nd = nh * hd

    def flat(w):
        return jnp.transpose(w, (1, 2, 0)).reshape(nd, width)

    def heads(g):
        return jnp.transpose(g.reshape(nh, hd, width), (2, 0, 1))

    wq, wk, wv, wo = flat(w_query), flat(w_key), flat(w_value), w_out.reshape(nd, width)
    gu2, bu, q, cb, wvq = run_query(nh, hd, probe, wq, b_query, wk, wv, b_value, enc_gain, enc_bias)
    wvq = lax.ppermute(wvq, 'tp', [(0, 1), (1, 0)])
    xh, sx, rs, r_raw, ml = run_fwd(encoded, gu2, bu)
    yt, ht, dpre, ot, da, pooled, do, gt, aux, rb = run_head(nh, hd, r_raw, ml, wv, wvq, wo, w_up, w_down, enc_gain, bu, cb, b_out, head_gain, head_bias, b_up, b_down, out_grad)
    rc = lax.ppermute(rb, 'sp', [(i, (i + 2) % 4) for i in range(4)])
    grad_encoded, z, dl, grad_w_up, grad_w_down, grad_w_out = run_bwd(xh, sx, rs, gt, gu2, aux, yt, dpre, ht, out_grad, ot, da)
    z, dq, grad_probe, rf = run_tail(nh, hd, z, dl, rb, rc, wk, wq, enc_gain)
    r_bf = (rf * enc_gain + enc_bias).astype(BF16)
    do3 = do.astype(BF16).reshape(-1, nh, hd)
    grad_w_value = heads(dot('bhd,hbw->hdw', do3, r_bf))
    grad_w_key = heads(q.reshape(nh, hd, 1) * z[:, None, :])
    grad_w_query = heads(dq.reshape(nd, 1) * probe[None])
    return (pooled, grad_encoded, grad_probe, grad_w_query, grad_w_key, grad_w_value, grad_w_out.reshape(nh, hd, width), grad_w_up, grad_w_down)


def solution(mesh):
    return jax.shard_map(local_head, mesh=mesh, in_specs=IN_SPECS, out_specs=OUT_SPECS, check_vma=False)
```

```python
import functools
import jax
import jax.numpy as jnp
from jax import lax
from jax.experimental import pallas as pl
from jax.experimental.pallas import tpu as pltpu
from jax.sharding import PartitionSpec as P

NORM_EPS = 1e-6
F32 = jnp.float32
BF16 = jnp.bfloat16
IN_SPECS = (P('dp', 'sp', None), P(), P(), P(), P(None, 'tp', None), P('tp', None), P(None, 'tp', None), P(None, 'tp', None), P('tp', None), P('tp', None, None), P(), P(), P(), P(None, 'tp'), P('tp'), P('tp', None), P(), P('dp', None))
OUT_SPECS = (P('dp', None), P('dp', 'sp', None), P('dp'), P('dp', 'tp', None), P('dp', 'tp', None), P('dp', 'tp', None), P(('dp', 'tp'), None, None), P('dp', 'tp'), P(('dp', 'tp'), None))
NN = (((1,), (0,)), ((), ()))
NT = (((1,), (1,)), ((), ()))
TN = (((0,), (0,)), ((), ()))


def mm(a, b, dims=NN):
    return lax.dot_general(a, b, dims, preferred_element_type=F32)


def dot(spec, a, b):
    return jnp.einsum(spec, a, b, preferred_element_type=F32)


def row_stats(xs):
    mean = jnp.mean(xs, axis=-1, keepdims=True)
    cen = xs - mean
    return cen, lax.rsqrt(jnp.mean(cen * cen, axis=-1, keepdims=True) + NORM_EPS)


def fwd_body(nk, x_ref, gu_ref, bu_ref, xh_ref, sx_ref, rs_ref, r_ref, ml_ref, st_ref):
    images, tokens, width = x_ref.shape
    nh = nk // 2
    eye = lax.broadcasted_iota(jnp.int32, (tokens, tokens), 0) == lax.broadcasted_iota(jnp.int32, (tokens, tokens), 1)
    ones = jnp.ones((16, width), BF16)
    worst = jnp.full((tokens, 1), -1.0, F32)
    for i in range(images):
        xb = x_ref[i]
        mean = mm(xb, ones, NT)[:, :1] * (1.0 / width)
        square = jnp.sum(jnp.where(eye, mm(xb, xb, NT), 0.0), axis=1, keepdims=True) * (1.0 / width)
        var = square - mean * mean
        worst = jnp.maximum(worst, mean * mean - 256.0 * var)
        st_ref[0, i] = jnp.broadcast_to(mean, (tokens, 128))
        st_ref[1, i] = jnp.broadcast_to(lax.rsqrt(jnp.maximum(var, 0.0) + NORM_EPS), (tokens, 128))

    @pl.when(jnp.max(worst) > 0.0)
    def _():
        for i in range(images):
            def redo(j, carry, i=i):
                rows = pl.ds(pl.multiple_of(j * 16, 16), 16)
                xs = x_ref[i, rows, :].astype(F32)
                st_ref[0, i, rows, :] = jnp.broadcast_to(jnp.mean(xs, axis=-1, keepdims=True), (16, 128))
                st_ref[1, i, rows, :] = jnp.broadcast_to(row_stats(xs)[1], (16, 128))
                return carry
            lax.fori_loop(0, tokens // 16, redo, 0)

    for i in range(images):
        rstd = st_ref[1, i, :, :1]
        xh_ref[i] = ((x_ref[i].astype(F32) - st_ref[0, i, :, :1]) * rstd).astype(BF16)
        rs_ref[0, :, i * nk:(i + 1) * nk] = st_ref[1, i, :, :nk]
    parts = []
    for i in range(images):
        s2 = mm(xh_ref[i], gu_ref[...], NT)
        parts.append(s2[:, :nk] + s2[:, nk:])
    sx = jnp.concatenate(parts, axis=1)
    sx_ref[0] = sx
    s = sx + bu_ref[...]
    m = jnp.max(s, axis=0, keepdims=True)
    e = jnp.exp(s - m)
    l = jnp.sum(e, axis=0, keepdims=True)
    row = lax.broadcasted_iota(jnp.int32, (8, m.shape[1]), 0)
    ml_ref[0] = jnp.where(row == 0, m, l)
    et = jnp.transpose(e.astype(BF16))
    for i in range(images):
        r_ref[:, i, :] = mm(et[i * nk:i * nk + nh], xh_ref[i])


def run_fwd(x, gu2, bu):
    nb, tokens, width = x.shape
    nk = gu2.shape[0] // 2
    bi = 128 // nk
    ng = nb // bi
    return pl.pallas_call(
        functools.partial(fwd_body, nk),
        grid=(ng,),
        in_specs=[
            pl.BlockSpec((bi, tokens, width), lambda i: (i, 0, 0)),
            pl.BlockSpec(gu2.shape, lambda i: (0, 0)),
            pl.BlockSpec(bu.shape, lambda i: (0, 0)),
        ],
        out_specs=[
            pl.BlockSpec((bi, tokens, width), lambda i: (i, 0, 0)),
            pl.BlockSpec((1, tokens, 128), lambda i: (i, 0, 0)),
            pl.BlockSpec((1, tokens, 128), lambda i: (i, 0, 0)),
            pl.BlockSpec((nk // 2, bi, width), lambda i: (0, i, 0)),
            pl.BlockSpec((1, 8, 128), lambda i: (i, 0, 0)),
        ],
        out_shape=[
            jax.ShapeDtypeStruct((nb, tokens, width), BF16),
            jax.ShapeDtypeStruct((ng, tokens, 128), F32),
            jax.ShapeDtypeStruct((ng, tokens, 128), F32),
            jax.ShapeDtypeStruct((nk // 2, nb, width), F32),
            jax.ShapeDtypeStruct((ng, 8, 128), F32),
        ],
        scratch_shapes=[pltpu.VMEM((2, bi, tokens, 128), F32)],
        cost_estimate=pl.CostEstimate(flops=8_000_000_000, bytes_accessed=40_000_000, transcendentals=0),
        name='fwd_tokens',
    )(x, gu2, bu)


def bwd_body(nk, xh_ref, sx_ref, rs_ref, gt_ref, gu_ref, aux_ref, yt_ref, dpre_ref, ht_ref, og_ref, ot_ref, da_ref, dx_ref, z_ref, dl_ref, gup_ref, gdn_ref, gwo_ref, zacc_ref):
    step = pl.program_id(0)
    images, tokens, width = xh_ref.shape
    nh = nk // 2

    @pl.when(step == 0)
    def _():
        zacc_ref[...] = jnp.zeros_like(zacc_ref)

    gup_ref[...] = mm(yt_ref[...], dpre_ref[...])
    gdn_ref[...] = mm(ht_ref[...], og_ref[...])
    gwo_ref[...] = mm(ot_ref[...], da_ref[...])
    sx = sx_ref[0]
    rstd = rs_ref[0]
    gts = [gt_ref[:, i, :].astype(BF16) for i in range(images)]
    dpx = jnp.concatenate([mm(xh_ref[i], gts[i], NT) for i in range(images)], axis=1)
    p = jnp.exp(sx - aux_ref[0, 0:1]) * aux_ref[0, 1:2]
    ds = p * (dpx + aux_ref[0, 2:3])
    dl_ref[0] = jnp.broadcast_to(jnp.sum(ds, axis=0, keepdims=True), dl_ref.shape[1:])
    prod = (ds * sx + p * dpx) * rstd * (1.0 / width)
    ph = prod.astype(BF16)
    po = (prod - ph.astype(F32)).astype(BF16)
    g0 = lax.broadcasted_iota(jnp.int32, (128, 128), 0) // nk
    g1 = lax.broadcasted_iota(jnp.int32, (128, 128), 1) // nk
    ind = jnp.where(g0 == g1, 1.0, 0.0).astype(BF16)
    c2 = mm(ph, ind) + mm(po, ind)
    dst = jnp.transpose(ds.astype(BF16))
    ca = (ds * rstd).astype(BF16)
    cb = (p * rstd).astype(BF16)
    z = zacc_ref[...]
    for i in range(images):
        xh = xh_ref[i]
        z = z + mm(dst[i * nk:i * nk + nh], xh)
        coef = jnp.concatenate([ca[:, i * nk:(i + 1) * nk], cb[:, i * nk:(i + 1) * nk]], axis=1)
        dxh = mm(coef, jnp.concatenate([gu_ref[...], gts[i]], axis=0))
        dx_ref[i] = (dxh - c2[:, i * nk:i * nk + 1] * xh.astype(F32)).astype(BF16)
    zacc_ref[...] = z
    z_ref[...] = z


def run_bwd(xh, sx, rs, gt, gu2, aux, yt, dpre, ht, out_grad, ot, da):
    nb, tokens, width = xh.shape
    nk = gu2.shape[0] // 2
    bi = 128 // nk
    ng = nb // bi
    ff, nd = ht.shape[0], ot.shape[0]
    return pl.pallas_call(
        functools.partial(bwd_body, nk),
        grid=(ng,),
        in_specs=[
            pl.BlockSpec((bi, tokens, width), lambda i: (i, 0, 0)),
            pl.BlockSpec((1, tokens, 128), lambda i: (i, 0, 0)),
            pl.BlockSpec((1, tokens, 128), lambda i: (i, 0, 0)),
            pl.BlockSpec((nk, bi, width), lambda i: (0, i, 0)),
            pl.BlockSpec((nk, width), lambda i: (0, 0)),
            pl.BlockSpec((1, 8, 128), lambda i: (i, 0, 0)),
            pl.BlockSpec((width // ng, nb), lambda i: (i, 0)),
            pl.BlockSpec((nb, ff), lambda i: (0, 0)),
            pl.BlockSpec((ff // ng, nb), lambda i: (i, 0)),
            pl.BlockSpec((nb, width), lambda i: (0, 0)),
            pl.BlockSpec((nd // ng, nb), lambda i: (i, 0)),
            pl.BlockSpec((nb, width), lambda i: (0, 0)),
        ],
        out_specs=[
            pl.BlockSpec((bi, tokens, width), lambda i: (i, 0, 0)),
            pl.BlockSpec((nk // 2, width), lambda i: (0, 0)),
            pl.BlockSpec((1, 8, 128), lambda i: (i, 0, 0)),
            pl.BlockSpec((width // ng, ff), lambda i: (i, 0)),
            pl.BlockSpec((ff // ng, width), lambda i: (i, 0)),
            pl.BlockSpec((nd // ng, width), lambda i: (i, 0)),
        ],
        out_shape=[
            jax.ShapeDtypeStruct((nb, tokens, width), BF16),
            jax.ShapeDtypeStruct((nk // 2, width), F32),
            jax.ShapeDtypeStruct((ng, 8, 128), F32),
            jax.ShapeDtypeStruct((width, ff), F32),
            jax.ShapeDtypeStruct((ff, width), F32),
            jax.ShapeDtypeStruct((nd, width), F32),
        ],
        scratch_shapes=[pltpu.VMEM((nk // 2, width), F32)],
        cost_estimate=pl.CostEstimate(flops=12_000_000_000, bytes_accessed=40_000_000, transcendentals=0),
        name='bwd_tokens',
    )(xh, sx, rs, gt, gu2, aux, yt, dpre, ht, out_grad, ot, da)


MESH = pl.DeviceIdType.MESH
VM = pl.BlockSpec(memory_space=pltpu.VMEM)
ANY = pl.BlockSpec(memory_space=pl.ANY)


def send(src, dst, sems, k, where):
    copy = pltpu.make_async_remote_copy(src_ref=src, dst_ref=dst, send_sem=sems.at[0, k], recv_sem=sems.at[1, k], device_id=where, device_id_type=MESH)
    copy.start()
    return copy


def greet(places):
    barrier = pltpu.get_barrier_semaphore()
    for where in places:
        pl.semaphore_signal(barrier, inc=1, device_id=where, device_id_type=MESH)
    pl.semaphore_wait(barrier, len(places))


def places():
    tp = lax.axis_index('tp')
    sp = lax.axis_index('sp')
    core = lax.rem(sp, 2)
    return {'tp': 1 - tp}, {'sp': sp + 1 - 2 * core}, {'sp': lax.rem(sp + 2, 4)}, core


def two(a):
    hi = a.astype(BF16)
    return hi, (a - hi.astype(F32)).astype(BF16)


def three(a):
    hi, rest = a.astype(BF16), a
    rest = rest - hi.astype(F32)
    mid = rest.astype(BF16)
    return hi, mid, (rest - mid.astype(F32)).astype(BF16)


def head_mask(rows, nh, hd):
    lane = lax.broadcasted_iota(jnp.int32, (rows, nh * hd), 1)
    row = lax.broadcasted_iota(jnp.int32, (rows, nh * hd), 0)
    return jnp.logical_and(lane >= row * hd, lane < (row + 1) * hd)


def unpack(packed, nk):
    groups, lanes = packed.shape
    per = lanes // nk
    rows = jnp.concatenate([jnp.broadcast_to(packed[g:g + 1], (per, lanes)) for g in range(groups)], axis=0)
    keep = own_lanes(rows.shape, nk, per)
    rows = jnp.where(keep, rows, 0.0)
    shift = nk
    while shift < lanes:
        rows = rows + pltpu.roll(rows, shift, 1)
        shift *= 2
    return rows


def own_lanes(shape, nk, per):
    lane = lax.broadcasted_iota(jnp.int32, shape, 1)
    row = lax.rem(lax.broadcasted_iota(jnp.int32, shape, 0), per)
    return jnp.logical_and(lane >= row * nk, lane < (row + 1) * nk)


def pack(rows, nk):
    images, lanes = rows.shape
    per = lanes // nk
    shift = nk
    while shift < lanes:
        rows = rows + pltpu.roll(rows, shift, 1)
        shift *= 2
    rows = jnp.where(own_lanes(rows.shape, nk, per), rows, 0.0)
    return jnp.concatenate([jnp.sum(rows[g * per:(g + 1) * per], axis=0, keepdims=True) for g in range(images // per)], axis=0)


def row_of(ref):
    return ref[...].reshape(1, ref.shape[0])


def flat_heads(ref):
    return jnp.concatenate([ref[h:h + 1, :] for h in range(ref.shape[0])], axis=1)


def query_body(nh, hd, probe_ref, wq_ref, bq_ref, wk_ref, wv_ref, bv_ref, gain_ref, bias_ref, gu_ref, bu_ref, q_ref, cb_ref, wvq_ref, us_ref, ur_ref, sems):
    tp_peer, _, _, _ = places()
    greet([tp_peer])
    width = probe_ref.shape[0]
    nk = 2 * nh
    q = (mm(jnp.broadcast_to(row_of(probe_ref), (8, width)).astype(BF16), wq_ref[...], NT)[:1] + flat_heads(bq_ref)).astype(BF16)
    qd = jnp.where(head_mask(nh, nh, hd), jnp.broadcast_to(q.astype(F32), (nh, nh * hd)), 0.0).astype(BF16)
    qf = qd.astype(F32)
    q_ref[...] = jnp.transpose(jnp.concatenate([qf, qf, qf, jnp.zeros_like(qf)], axis=0)).astype(BF16)
    u = mm(qd, wk_ref[...])
    us_ref[...] = u
    copy = send(us_ref, ur_ref, sems, 0, tp_peer)
    bias = row_of(bias_ref)
    bh, bl = two(bias)
    row = lax.broadcasted_iota(jnp.int32, (8, width), 0)
    b2 = jnp.where(row == 0, bh.astype(F32), jnp.where(row == 1, bl.astype(F32), 0.0)).astype(BF16)
    cb_ref[...] = jnp.sum(mm(b2, wv_ref[...], NT), axis=0, keepdims=True) + flat_heads(bv_ref)
    quarter = wvq_ref.shape[0]
    wvq_ref[...] = wv_ref[pl.ds(pl.multiple_of(lax.axis_index('sp') * quarter, quarter), quarter), :].astype(F32)
    copy.wait()
    scale = hd ** -0.5
    ua = jnp.concatenate([u, ur_ref[...]], axis=0) * scale
    gu = ua * row_of(gain_ref)
    gu = gu - jnp.mean(gu, axis=1, keepdims=True)
    gh, gl = two(gu)
    gu_ref[:nk] = gh
    gu_ref[nk:] = gl
    bu = jnp.broadcast_to(jnp.sum(ua * bias, axis=1, keepdims=True), (nk, 128))
    bu_ref[...] = jnp.transpose(jnp.concatenate([bu] * (128 // nk), axis=0))[:1]


def run_query(nh, hd, probe, wq, bq, wk, wv, bv, gain, bias):
    width = probe.shape[0]
    return pl.pallas_call(
        functools.partial(query_body, nh, hd),
        in_specs=[VM] * 8,
        out_specs=[VM] * 5,
        out_shape=[
            jax.ShapeDtypeStruct((4 * nh, width), BF16),
            jax.ShapeDtypeStruct((1, 128), F32),
            jax.ShapeDtypeStruct((nh * hd, 4 * nh), BF16),
            jax.ShapeDtypeStruct((1, nh * hd), F32),
            jax.ShapeDtypeStruct((nh * hd // 4, width), F32),
        ],
        scratch_shapes=[pltpu.VMEM((nh, width), F32), pltpu.VMEM((nh, width), F32), pltpu.SemaphoreType.DMA((2, 1))],
        compiler_params=pltpu.CompilerParams(collective_id=0, has_side_effects=True),
        cost_estimate=pl.CostEstimate(flops=50_000_000, bytes_accessed=6_000_000, transcendentals=0),
        name='query_fold',
    )(probe, wq, bq, wk, wv, bv, gain, bias)


def swap_halves(src, buf, sems, k, tp_peer, core):
    half = src.shape[0] // 2
    rows = pl.ds(pl.multiple_of(core * half, half), half)
    return send(src.at[rows], buf.at[rows], sems, k, tp_peer)


def pass_on(buf, sems, k, sib, core):
    half = buf.shape[0] // 2
    rows = pl.ds(pl.multiple_of(core * half, half), half)
    return send(buf.at[rows], buf.at[rows], sems, k, sib)


def head_body(nh, hd, r_ref, ml_ref, wv_ref, wvh_ref, wo_ref, wup_hbm, wdn_hbm, gain_ref, bu_ref, cb_ref, bo_ref, hg_ref, hb_ref, bup_ref, bdn_ref, og_ref,
              yt_out, gt_t_out, dpre_out, ot_out, da_out, pooled_out, dot_out, gt_out, aux_out, rb_out,
              wup, wdn, wall, osd, mls, ora, mra, osd2, mls2, orb, mrb, aps, apr, rs, ra, dys, dyr, mps, mpr, dos, dor, kps, kpr, dg_s, lsem, sems):
    tp_peer, sib, xp, core = places()
    sp = lax.axis_index('sp')
    nk = 2 * nh
    nb = og_ref.shape[0]
    width = og_ref.shape[1]
    load_up = pltpu.make_async_copy(wup_hbm, wup, lsem.at[0])
    load_dn = pltpu.make_async_copy(wdn_hbm, wdn, lsem.at[1])
    load_dn.start()
    load_up.start()
    gain = row_of(gain_ref)
    groups = ml_ref.shape[0]
    for h in range(nh):
        rh = (r_ref[h] * gain).astype(BF16)
        osd[:, h * hd:(h + 1) * hd] = mm(rh, wv_ref[h * hd:(h + 1) * hd, :], NT)
    m0 = jnp.concatenate([ml_ref[g, 0:1] for g in range(groups)], axis=0)
    l0 = jnp.concatenate([ml_ref[g, 1:2] for g in range(groups)], axis=0)
    mls[:groups] = m0
    mls[groups:] = l0
    greet([tp_peer, sib, xp])
    c1 = send(osd, ora, sems, 1, sib)
    c2 = send(mls, mra, sems, 2, sib)
    wall[sp] = wvh_ref[...]
    w1 = send(wvh_ref, wall.at[sp], sems, 0, sib)
    onehot = jnp.where(head_mask(128, nh, hd), 1.0, 0.0).astype(BF16)

    def spread(rows):
        return sum(mm(part, onehot) for part in three(rows))

    def join(oa, ma, la, ob, mb, lb):
        mn = jnp.maximum(ma, mb)
        fa, fb = jnp.exp(ma - mn), jnp.exp(mb - mn)
        o = oa * spread(unpack(fa, nk)) + ob * spread(unpack(fb, nk))
        return o, mn, fa * la + fb * lb

    c1.wait()
    c2.wait()
    o1, m1, l1 = join(osd[...], m0, l0, ora[...], mra[:groups], mra[groups:])
    osd2[...] = o1
    mls2[:groups] = m1
    mls2[groups:] = l1
    c3 = send(osd2, orb, sems, 3, xp)
    c4 = send(mls2, mrb, sems, 4, xp)
    w2 = send(wvh_ref, wall.at[sp], sems, 8, xp)
    load_dn.wait()
    dg_s[...] = mm(og_ref[...], wdn[...], NT)
    c3.wait()
    c4.wait()
    o, m, l = join(o1, m1, l1, orb[...], mrb[:groups], mrb[groups:])
    inv_l = 1.0 / l
    o = o * spread(unpack(inv_l, nk)) + cb_ref[...]
    o_bf = o.astype(BF16)
    ap = mm(o_bf, wo_ref[...])
    aps[...] = ap
    c5 = swap_halves(aps, apr, sems, 5, tp_peer, core)
    wr = unpack(jnp.exp(m0 - m) * inv_l, nk)
    for h in range(nh):
        rs[h] = r_ref[h] * wr[:, h:h + 1]
    nq = nh // 2
    mine = pl.ds(core * nq, nq)
    theirs = pl.ds((1 - core) * nq, nq)
    r1 = send(rs.at[theirs], ra, sems, 6, sib)
    c5.wait()
    c6 = pass_on(apr, sems, 7, sib, core)
    r1.wait()
    rb_out[...] = rs[mine] + ra[...]
    c6.wait()
    a = ap + apr[...] + row_of(bo_ref)
    acen, arstd = row_stats(a)
    ahat = acen * arstd
    hgain = row_of(hg_ref)
    y = (ahat * hgain + row_of(hb_ref)).astype(BF16)
    load_up.wait()
    pre = mm(y, wup[...]) + row_of(bup_ref)
    k0 = 0.7978845608028654
    k1 = 0.044715
    sq = pre * pre
    th = jnp.tanh(k0 * (pre + k1 * (pre * sq)))
    half = 0.5 * (1.0 + th)
    g = (pre * half).astype(BF16)
    dgelu = half + 0.5 * pre * (1.0 - th * th) * (k0 * (1.0 + 3.0 * k1 * sq))
    dpre = (dg_s[...] * dgelu).astype(BF16)
    dpre_out[...] = dpre
    dyp = mm(dpre, wup[...], NT)
    dys[...] = dyp
    c7 = swap_halves(dys, dyr, sems, 9, tp_peer, core)
    mp = mm(g, wdn[...])
    mps[...] = mp
    c8 = swap_halves(mps, mpr, sems, 10, tp_peer, core)
    yt_out[...] = jnp.transpose(y)
    gt_t_out[...] = jnp.transpose(g)
    ot_out[...] = jnp.transpose(o_bf)
    c7.wait()
    c9 = pass_on(dyr, sems, 11, sib, core)
    c9.wait()
    dah = (dyp + dyr[...]) * hgain
    da = arstd * (dah - jnp.mean(dah, axis=1, keepdims=True) - ahat * jnp.mean(dah * ahat, axis=1, keepdims=True))
    da = (og_ref[...].astype(F32) + da).astype(BF16)
    da_out[...] = da
    do_bf = mm(da, wo_ref[...], NT).astype(BF16)
    do = do_bf.astype(F32)
    dos[...] = do
    kap = sum(mm(part, onehot, NT) for part in two(do * (cb_ref[...] - o)))
    kps[...] = kap
    c10 = swap_halves(dos, dor, sems, 12, tp_peer, core)
    c11 = send(kps, kpr, sems, 13, tp_peer)

    def back(k, h, d, w):
        t = mm(d, w) * gain
        t = t - jnp.mean(t, axis=1, keepdims=True)
        gt_out[k * nh + h] = t

    dot_out[...] = jnp.transpose(do_bf)
    for h in range(nh):
        back(0, h, do_bf[:, h * hd:(h + 1) * hd], wv_ref[h * hd:(h + 1) * hd, :])
    c10.wait()
    c12 = pass_on(dor, sems, 14, sib, core)
    w1.wait()
    w2.wait()
    from_x = lax.rem(sp + 2, 4)
    w3 = send(wall.at[from_x], wall.at[from_x], sems, 16, sib)
    c8.wait()
    c13 = pass_on(mpr, sems, 15, sib, core)
    c11.wait()
    kall = kap + pltpu.roll(kpr[...], nh, 1)
    kpk = pack(kall, nk)
    mb = m - bu_ref[...]
    for g_ in range(groups):
        aux_out[g_, 0:1] = mb[g_:g_ + 1]
        aux_out[g_, 1:2] = inv_l[g_:g_ + 1]
        aux_out[g_, 2:3] = kpk[g_:g_ + 1]
    c12.wait()
    dob = dor[...].astype(BF16)
    w3.wait()
    for h in range(nh):
        lo = (h % 2) * hd
        back(1, h, dob[:, h * hd:(h + 1) * hd], wall[h // 2, lo:lo + hd, :].astype(BF16))
    c13.wait()
    pooled_out[...] = (a + mp + mpr[...] + row_of(bdn_ref)).astype(BF16)


def run_head(nh, hd, r_raw, ml, wv, wvh, wo, w_up, w_down, gain, bu, cb, b_out, hgain, hbias, b_up, b_down, out_grad):
    nb, width = out_grad.shape
    ff = w_up.shape[1]
    nd = nh * hd
    groups = ml.shape[0]
    full = pltpu.VMEM((nb, width), F32)
    heads = pltpu.VMEM((nb, nd), F32)
    stat = pltpu.VMEM((2 * groups, 128), F32)
    rhalf = pltpu.VMEM((nh // 2, nb, width), F32)
    return pl.pallas_call(
        functools.partial(head_body, nh, hd),
        in_specs=[VM] * 5 + [ANY] * 2 + [VM] * 9,
        out_specs=[VM] * 10,
        out_shape=[
            jax.ShapeDtypeStruct((width, nb), BF16),
            jax.ShapeDtypeStruct((ff, nb), BF16),
            jax.ShapeDtypeStruct((nb, ff), BF16),
            jax.ShapeDtypeStruct((nd, nb), BF16),
            jax.ShapeDtypeStruct((nb, width), BF16),
            jax.ShapeDtypeStruct((nb, width), BF16),
            jax.ShapeDtypeStruct((nd, nb), BF16),
            jax.ShapeDtypeStruct((2 * nh, nb, width), F32),
            jax.ShapeDtypeStruct((groups, 8, 128), F32),
            jax.ShapeDtypeStruct((nh // 2, nb, width), F32),
        ],
        scratch_shapes=[
            pltpu.VMEM(w_up.shape, BF16), pltpu.VMEM(w_down.shape, BF16), pltpu.VMEM((4,) + wvh.shape, F32),
            heads, stat, heads, stat, heads, stat, heads, stat,
            full, full, pltpu.VMEM((nh, nb, width), F32), rhalf,
            full, full, full, full, heads, heads, pltpu.VMEM((nb, 128), F32), pltpu.VMEM((nb, 128), F32),
            pltpu.VMEM((nb, ff), F32),
            pltpu.SemaphoreType.DMA((2,)), pltpu.SemaphoreType.DMA((2, 17)),
        ],
        compiler_params=pltpu.CompilerParams(collective_id=1, has_side_effects=True, vmem_limit_bytes=60 * 1024 * 1024),
        cost_estimate=pl.CostEstimate(flops=3_000_000_000, bytes_accessed=30_000_000, transcendentals=0),
        name='pool_head',
    )(r_raw, ml, wv, wvh, wo, w_up, w_down, gain, bu, cb, b_out, hgain, hbias, b_up, b_down, out_grad)


def tail_body(nh, hd, z_ref, dl_ref, rb_ref, rc_ref, wk_hbm, wq_hbm, gain_ref, probe_ref, z_out, dq_out, pm_out, gp_out, rf_out, zs, za, zs2, zb, ds, da, ds2, db, ps, pr, rd, re, wk, wq, lsem, sems):
    tp_peer, sib, xp, core = places()
    nk = 2 * nh
    groups = dl_ref.shape[0]
    width = z_ref.shape[1]
    nq = nh // 2
    mine = pl.ds(core * nq, nq)
    theirs = pl.ds((1 - core) * nq, nq)
    load_k = pltpu.make_async_copy(wk_hbm, wk, lsem.at[0])
    load_q = pltpu.make_async_copy(wq_hbm, wq, lsem.at[1])
    load_k.start()
    load_q.start()
    ds[...] = jnp.concatenate([dl_ref[g, 0:1] for g in range(groups)], axis=0)
    zs[...] = z_ref[...]
    greet([tp_peer, sib, xp])
    c1 = send(zs, za, sems, 0, sib)
    d1 = send(ds, da, sems, 1, sib)
    rd[...] = rb_ref[...] + rc_ref[...]
    r1 = send(rd, re, sems, 2, sib)
    c1.wait()
    d1.wait()
    zs2[...] = zs[...] + za[...]
    ds2[...] = ds[...] + da[...]
    c2 = send(zs2, zb, sems, 3, xp)
    d2 = send(ds2, db, sems, 4, xp)
    rf_out[mine] = rd[...]
    p1, p2, p3 = three(row_of(probe_ref))
    pm_out[...] = jnp.concatenate([p1, p2, p1, p3, p2, p1, jnp.zeros((2, width), BF16)], axis=0)
    r1.wait()
    rf_out[theirs] = re[...]
    load_k.wait()
    load_q.wait()
    c2.wait()
    d2.wait()
    dl = unpack(ds2[...] + db[...], nk)
    fix = jnp.concatenate([jnp.sum(rf_out[h] * dl[:, h:h + 1], axis=0, keepdims=True) for h in range(nh)], axis=0)
    z = (zs2[...] + zb[...] - fix) * row_of(gain_ref) * (hd ** -0.5)
    dqm = mm(z.astype(BF16), wk[...], NT)
    dq = jnp.sum(jnp.where(head_mask(nh, nh, hd), dqm, 0.0), axis=0, keepdims=True)
    gp = mm(jnp.broadcast_to(dq, (8, nh * hd)).astype(BF16), wq[...])[:1]
    ps[...] = gp
    c3 = send(ps, pr, sems, 5, tp_peer)
    z_out[...] = jnp.concatenate(list(three(z)) + [jnp.zeros((nh, width), BF16)], axis=0)
    d1_, d2_, d3_ = (part.astype(F32) for part in three(dq))
    zero = jnp.zeros_like(dq)
    dq_out[...] = jnp.transpose(jnp.concatenate([d1_, d1_, d2_, d1_, d2_, d3_, zero, zero], axis=0)).astype(BF16)
    c3.wait()
    gp_out[...] = (gp + pr[...]).reshape(width)


def run_tail(nh, hd, z, dl, rb, rc, wk, wq, gain, probe):
    width = z.shape[1]
    nd = nh * hd
    zz = pltpu.VMEM((nh, width), F32)
    dd = pltpu.VMEM((dl.shape[0], 128), F32)
    pp = pltpu.VMEM((1, width), F32)
    return pl.pallas_call(
        functools.partial(tail_body, nh, hd),
        in_specs=[VM] * 4 + [ANY] * 2 + [VM] * 2,
        out_specs=[VM] * 5,
        out_shape=[
            jax.ShapeDtypeStruct((4 * nh, width), BF16),
            jax.ShapeDtypeStruct((nd, 8), BF16),
            jax.ShapeDtypeStruct((8, width), BF16),
            jax.ShapeDtypeStruct((width,), F32),
            jax.ShapeDtypeStruct((nh,) + rb.shape[1:], F32),
        ],
        scratch_shapes=[zz, zz, zz, zz, dd, dd, dd, dd, pp, pp, pltpu.VMEM(rb.shape, F32), pltpu.VMEM(rb.shape, F32), pltpu.VMEM(wk.shape, BF16), pltpu.VMEM(wq.shape, BF16), pltpu.SemaphoreType.DMA((2,)), pltpu.SemaphoreType.DMA((2, 6))],
        compiler_params=pltpu.CompilerParams(collective_id=2, has_side_effects=True),
        cost_estimate=pl.CostEstimate(flops=50_000_000, bytes_accessed=6_000_000, transcendentals=0),
        name='query_back',
    )(z, dl, rb, rc, wk, wq, gain, probe)


def outer_body(hd, qt_ref, z_ref, dqt_ref, pm_ref, dot_ref, rf_ref, gain_ref, bias_ref, pooled_ref, gp_ref, gwk_ref, gwq_ref, gwv_ref, pooled_out, gp_out):
    gwk_ref[...] = mm(qt_ref[...], z_ref[...])
    gwq_ref[...] = mm(dqt_ref[...], pm_ref[...])
    gain, bias = row_of(gain_ref), row_of(bias_ref)
    for h in range(rf_ref.shape[0]):
        r = (rf_ref[h] * gain + bias).astype(BF16)
        gwv_ref[h * hd:(h + 1) * hd, :] = mm(dot_ref[h * hd:(h + 1) * hd, :], r)
    pooled_out[...] = pooled_ref[...]
    gp_out[...] = gp_ref[...]


def run_outer(nh, hd, qt, z, dqt, pm, dot, rf, gain, bias, pooled, gp):
    nb, width = pooled.shape
    per = 2
    rows = per * hd
    blk = lambda a: pl.BlockSpec((rows, a.shape[1]), lambda i: (i, 0))
    whole = lambda a: pl.BlockSpec(a.shape, lambda i: (0,) * a.ndim)
    big = jax.ShapeDtypeStruct((nh * hd, width), F32)
    return pl.pallas_call(
        functools.partial(outer_body, hd),
        grid=(nh // per,),
        in_specs=[blk(qt), whole(z), blk(dqt), whole(pm), blk(dot), pl.BlockSpec((per, nb, width), lambda i: (i, 0, 0)), whole(gain), whole(bias), whole(pooled), whole(gp)],
        out_specs=[blk(big), blk(big), blk(big), whole(pooled), whole(gp)],
        out_shape=[big, big, big, jax.ShapeDtypeStruct(pooled.shape, BF16), jax.ShapeDtypeStruct(gp.shape, F32)],
        cost_estimate=pl.CostEstimate(flops=300_000_000, bytes_accessed=14_000_000, transcendentals=0),
        name='outer_grads',
    )(qt, z, dqt, pm, dot, rf, gain, bias, pooled, gp)


def local_head(encoded, enc_gain, enc_bias, probe, w_query, b_query, w_key, w_value, b_value, w_out, b_out, head_gain, head_bias, w_up, b_up, w_down, b_down, out_grad):
    nh, hd = b_query.shape
    width = probe.shape[0]
    nd = nh * hd

    def flat(w):
        return jnp.transpose(w, (1, 2, 0)).reshape(nd, width)

    def heads(g):
        return jnp.transpose(g.reshape(nh, hd, width), (2, 0, 1))

    wq, wk, wv, wo = flat(w_query), flat(w_key), flat(w_value), w_out.reshape(nd, width)
    gu2, bu, qt, cb, wvq = run_query(nh, hd, probe, wq, b_query, wk, wv, b_value, enc_gain, enc_bias)
    wvq = lax.ppermute(wvq, 'tp', [(0, 1), (1, 0)])
    xh, sx, rs, r_raw, ml = run_fwd(encoded, gu2, bu)
    yt, ht, dpre, ot, da, pooled, do_t, gt, aux, rb = run_head(nh, hd, r_raw, ml, wv, wvq, wo, w_up, w_down, enc_gain, bu, cb, b_out, head_gain, head_bias, b_up, b_down, out_grad)
    rc = lax.ppermute(rb, 'sp', [(i, (i + 2) % 4) for i in range(4)])
    grad_encoded, z, dl, grad_w_up, grad_w_down, grad_w_out = run_bwd(xh, sx, rs, gt, gu2, aux, yt, dpre, ht, out_grad, ot, da)
    z, dqt, pm, grad_probe, rf = run_tail(nh, hd, z, dl, rb, rc, wk, wq, enc_gain, probe)
    gwk, gwq, gwv, pooled, grad_probe = run_outer(nh, hd, qt, z, dqt, pm, do_t, rf, enc_gain, enc_bias, pooled, grad_probe)
    grad_w_query, grad_w_key, grad_w_value = heads(gwq), heads(gwk), heads(gwv)
    return (pooled, grad_encoded, grad_probe, grad_w_query, grad_w_key, grad_w_value, grad_w_out.reshape(nh, hd, width), grad_w_up, grad_w_down)


def solution(mesh):
    return jax.shard_map(local_head, mesh=mesh, in_specs=IN_SPECS, out_specs=OUT_SPECS, check_vma=False)
```

```python
import functools
import jax
import jax.numpy as jnp
from jax import lax
from jax.experimental import pallas as pl
from jax.experimental.pallas import tpu as pltpu
from jax.sharding import PartitionSpec as P

NORM_EPS = 1e-6
F32 = jnp.float32
BF16 = jnp.bfloat16
IN_SPECS = (P('dp', 'sp', None), P(), P(), P(), P(None, 'tp', None), P('tp', None), P(None, 'tp', None), P(None, 'tp', None), P('tp', None), P('tp', None, None), P(), P(), P(), P(None, 'tp'), P('tp'), P('tp', None), P(), P('dp', None))
OUT_SPECS = (P('dp', None), P('dp', 'sp', None), P('dp'), P('dp', 'tp', None), P('dp', 'tp', None), P('dp', 'tp', None), P(('dp', 'tp'), None, None), P('dp', 'tp'), P(('dp', 'tp'), None))
NN = (((1,), (0,)), ((), ()))
NT = (((1,), (1,)), ((), ()))
TN = (((0,), (0,)), ((), ()))


def mm(a, b, dims=NN):
    return lax.dot_general(a, b, dims, preferred_element_type=F32)


def dot(spec, a, b):
    return jnp.einsum(spec, a, b, preferred_element_type=F32)


def row_stats(xs):
    mean = jnp.mean(xs, axis=-1, keepdims=True)
    cen = xs - mean
    return cen, lax.rsqrt(jnp.mean(cen * cen, axis=-1, keepdims=True) + NORM_EPS)


def fwd_body(nk, x_ref, gu_ref, bu_ref, xh_ref, sx_ref, rs_ref, r_ref, ml_ref):
    images, tokens, width = x_ref.shape
    nh = nk // 2
    strip = 16
    for i in range(images):
        for j in range(0, tokens, strip):
            cen, rstd = row_stats(x_ref[i, j:j + strip, :].astype(F32))
            xh_ref[i, j:j + strip, :] = (cen * rstd).astype(BF16)
            rs_ref[0, j:j + strip, i * nk:(i + 1) * nk] = jnp.broadcast_to(rstd, (strip, nk))
    parts = []
    for i in range(images):
        s2 = mm(xh_ref[i], gu_ref[...], NT)
        parts.append(s2[:, :nk] + s2[:, nk:])
    sx = jnp.concatenate(parts, axis=1)
    sx_ref[0] = sx
    s = sx + bu_ref[...]
    m = jnp.max(s, axis=0, keepdims=True)
    e = jnp.exp(s - m)
    l = jnp.sum(e, axis=0, keepdims=True)
    row = lax.broadcasted_iota(jnp.int32, (8, m.shape[1]), 0)
    ml_ref[0] = jnp.where(row == 0, m, l)
    et = jnp.transpose(e.astype(BF16))
    for i in range(images):
        r_ref[:, i, :] = mm(et[i * nk:i * nk + nh], xh_ref[i])


def run_fwd(x, gu2, bu):
    nb, tokens, width = x.shape
    nk = gu2.shape[0] // 2
    bi = 128 // nk
    ng = nb // bi
    return pl.pallas_call(
        functools.partial(fwd_body, nk),
        grid=(ng,),
        in_specs=[
            pl.BlockSpec((bi, tokens, width), lambda i: (i, 0, 0)),
            pl.BlockSpec(gu2.shape, lambda i: (0, 0)),
            pl.BlockSpec(bu.shape, lambda i: (0, 0)),
        ],
        out_specs=[
            pl.BlockSpec((bi, tokens, width), lambda i: (i, 0, 0)),
            pl.BlockSpec((1, tokens, 128), lambda i: (i, 0, 0)),
            pl.BlockSpec((1, tokens, 128), lambda i: (i, 0, 0)),
            pl.BlockSpec((nk // 2, bi, width), lambda i: (0, i, 0)),
            pl.BlockSpec((1, 8, 128), lambda i: (i, 0, 0)),
        ],
        out_shape=[
            jax.ShapeDtypeStruct((nb, tokens, width), BF16),
            jax.ShapeDtypeStruct((ng, tokens, 128), F32),
            jax.ShapeDtypeStruct((ng, tokens, 128), F32),
            jax.ShapeDtypeStruct((nk // 2, nb, width), F32),
            jax.ShapeDtypeStruct((ng, 8, 128), F32),
        ],
        cost_estimate=pl.CostEstimate(flops=8_000_000_000, bytes_accessed=40_000_000, transcendentals=0),
        name='fwd_tokens',
    )(x, gu2, bu)


def bwd_body(nk, xh_ref, sx_ref, rs_ref, gt_ref, gu_ref, aux_ref, yt_ref, dpre_ref, ht_ref, og_ref, ot_ref, da_ref, dx_ref, z_ref, dl_ref, gup_ref, gdn_ref, gwo_ref, zacc_ref):
    step = pl.program_id(0)
    images, tokens, width = xh_ref.shape
    nh = nk // 2

    @pl.when(step == 0)
    def _():
        zacc_ref[...] = jnp.zeros_like(zacc_ref)

    gup_ref[...] = mm(yt_ref[...], dpre_ref[...])
    gdn_ref[...] = mm(ht_ref[...], og_ref[...])
    gwo_ref[...] = mm(ot_ref[...], da_ref[...])
    sx = sx_ref[0]
    rstd = rs_ref[0]
    gts = [gt_ref[:, i, :].astype(BF16) for i in range(images)]
    dpx = jnp.concatenate([mm(xh_ref[i], gts[i], NT) for i in range(images)], axis=1)
    p = jnp.exp(sx - aux_ref[0, 0:1]) * aux_ref[0, 1:2]
    ds = p * (dpx + aux_ref[0, 2:3])
    dl_ref[0] = jnp.broadcast_to(jnp.sum(ds, axis=0, keepdims=True), dl_ref.shape[1:])
    prod = (ds * sx + p * dpx) * rstd * (1.0 / width)
    ph = prod.astype(BF16)
    po = (prod - ph.astype(F32)).astype(BF16)
    g0 = lax.broadcasted_iota(jnp.int32, (128, 128), 0) // nk
    g1 = lax.broadcasted_iota(jnp.int32, (128, 128), 1) // nk
    ind = jnp.where(g0 == g1, 1.0, 0.0).astype(BF16)
    c2 = mm(ph, ind) + mm(po, ind)
    dst = jnp.transpose(ds.astype(BF16))
    ca = (ds * rstd).astype(BF16)
    cb = (p * rstd).astype(BF16)
    z = zacc_ref[...]
    for i in range(images):
        xh = xh_ref[i]
        z = z + mm(dst[i * nk:i * nk + nh], xh)
        coef = jnp.concatenate([ca[:, i * nk:(i + 1) * nk], cb[:, i * nk:(i + 1) * nk]], axis=1)
        dxh = mm(coef, jnp.concatenate([gu_ref[...], gts[i]], axis=0))
        dx_ref[i] = (dxh - c2[:, i * nk:i * nk + 1] * xh.astype(F32)).astype(BF16)
    zacc_ref[...] = z
    z_ref[...] = z


def run_bwd(xh, sx, rs, gt, gu2, aux, yt, dpre, ht, out_grad, ot, da):
    nb, tokens, width = xh.shape
    nk = gu2.shape[0] // 2
    bi = 128 // nk
    ng = nb // bi
    ff, nd = ht.shape[0], ot.shape[0]
    return pl.pallas_call(
        functools.partial(bwd_body, nk),
        grid=(ng,),
        in_specs=[
            pl.BlockSpec((bi, tokens, width), lambda i: (i, 0, 0)),
            pl.BlockSpec((1, tokens, 128), lambda i: (i, 0, 0)),
            pl.BlockSpec((1, tokens, 128), lambda i: (i, 0, 0)),
            pl.BlockSpec((nk, bi, width), lambda i: (0, i, 0)),
            pl.BlockSpec((nk, width), lambda i: (0, 0)),
            pl.BlockSpec((1, 8, 128), lambda i: (i, 0, 0)),
            pl.BlockSpec((width // ng, nb), lambda i: (i, 0)),
            pl.BlockSpec((nb, ff), lambda i: (0, 0)),
            pl.BlockSpec((ff // ng, nb), lambda i: (i, 0)),
            pl.BlockSpec((nb, width), lambda i: (0, 0)),
            pl.BlockSpec((nd // ng, nb), lambda i: (i, 0)),
            pl.BlockSpec((nb, width), lambda i: (0, 0)),
        ],
        out_specs=[
            pl.BlockSpec((bi, tokens, width), lambda i: (i, 0, 0)),
            pl.BlockSpec((nk // 2, width), lambda i: (0, 0)),
            pl.BlockSpec((1, 8, 128), lambda i: (i, 0, 0)),
            pl.BlockSpec((width // ng, ff), lambda i: (i, 0)),
            pl.BlockSpec((ff // ng, width), lambda i: (i, 0)),
            pl.BlockSpec((nd // ng, width), lambda i: (i, 0)),
        ],
        out_shape=[
            jax.ShapeDtypeStruct((nb, tokens, width), BF16),
            jax.ShapeDtypeStruct((nk // 2, width), F32),
            jax.ShapeDtypeStruct((ng, 8, 128), F32),
            jax.ShapeDtypeStruct((width, ff), F32),
            jax.ShapeDtypeStruct((ff, width), F32),
            jax.ShapeDtypeStruct((nd, width), F32),
        ],
        scratch_shapes=[pltpu.VMEM((nk // 2, width), F32)],
        cost_estimate=pl.CostEstimate(flops=12_000_000_000, bytes_accessed=40_000_000, transcendentals=0),
        name='bwd_tokens',
    )(xh, sx, rs, gt, gu2, aux, yt, dpre, ht, out_grad, ot, da)


MESH = pl.DeviceIdType.MESH
VM = pl.BlockSpec(memory_space=pltpu.VMEM)
ANY = pl.BlockSpec(memory_space=pl.ANY)


def send(src, dst, sems, k, where):
    copy = pltpu.make_async_remote_copy(src_ref=src, dst_ref=dst, send_sem=sems.at[0, k], recv_sem=sems.at[1, k], device_id=where, device_id_type=MESH)
    copy.start()
    return copy


def greet(places):
    barrier = pltpu.get_barrier_semaphore()
    for where in places:
        pl.semaphore_signal(barrier, inc=1, device_id=where, device_id_type=MESH)
    pl.semaphore_wait(barrier, len(places))


def places():
    tp = lax.axis_index('tp')
    sp = lax.axis_index('sp')
    core = lax.rem(sp, 2)
    return {'tp': 1 - tp}, {'sp': sp + 1 - 2 * core}, {'sp': lax.rem(sp + 2, 4)}, core


def two(a):
    hi = a.astype(BF16)
    return hi, (a - hi.astype(F32)).astype(BF16)


def three(a):
    hi, rest = a.astype(BF16), a
    rest = rest - hi.astype(F32)
    mid = rest.astype(BF16)
    return hi, mid, (rest - mid.astype(F32)).astype(BF16)


def head_mask(rows, nh, hd):
    lane = lax.broadcasted_iota(jnp.int32, (rows, nh * hd), 1)
    row = lax.broadcasted_iota(jnp.int32, (rows, nh * hd), 0)
    return jnp.logical_and(lane >= row * hd, lane < (row + 1) * hd)


def unpack(packed, nk):
    groups, lanes = packed.shape
    per = lanes // nk
    rows = jnp.concatenate([jnp.broadcast_to(packed[g:g + 1], (per, lanes)) for g in range(groups)], axis=0)
    keep = own_lanes(rows.shape, nk, per)
    rows = jnp.where(keep, rows, 0.0)
    shift = nk
    while shift < lanes:
        rows = rows + pltpu.roll(rows, shift, 1)
        shift *= 2
    return rows


def own_lanes(shape, nk, per):
    lane = lax.broadcasted_iota(jnp.int32, shape, 1)
    row = lax.rem(lax.broadcasted_iota(jnp.int32, shape, 0), per)
    return jnp.logical_and(lane >= row * nk, lane < (row + 1) * nk)


def pack(rows, nk):
    images, lanes = rows.shape
    per = lanes // nk
    shift = nk
    while shift < lanes:
        rows = rows + pltpu.roll(rows, shift, 1)
        shift *= 2
    rows = jnp.where(own_lanes(rows.shape, nk, per), rows, 0.0)
    return jnp.concatenate([jnp.sum(rows[g * per:(g + 1) * per], axis=0, keepdims=True) for g in range(images // per)], axis=0)


def row_of(ref):
    return ref[...].reshape(1, ref.shape[0])


def flat_heads(ref):
    return jnp.concatenate([ref[h:h + 1, :] for h in range(ref.shape[0])], axis=1)


def query_body(nh, hd, probe_ref, wq_ref, bq_ref, wk_hbm, wv_hbm, bv_ref, gain_ref, bias_ref, gu_ref, bu_ref, q_ref, cb_ref, wvq_ref, us_ref, ur_ref, wk_ref, wv_ref, lsem, sems):
    tp_peer, _, _, _ = places()
    load_k = pltpu.make_async_copy(wk_hbm, wk_ref, lsem.at[0])
    load_v = pltpu.make_async_copy(wv_hbm, wv_ref, lsem.at[1])
    load_k.start()
    load_v.start()
    greet([tp_peer])
    width = probe_ref.shape[0]
    nk = 2 * nh
    q = (mm(jnp.broadcast_to(row_of(probe_ref), (8, width)).astype(BF16), wq_ref[...], NT)[:1] + flat_heads(bq_ref)).astype(BF16)
    qd = jnp.where(head_mask(nh, nh, hd), jnp.broadcast_to(q.astype(F32), (nh, nh * hd)), 0.0).astype(BF16)
    qf = qd.astype(F32)
    q_ref[...] = jnp.transpose(jnp.concatenate([qf, qf, qf, jnp.zeros_like(qf)], axis=0)).astype(BF16)
    load_k.wait()
    u = mm(qd, wk_ref[...])
    us_ref[...] = u
    copy = send(us_ref, ur_ref, sems, 0, tp_peer)
    load_v.wait()
    bias = row_of(bias_ref)
    bh, bl = two(bias)
    row = lax.broadcasted_iota(jnp.int32, (8, width), 0)
    b2 = jnp.where(row == 0, bh.astype(F32), jnp.where(row == 1, bl.astype(F32), 0.0)).astype(BF16)
    cb_ref[...] = jnp.sum(mm(b2, wv_ref[...], NT), axis=0, keepdims=True) + flat_heads(bv_ref)
    quarter = wvq_ref.shape[0]
    wvq_ref[...] = wv_ref[pl.ds(pl.multiple_of(lax.axis_index('sp') * quarter, quarter), quarter), :].astype(F32)
    copy.wait()
    scale = hd ** -0.5
    ua = jnp.concatenate([u, ur_ref[...]], axis=0) * scale
    gu = ua * row_of(gain_ref)
    gu = gu - jnp.mean(gu, axis=1, keepdims=True)
    gh, gl = two(gu)
    gu_ref[:nk] = gh
    gu_ref[nk:] = gl
    bu = jnp.broadcast_to(jnp.sum(ua * bias, axis=1, keepdims=True), (nk, 128))
    bu_ref[...] = jnp.transpose(jnp.concatenate([bu] * (128 // nk), axis=0))[:1]


def run_query(nh, hd, probe, wq, bq, wk, wv, bv, gain, bias):
    width = probe.shape[0]
    return pl.pallas_call(
        functools.partial(query_body, nh, hd),
        in_specs=[VM] * 3 + [ANY] * 2 + [VM] * 3,
        out_specs=[VM] * 5,
        out_shape=[
            jax.ShapeDtypeStruct((4 * nh, width), BF16),
            jax.ShapeDtypeStruct((1, 128), F32),
            jax.ShapeDtypeStruct((nh * hd, 4 * nh), BF16),
            jax.ShapeDtypeStruct((1, nh * hd), F32),
            jax.ShapeDtypeStruct((nh * hd // 4, width), F32),
        ],
        scratch_shapes=[pltpu.VMEM((nh, width), F32), pltpu.VMEM((nh, width), F32), pltpu.VMEM(wk.shape, BF16), pltpu.VMEM(wv.shape, BF16), pltpu.SemaphoreType.DMA((2,)), pltpu.SemaphoreType.DMA((2, 1))],
        compiler_params=pltpu.CompilerParams(collective_id=0, has_side_effects=True),
        cost_estimate=pl.CostEstimate(flops=50_000_000, bytes_accessed=6_000_000, transcendentals=0),
        name='query_fold',
    )(probe, wq, bq, wk, wv, bv, gain, bias)


def swap_halves(src, buf, sems, k, tp_peer, core):
    half = src.shape[0] // 2
    rows = pl.ds(pl.multiple_of(core * half, half), half)
    return send(src.at[rows], buf.at[rows], sems, k, tp_peer)


def pass_on(buf, sems, k, sib, core):
    half = buf.shape[0] // 2
    rows = pl.ds(pl.multiple_of(core * half, half), half)
    return send(buf.at[rows], buf.at[rows], sems, k, sib)


def head_body(nh, hd, r_ref, ml_ref, wv_ref, wvh_ref, wo_hbm, wup_hbm, wdn_hbm, gain_ref, bu_ref, cb_ref, bo_ref, hg_ref, hb_ref, bup_ref, bdn_ref, og_ref,
              yt_out, gt_t_out, dpre_out, ot_out, da_out, pooled_out, dot_out, gt_out, aux_out, rf1_out, rb2_out,
              wo_ref, rb1, rc1, wup, wdn, wall, osd, mls, ora, mra, osd2, mls2, orb, mrb, aps, apr, rs, ra, dys, dyr, mps, mpr, dos, dor, kps, kpr, dg_s, lsem, sems):
    tp_peer, sib, xp, core = places()
    sp = lax.axis_index('sp')
    nk = 2 * nh
    nb = og_ref.shape[0]
    width = og_ref.shape[1]
    load_up = pltpu.make_async_copy(wup_hbm, wup, lsem.at[0])
    load_dn = pltpu.make_async_copy(wdn_hbm, wdn, lsem.at[1])
    load_o = pltpu.make_async_copy(wo_hbm, wo_ref, lsem.at[2])
    load_dn.start()
    load_o.start()
    load_up.start()
    gain = row_of(gain_ref)
    groups = ml_ref.shape[0]
    for h in range(nh):
        rh = (r_ref[h] * gain).astype(BF16)
        osd[:, h * hd:(h + 1) * hd] = mm(rh, wv_ref[h * hd:(h + 1) * hd, :], NT)
    m0 = jnp.concatenate([ml_ref[g, 0:1] for g in range(groups)], axis=0)
    l0 = jnp.concatenate([ml_ref[g, 1:2] for g in range(groups)], axis=0)
    mls[:groups] = m0
    mls[groups:] = l0
    greet([tp_peer, sib, xp])
    c1 = send(osd, ora, sems, 1, sib)
    c2 = send(mls, mra, sems, 2, sib)
    wall[sp] = wvh_ref[...]
    w1 = send(wvh_ref, wall.at[sp], sems, 0, sib)
    onehot = jnp.where(head_mask(128, nh, hd), 1.0, 0.0).astype(BF16)

    def spread(rows):
        return sum(mm(part, onehot) for part in three(rows))

    def join(oa, ma, la, ob, mb, lb):
        mn = jnp.maximum(ma, mb)
        fa, fb = jnp.exp(ma - mn), jnp.exp(mb - mn)
        o = oa * spread(unpack(fa, nk)) + ob * spread(unpack(fb, nk))
        return o, mn, fa * la + fb * lb

    c1.wait()
    c2.wait()
    o1, m1, l1 = join(osd[...], m0, l0, ora[...], mra[:groups], mra[groups:])
    osd2[...] = o1
    mls2[:groups] = m1
    mls2[groups:] = l1
    c3 = send(osd2, orb, sems, 3, xp)
    c4 = send(mls2, mrb, sems, 4, xp)
    w2 = send(wvh_ref, wall.at[sp], sems, 8, xp)
    load_dn.wait()
    dg_s[...] = mm(og_ref[...], wdn[...], NT)
    c3.wait()
    c4.wait()
    o, m, l = join(o1, m1, l1, orb[...], mrb[:groups], mrb[groups:])
    inv_l = 1.0 / l
    o = o * spread(unpack(inv_l, nk)) + cb_ref[...]
    o_bf = o.astype(BF16)
    load_o.wait()
    ap = mm(o_bf, wo_ref[...])
    aps[...] = ap
    c5 = swap_halves(aps, apr, sems, 5, tp_peer, core)
    wr = unpack(jnp.exp(m0 - m) * inv_l, nk)
    for h in range(nh):
        rs[h] = r_ref[h] * wr[:, h:h + 1]
    nq = nh // 2
    mine = pl.ds(core * nq, nq)
    theirs = pl.ds((1 - core) * nq, nq)
    r1 = send(rs.at[theirs], ra, sems, 6, sib)
    c5.wait()
    c6 = pass_on(apr, sems, 7, sib, core)
    r1.wait()
    rb = rs[mine] + ra[...]
    rb1[...] = rb[:1]
    rb2_out[...] = rb[1:]
    r2 = send(rb1, rc1, sems, 17, xp)
    c6.wait()
    a = ap + apr[...] + row_of(bo_ref)
    acen, arstd = row_stats(a)
    ahat = acen * arstd
    hgain = row_of(hg_ref)
    y = (ahat * hgain + row_of(hb_ref)).astype(BF16)
    load_up.wait()
    pre = mm(y, wup[...]) + row_of(bup_ref)
    k0 = 0.7978845608028654
    k1 = 0.044715
    sq = pre * pre
    th = jnp.tanh(k0 * (pre + k1 * (pre * sq)))
    half = 0.5 * (1.0 + th)
    g = (pre * half).astype(BF16)
    dgelu = half + 0.5 * pre * (1.0 - th * th) * (k0 * (1.0 + 3.0 * k1 * sq))
    dpre = (dg_s[...] * dgelu).astype(BF16)
    dpre_out[...] = dpre
    dyp = mm(dpre, wup[...], NT)
    dys[...] = dyp
    c7 = swap_halves(dys, dyr, sems, 9, tp_peer, core)
    mp = mm(g, wdn[...])
    mps[...] = mp
    c8 = swap_halves(mps, mpr, sems, 10, tp_peer, core)
    yt_out[...] = jnp.transpose(y)
    gt_t_out[...] = jnp.transpose(g)
    ot_out[...] = jnp.transpose(o_bf)
    c7.wait()
    c9 = pass_on(dyr, sems, 11, sib, core)
    c9.wait()
    dah = (dyp + dyr[...]) * hgain
    da = arstd * (dah - jnp.mean(dah, axis=1, keepdims=True) - ahat * jnp.mean(dah * ahat, axis=1, keepdims=True))
    da = (og_ref[...].astype(F32) + da).astype(BF16)
    da_out[...] = da
    do_bf = mm(da, wo_ref[...], NT).astype(BF16)
    do = do_bf.astype(F32)
    dos[...] = do
    kap = sum(mm(part, onehot, NT) for part in two(do * (cb_ref[...] - o)))
    kps[...] = kap
    c10 = swap_halves(dos, dor, sems, 12, tp_peer, core)
    c11 = send(kps, kpr, sems, 13, tp_peer)

    def back(k, h, d, w):
        t = mm(d, w) * gain
        t = t - jnp.mean(t, axis=1, keepdims=True)
        gt_out[k * nh + h] = t

    dot_out[...] = jnp.transpose(do_bf)
    for h in range(nh):
        back(0, h, do_bf[:, h * hd:(h + 1) * hd], wv_ref[h * hd:(h + 1) * hd, :])
    c10.wait()
    c12 = pass_on(dor, sems, 14, sib, core)
    w1.wait()
    w2.wait()
    from_x = lax.rem(sp + 2, 4)
    w3 = send(wall.at[from_x], wall.at[from_x], sems, 16, sib)
    c8.wait()
    c13 = pass_on(mpr, sems, 15, sib, core)
    c11.wait()
    kall = kap + pltpu.roll(kpr[...], nh, 1)
    kpk = pack(kall, nk)
    mb = m - bu_ref[...]
    for g_ in range(groups):
        aux_out[g_, 0:1] = mb[g_:g_ + 1]
        aux_out[g_, 1:2] = inv_l[g_:g_ + 1]
        aux_out[g_, 2:3] = kpk[g_:g_ + 1]
    c12.wait()
    dob = dor[...].astype(BF16)
    w3.wait()
    for h in range(nh):
        lo = (h % 2) * hd
        back(1, h, dob[:, h * hd:(h + 1) * hd], wall[h // 2, lo:lo + hd, :].astype(BF16))
    c13.wait()
    pooled_out[...] = (a + mp + mpr[...] + row_of(bdn_ref)).astype(BF16)
    r2.wait()
    rf1_out[...] = rb1[...] + rc1[...]


def run_head(nh, hd, r_raw, ml, wv, wvh, wo, w_up, w_down, gain, bu, cb, b_out, hgain, hbias, b_up, b_down, out_grad):
    nb, width = out_grad.shape
    ff = w_up.shape[1]
    nd = nh * hd
    groups = ml.shape[0]
    full = pltpu.VMEM((nb, width), F32)
    heads = pltpu.VMEM((nb, nd), F32)
    stat = pltpu.VMEM((2 * groups, 128), F32)
    rhalf = pltpu.VMEM((nh // 2, nb, width), F32)
    return pl.pallas_call(
        functools.partial(head_body, nh, hd),
        in_specs=[VM] * 4 + [ANY] * 3 + [VM] * 9,
        out_specs=[VM] * 11,
        out_shape=[
            jax.ShapeDtypeStruct((width, nb), BF16),
            jax.ShapeDtypeStruct((ff, nb), BF16),
            jax.ShapeDtypeStruct((nb, ff), BF16),
            jax.ShapeDtypeStruct((nd, nb), BF16),
            jax.ShapeDtypeStruct((nb, width), BF16),
            jax.ShapeDtypeStruct((nb, width), BF16),
            jax.ShapeDtypeStruct((nd, nb), BF16),
            jax.ShapeDtypeStruct((2 * nh, nb, width), F32),
            jax.ShapeDtypeStruct((groups, 8, 128), F32),
            jax.ShapeDtypeStruct((1, nb, width), F32),
            jax.ShapeDtypeStruct((nh // 2 - 1, nb, width), F32),
        ],
        scratch_shapes=[
            pltpu.VMEM(wo.shape, BF16), pltpu.VMEM((1, nb, width), F32), pltpu.VMEM((1, nb, width), F32), pltpu.VMEM(w_up.shape, BF16), pltpu.VMEM(w_down.shape, BF16), pltpu.VMEM((4,) + wvh.shape, F32),
            heads, stat, heads, stat, heads, stat, heads, stat,
            full, full, pltpu.VMEM((nh, nb, width), F32), rhalf,
            full, full, full, full, heads, heads, pltpu.VMEM((nb, 128), F32), pltpu.VMEM((nb, 128), F32),
            pltpu.VMEM((nb, ff), F32),
            pltpu.SemaphoreType.DMA((3,)), pltpu.SemaphoreType.DMA((2, 18)),
        ],
        compiler_params=pltpu.CompilerParams(collective_id=1, has_side_effects=True, vmem_limit_bytes=60 * 1024 * 1024),
        cost_estimate=pl.CostEstimate(flops=3_000_000_000, bytes_accessed=30_000_000, transcendentals=0),
        name='pool_head',
    )(r_raw, ml, wv, wvh, wo, w_up, w_down, gain, bu, cb, b_out, hgain, hbias, b_up, b_down, out_grad)


def tail_body(nh, hd, z_ref, dl_ref, rf1_ref, rb_ref, rc_ref, wk_hbm, wq_hbm, gain_ref, probe_ref, z_out, dq_out, pm_out, gp_out, rf_out, zs, za, zs2, zb, ds, da, ds2, db, ps, pr, rd, re, wk, wq, lsem, sems):
    tp_peer, sib, xp, core = places()
    nk = 2 * nh
    groups = dl_ref.shape[0]
    width = z_ref.shape[1]
    nq = nh // 2
    mine = pl.ds(core * nq, nq)
    theirs = pl.ds((1 - core) * nq, nq)
    load_k = pltpu.make_async_copy(wk_hbm, wk, lsem.at[0])
    load_q = pltpu.make_async_copy(wq_hbm, wq, lsem.at[1])
    load_k.start()
    load_q.start()
    ds[...] = jnp.concatenate([dl_ref[g, 0:1] for g in range(groups)], axis=0)
    zs[...] = z_ref[...]
    greet([tp_peer, sib, xp])
    c1 = send(zs, za, sems, 0, sib)
    d1 = send(ds, da, sems, 1, sib)
    rd[:1] = rf1_ref[...]
    rd[1:] = rb_ref[...] + rc_ref[...]
    r1 = send(rd, re, sems, 2, sib)
    c1.wait()
    d1.wait()
    zs2[...] = zs[...] + za[...]
    ds2[...] = ds[...] + da[...]
    c2 = send(zs2, zb, sems, 3, xp)
    d2 = send(ds2, db, sems, 4, xp)
    rf_out[mine] = rd[...]
    p1, p2, p3 = three(row_of(probe_ref))
    pm_out[...] = jnp.concatenate([p1, p2, p1, p3, p2, p1, jnp.zeros((2, width), BF16)], axis=0)
    r1.wait()
    rf_out[theirs] = re[...]
    load_k.wait()
    load_q.wait()
    c2.wait()
    d2.wait()
    dl = unpack(ds2[...] + db[...], nk)
    fix = jnp.concatenate([jnp.sum(rf_out[h] * dl[:, h:h + 1], axis=0, keepdims=True) for h in range(nh)], axis=0)
    z = (zs2[...] + zb[...] - fix) * row_of(gain_ref) * (hd ** -0.5)
    dqm = mm(z.astype(BF16), wk[...], NT)
    dq = jnp.sum(jnp.where(head_mask(nh, nh, hd), dqm, 0.0), axis=0, keepdims=True)
    gp = mm(jnp.broadcast_to(dq, (8, nh * hd)).astype(BF16), wq[...])[:1]
    ps[...] = gp
    c3 = send(ps, pr, sems, 5, tp_peer)
    z_out[...] = jnp.concatenate(list(three(z)) + [jnp.zeros((nh, width), BF16)], axis=0)
    d1_, d2_, d3_ = (part.astype(F32) for part in three(dq))
    zero = jnp.zeros_like(dq)
    dq_out[...] = jnp.transpose(jnp.concatenate([d1_, d1_, d2_, d1_, d2_, d3_, zero, zero], axis=0)).astype(BF16)
    c3.wait()
    gp_out[...] = (gp + pr[...]).reshape(width)


def run_tail(nh, hd, z, dl, rf1, rb, rc, wk, wq, gain, probe):
    width = z.shape[1]
    nd = nh * hd
    zz = pltpu.VMEM((nh, width), F32)
    dd = pltpu.VMEM((dl.shape[0], 128), F32)
    pp = pltpu.VMEM((1, width), F32)
    rr = pltpu.VMEM((nh // 2,) + rb.shape[1:], F32)
    return pl.pallas_call(
        functools.partial(tail_body, nh, hd),
        in_specs=[VM] * 5 + [ANY] * 2 + [VM] * 2,
        out_specs=[VM] * 5,
        out_shape=[
            jax.ShapeDtypeStruct((4 * nh, width), BF16),
            jax.ShapeDtypeStruct((nd, 8), BF16),
            jax.ShapeDtypeStruct((8, width), BF16),
            jax.ShapeDtypeStruct((width,), F32),
            jax.ShapeDtypeStruct((nh,) + rb.shape[1:], F32),
        ],
        scratch_shapes=[zz, zz, zz, zz, dd, dd, dd, dd, pp, pp, rr, rr, pltpu.VMEM(wk.shape, BF16), pltpu.VMEM(wq.shape, BF16), pltpu.SemaphoreType.DMA((2,)), pltpu.SemaphoreType.DMA((2, 6))],
        compiler_params=pltpu.CompilerParams(collective_id=2, has_side_effects=True),
        cost_estimate=pl.CostEstimate(flops=50_000_000, bytes_accessed=6_000_000, transcendentals=0),
        name='query_back',
    )(z, dl, rf1, rb, rc, wk, wq, gain, probe)


def outer_body(hd, qt_ref, z_ref, dqt_ref, pm_ref, dot_ref, rf_ref, gain_ref, bias_ref, pooled_ref, gp_ref, gwk_ref, gwq_ref, gwv_ref, pooled_out, gp_out):
    gwk_ref[...] = mm(qt_ref[...], z_ref[...])
    gwq_ref[...] = mm(dqt_ref[...], pm_ref[...])
    gain, bias = row_of(gain_ref), row_of(bias_ref)
    for h in range(rf_ref.shape[0]):
        r = (rf_ref[h] * gain + bias).astype(BF16)
        gwv_ref[h * hd:(h + 1) * hd, :] = mm(dot_ref[h * hd:(h + 1) * hd, :], r)
    pooled_out[...] = pooled_ref[...]
    gp_out[...] = gp_ref[...]


def run_outer(nh, hd, qt, z, dqt, pm, dot, rf, gain, bias, pooled, gp):
    nb, width = pooled.shape
    per = 1
    rows = per * hd
    blk = lambda a: pl.BlockSpec((rows, a.shape[1]), lambda i: (i, 0))
    whole = lambda a: pl.BlockSpec(a.shape, lambda i: (0,) * a.ndim)
    big = jax.ShapeDtypeStruct((nh * hd, width), F32)
    return pl.pallas_call(
        functools.partial(outer_body, hd),
        grid=(nh // per,),
        in_specs=[blk(qt), whole(z), blk(dqt), whole(pm), blk(dot), pl.BlockSpec((per, nb, width), lambda i: (i, 0, 0)), whole(gain), whole(bias), whole(pooled), whole(gp)],
        out_specs=[blk(big), blk(big), blk(big), whole(pooled), whole(gp)],
        out_shape=[big, big, big, jax.ShapeDtypeStruct(pooled.shape, BF16), jax.ShapeDtypeStruct(gp.shape, F32)],
        cost_estimate=pl.CostEstimate(flops=300_000_000, bytes_accessed=14_000_000, transcendentals=0),
        name='outer_grads',
    )(qt, z, dqt, pm, dot, rf, gain, bias, pooled, gp)


def local_head(encoded, enc_gain, enc_bias, probe, w_query, b_query, w_key, w_value, b_value, w_out, b_out, head_gain, head_bias, w_up, b_up, w_down, b_down, out_grad):
    nh, hd = b_query.shape
    width = probe.shape[0]
    nd = nh * hd

    def flat(w):
        return jnp.transpose(w, (1, 2, 0)).reshape(nd, width)

    def heads(g):
        return jnp.transpose(g.reshape(nh, hd, width), (2, 0, 1))

    wq, wk, wv, wo = flat(w_query), flat(w_key), flat(w_value), w_out.reshape(nd, width)
    gu2, bu, qt, cb, wvq = run_query(nh, hd, probe, wq, b_query, wk, wv, b_value, enc_gain, enc_bias)
    wvq = lax.ppermute(wvq, 'tp', [(0, 1), (1, 0)])
    xh, sx, rs, r_raw, ml = run_fwd(encoded, gu2, bu)
    yt, ht, dpre, ot, da, pooled, do_t, gt, aux, rf1, rb = run_head(nh, hd, r_raw, ml, wv, wvq, wo, w_up, w_down, enc_gain, bu, cb, b_out, head_gain, head_bias, b_up, b_down, out_grad)
    rc = lax.ppermute(rb, 'sp', [(i, (i + 2) % 4) for i in range(4)])
    grad_encoded, z, dl, grad_w_up, grad_w_down, grad_w_out = run_bwd(xh, sx, rs, gt, gu2, aux, yt, dpre, ht, out_grad, ot, da)
    z, dqt, pm, grad_probe, rf = run_tail(nh, hd, z, dl, rf1, rb, rc, wk, wq, enc_gain, probe)
    gwk, gwq, gwv, pooled, grad_probe = run_outer(nh, hd, qt, z, dqt, pm, do_t, rf, enc_gain, enc_bias, pooled, grad_probe)
    grad_w_query, grad_w_key, grad_w_value = heads(gwq), heads(gwk), heads(gwv)
    return (pooled, grad_encoded, grad_probe, grad_w_query, grad_w_key, grad_w_value, grad_w_out.reshape(nh, hd, width), grad_w_up, grad_w_down)


def solution(mesh):
    return jax.shard_map(local_head, mesh=mesh, in_specs=IN_SPECS, out_specs=OUT_SPECS, check_vma=False)
```

```python
import functools
import jax
import jax.numpy as jnp
from jax import lax
from jax.experimental import pallas as pl
from jax.experimental.pallas import tpu as pltpu
from jax.sharding import PartitionSpec as P

NORM_EPS = 1e-6
F32 = jnp.float32
BF16 = jnp.bfloat16
IN_SPECS = (P('dp', 'sp', None), P(), P(), P(), P(None, 'tp', None), P('tp', None), P(None, 'tp', None), P(None, 'tp', None), P('tp', None), P('tp', None, None), P(), P(), P(), P(None, 'tp'), P('tp'), P('tp', None), P(), P('dp', None))
OUT_SPECS = (P('dp', None), P('dp', 'sp', None), P('dp'), P('dp', 'tp', None), P('dp', 'tp', None), P('dp', 'tp', None), P(('dp', 'tp'), None, None), P('dp', 'tp'), P(('dp', 'tp'), None))
NN = (((1,), (0,)), ((), ()))
NT = (((1,), (1,)), ((), ()))
TN = (((0,), (0,)), ((), ()))


def mm(a, b, dims=NN):
    return lax.dot_general(a, b, dims, preferred_element_type=F32)


def dot(spec, a, b):
    return jnp.einsum(spec, a, b, preferred_element_type=F32)


def row_stats(xs):
    mean = jnp.mean(xs, axis=-1, keepdims=True)
    cen = xs - mean
    return cen, lax.rsqrt(jnp.mean(cen * cen, axis=-1, keepdims=True) + NORM_EPS)


def fwd_body(nk, x_ref, gu_ref, bu_ref, xh_ref, sx_ref, rs_ref, r_ref, ml_ref):
    images, tokens, width = x_ref.shape
    nh = nk // 2
    strip = 16
    for i in range(images):
        for j in range(0, tokens, strip):
            cen, rstd = row_stats(x_ref[i, j:j + strip, :].astype(F32))
            xh_ref[i, j:j + strip, :] = (cen * rstd).astype(BF16)
            rs_ref[0, j:j + strip, i * nk:(i + 1) * nk] = jnp.broadcast_to(rstd, (strip, nk))
    parts = []
    for i in range(images):
        s2 = mm(xh_ref[i], gu_ref[...], NT)
        parts.append(s2[:, :nk] + s2[:, nk:])
    sx = jnp.concatenate(parts, axis=1)
    sx_ref[0] = sx
    s = sx + bu_ref[...]
    m = jnp.max(s, axis=0, keepdims=True)
    e = jnp.exp(s - m)
    l = jnp.sum(e, axis=0, keepdims=True)
    row = lax.broadcasted_iota(jnp.int32, (8, m.shape[1]), 0)
    ml_ref[0] = jnp.where(row == 0, m, l)
    et = jnp.transpose(e.astype(BF16))
    for i in range(images):
        r_ref[:, i, :] = mm(et[i * nk:i * nk + nh], xh_ref[i])


def run_fwd(x, gu2, bu):
    nb, tokens, width = x.shape
    nk = gu2.shape[0] // 2
    bi = 128 // nk
    ng = nb // bi
    return pl.pallas_call(
        functools.partial(fwd_body, nk),
        grid=(ng,),
        in_specs=[
            pl.BlockSpec((bi, tokens, width), lambda i: (i, 0, 0)),
            pl.BlockSpec(gu2.shape, lambda i: (0, 0)),
            pl.BlockSpec(bu.shape, lambda i: (0, 0)),
        ],
        out_specs=[
            pl.BlockSpec((bi, tokens, width), lambda i: (i, 0, 0)),
            pl.BlockSpec((1, tokens, 128), lambda i: (i, 0, 0)),
            pl.BlockSpec((1, tokens, 128), lambda i: (i, 0, 0)),
            pl.BlockSpec((nk // 2, bi, width), lambda i: (0, i, 0)),
            pl.BlockSpec((1, 8, 128), lambda i: (i, 0, 0)),
        ],
        out_shape=[
            jax.ShapeDtypeStruct((nb, tokens, width), BF16),
            jax.ShapeDtypeStruct((ng, tokens, 128), F32),
            jax.ShapeDtypeStruct((ng, tokens, 128), F32),
            jax.ShapeDtypeStruct((nk // 2, nb, width), F32),
            jax.ShapeDtypeStruct((ng, 8, 128), F32),
        ],
        cost_estimate=pl.CostEstimate(flops=8_000_000_000, bytes_accessed=40_000_000, transcendentals=0),
        name='fwd_tokens',
    )(x, gu2, bu)


def bwd_body(nk, xh_ref, sx_ref, rs_ref, gt_ref, gu_ref, aux_ref, yt_ref, dpre_ref, ht_ref, og_ref, ot_ref, da_ref, dx_ref, z_ref, dl_ref, gup_ref, gdn_ref, gwo_ref, zacc_ref):
    step = pl.program_id(0)
    images, tokens, width = xh_ref.shape
    nh = nk // 2

    @pl.when(step == 0)
    def _():
        zacc_ref[...] = jnp.zeros_like(zacc_ref)

    gup_ref[...] = mm(yt_ref[...], dpre_ref[...])
    gdn_ref[...] = mm(ht_ref[...], og_ref[...])
    gwo_ref[...] = mm(ot_ref[...], da_ref[...])
    sx = sx_ref[0]
    rstd = rs_ref[0]
    gts = [gt_ref[:, i, :] for i in range(images)]
    dpx = jnp.concatenate([mm(xh_ref[i], gts[i], NT) for i in range(images)], axis=1)
    p = jnp.exp(sx - aux_ref[0, 0:1]) * aux_ref[0, 1:2]
    ds = p * (dpx + aux_ref[0, 2:3])
    dl_ref[0] = jnp.broadcast_to(jnp.sum(ds, axis=0, keepdims=True), dl_ref.shape[1:])
    prod = (ds * sx + p * dpx) * rstd * (1.0 / width)
    ph = prod.astype(BF16)
    po = (prod - ph.astype(F32)).astype(BF16)
    g0 = lax.broadcasted_iota(jnp.int32, (128, 128), 0) // nk
    g1 = lax.broadcasted_iota(jnp.int32, (128, 128), 1) // nk
    ind = jnp.where(g0 == g1, 1.0, 0.0).astype(BF16)
    c2 = mm(ph, ind) + mm(po, ind)
    dst = jnp.transpose(ds.astype(BF16))
    ca = (ds * rstd).astype(BF16)
    cb = (p * rstd).astype(BF16)
    z = zacc_ref[...]
    for i in range(images):
        xh = xh_ref[i]
        z = z + mm(dst[i * nk:i * nk + nh], xh)
        coef = jnp.concatenate([ca[:, i * nk:(i + 1) * nk], cb[:, i * nk:(i + 1) * nk]], axis=1)
        dxh = mm(coef, jnp.concatenate([gu_ref[...], gts[i]], axis=0))
        dx_ref[i] = (dxh - c2[:, i * nk:i * nk + 1] * xh.astype(F32)).astype(BF16)
    zacc_ref[...] = z
    z_ref[...] = z


def run_bwd(xh, sx, rs, gt, gu2, aux, yt, dpre, ht, out_grad, ot, da):
    nb, tokens, width = xh.shape
    nk = gu2.shape[0] // 2
    bi = 128 // nk
    ng = nb // bi
    ff, nd = ht.shape[0], ot.shape[0]
    return pl.pallas_call(
        functools.partial(bwd_body, nk),
        grid=(ng,),
        in_specs=[
            pl.BlockSpec((bi, tokens, width), lambda i: (i, 0, 0)),
            pl.BlockSpec((1, tokens, 128), lambda i: (i, 0, 0)),
            pl.BlockSpec((1, tokens, 128), lambda i: (i, 0, 0)),
            pl.BlockSpec((nk, bi, width), lambda i: (0, i, 0)),
            pl.BlockSpec((nk, width), lambda i: (0, 0)),
            pl.BlockSpec((1, 8, 128), lambda i: (i, 0, 0)),
            pl.BlockSpec((width // ng, nb), lambda i: (i, 0)),
            pl.BlockSpec((nb, ff), lambda i: (0, 0)),
            pl.BlockSpec((ff // ng, nb), lambda i: (i, 0)),
            pl.BlockSpec((nb, width), lambda i: (0, 0)),
            pl.BlockSpec((nd // ng, nb), lambda i: (i, 0)),
            pl.BlockSpec((nb, width), lambda i: (0, 0)),
        ],
        out_specs=[
            pl.BlockSpec((bi, tokens, width), lambda i: (i, 0, 0)),
            pl.BlockSpec((nk // 2, width), lambda i: (0, 0)),
            pl.BlockSpec((1, 8, 128), lambda i: (i, 0, 0)),
            pl.BlockSpec((width // ng, ff), lambda i: (i, 0)),
            pl.BlockSpec((ff // ng, width), lambda i: (i, 0)),
            pl.BlockSpec((nd // ng, width), lambda i: (i, 0)),
        ],
        out_shape=[
            jax.ShapeDtypeStruct((nb, tokens, width), BF16),
            jax.ShapeDtypeStruct((nk // 2, width), F32),
            jax.ShapeDtypeStruct((ng, 8, 128), F32),
            jax.ShapeDtypeStruct((width, ff), F32),
            jax.ShapeDtypeStruct((ff, width), F32),
            jax.ShapeDtypeStruct((nd, width), F32),
        ],
        scratch_shapes=[pltpu.VMEM((nk // 2, width), F32)],
        cost_estimate=pl.CostEstimate(flops=12_000_000_000, bytes_accessed=40_000_000, transcendentals=0),
        name='bwd_tokens',
    )(xh, sx, rs, gt, gu2, aux, yt, dpre, ht, out_grad, ot, da)


MESH = pl.DeviceIdType.MESH
VM = pl.BlockSpec(memory_space=pltpu.VMEM)
ANY = pl.BlockSpec(memory_space=pl.ANY)


def send(src, dst, sems, k, where):
    copy = pltpu.make_async_remote_copy(src_ref=src, dst_ref=dst, send_sem=sems.at[0, k], recv_sem=sems.at[1, k], device_id=where, device_id_type=MESH)
    copy.start()
    return copy


def greet(places):
    barrier = pltpu.get_barrier_semaphore()
    for where in places:
        pl.semaphore_signal(barrier, inc=1, device_id=where, device_id_type=MESH)
    pl.semaphore_wait(barrier, len(places))


def places():
    tp = lax.axis_index('tp')
    sp = lax.axis_index('sp')
    core = lax.rem(sp, 2)
    return {'tp': 1 - tp}, {'sp': sp + 1 - 2 * core}, {'sp': lax.rem(sp + 2, 4)}, core


def two(a):
    hi = a.astype(BF16)
    return hi, (a - hi.astype(F32)).astype(BF16)


def three(a):
    hi, rest = a.astype(BF16), a
    rest = rest - hi.astype(F32)
    mid = rest.astype(BF16)
    return hi, mid, (rest - mid.astype(F32)).astype(BF16)


def head_mask(rows, nh, hd):
    lane = lax.broadcasted_iota(jnp.int32, (rows, nh * hd), 1)
    row = lax.broadcasted_iota(jnp.int32, (rows, nh * hd), 0)
    return jnp.logical_and(lane >= row * hd, lane < (row + 1) * hd)


def unpack(packed, nk):
    groups, lanes = packed.shape
    per = lanes // nk
    rows = jnp.concatenate([jnp.broadcast_to(packed[g:g + 1], (per, lanes)) for g in range(groups)], axis=0)
    keep = own_lanes(rows.shape, nk, per)
    rows = jnp.where(keep, rows, 0.0)
    shift = nk
    while shift < lanes:
        rows = rows + pltpu.roll(rows, shift, 1)
        shift *= 2
    return rows


def own_lanes(shape, nk, per):
    lane = lax.broadcasted_iota(jnp.int32, shape, 1)
    row = lax.rem(lax.broadcasted_iota(jnp.int32, shape, 0), per)
    return jnp.logical_and(lane >= row * nk, lane < (row + 1) * nk)


def pack(rows, nk):
    images, lanes = rows.shape
    per = lanes // nk
    shift = nk
    while shift < lanes:
        rows = rows + pltpu.roll(rows, shift, 1)
        shift *= 2
    rows = jnp.where(own_lanes(rows.shape, nk, per), rows, 0.0)
    return jnp.concatenate([jnp.sum(rows[g * per:(g + 1) * per], axis=0, keepdims=True) for g in range(images // per)], axis=0)


def row_of(ref):
    return ref[...].reshape(1, ref.shape[0])


def flat_heads(ref):
    return jnp.concatenate([ref[h:h + 1, :] for h in range(ref.shape[0])], axis=1)


def query_body(nh, hd, probe_ref, wq_ref, bq_ref, wk_hbm, wv_hbm, bv_ref, gain_ref, bias_ref, gu_ref, bu_ref, q_ref, cb_ref, wvq_ref, us_ref, ur_ref, wk_ref, wv_ref, lsem, sems):
    tp_peer, _, _, _ = places()
    load_k = pltpu.make_async_copy(wk_hbm, wk_ref, lsem.at[0])
    load_v = pltpu.make_async_copy(wv_hbm, wv_ref, lsem.at[1])
    load_k.start()
    load_v.start()
    greet([tp_peer])
    width = probe_ref.shape[0]
    nk = 2 * nh
    q = (mm(jnp.broadcast_to(row_of(probe_ref), (8, width)).astype(BF16), wq_ref[...], NT)[:1] + flat_heads(bq_ref)).astype(BF16)
    qd = jnp.where(head_mask(nh, nh, hd), jnp.broadcast_to(q.astype(F32), (nh, nh * hd)), 0.0).astype(BF16)
    qf = qd.astype(F32)
    q_ref[...] = jnp.transpose(jnp.concatenate([qf, qf, qf, jnp.zeros_like(qf)], axis=0)).astype(BF16)
    load_k.wait()
    u = mm(qd, wk_ref[...])
    us_ref[...] = u
    copy = send(us_ref, ur_ref, sems, 0, tp_peer)
    load_v.wait()
    bias = row_of(bias_ref)
    bh, bl = two(bias)
    row = lax.broadcasted_iota(jnp.int32, (8, width), 0)
    b2 = jnp.where(row == 0, bh.astype(F32), jnp.where(row == 1, bl.astype(F32), 0.0)).astype(BF16)
    cb_ref[...] = jnp.sum(mm(b2, wv_ref[...], NT), axis=0, keepdims=True) + flat_heads(bv_ref)
    quarter = wvq_ref.shape[0]
    wvq_ref[...] = wv_ref[pl.ds(pl.multiple_of(lax.axis_index('sp') * quarter, quarter), quarter), :].astype(F32)
    copy.wait()
    scale = hd ** -0.5
    ua = jnp.concatenate([u, ur_ref[...]], axis=0) * scale
    gu = ua * row_of(gain_ref)
    gu = gu - jnp.mean(gu, axis=1, keepdims=True)
    gh, gl = two(gu)
    gu_ref[:nk] = gh
    gu_ref[nk:] = gl
    bu = jnp.broadcast_to(jnp.sum(ua * bias, axis=1, keepdims=True), (nk, 128))
    bu_ref[...] = jnp.transpose(jnp.concatenate([bu] * (128 // nk), axis=0))[:1]


def run_query(nh, hd, probe, wq, bq, wk, wv, bv, gain, bias):
    width = probe.shape[0]
    return pl.pallas_call(
        functools.partial(query_body, nh, hd),
        in_specs=[VM] * 3 + [ANY] * 2 + [VM] * 3,
        out_specs=[VM] * 5,
        out_shape=[
            jax.ShapeDtypeStruct((4 * nh, width), BF16),
            jax.ShapeDtypeStruct((1, 128), F32),
            jax.ShapeDtypeStruct((nh * hd, 4 * nh), BF16),
            jax.ShapeDtypeStruct((1, nh * hd), F32),
            jax.ShapeDtypeStruct((nh * hd // 4, width), F32),
        ],
        scratch_shapes=[pltpu.VMEM((nh, width), F32), pltpu.VMEM((nh, width), F32), pltpu.VMEM(wk.shape, BF16), pltpu.VMEM(wv.shape, BF16), pltpu.SemaphoreType.DMA((2,)), pltpu.SemaphoreType.DMA((2, 1))],
        compiler_params=pltpu.CompilerParams(collective_id=0, has_side_effects=True),
        cost_estimate=pl.CostEstimate(flops=50_000_000, bytes_accessed=6_000_000, transcendentals=0),
        name='query_fold',
    )(probe, wq, bq, wk, wv, bv, gain, bias)


def swap_halves(src, buf, sems, k, tp_peer, core):
    half = src.shape[0] // 2
    rows = pl.ds(pl.multiple_of(core * half, half), half)
    return send(src.at[rows], buf.at[rows], sems, k, tp_peer)


def pass_on(buf, sems, k, sib, core):
    half = buf.shape[0] // 2
    rows = pl.ds(pl.multiple_of(core * half, half), half)
    return send(buf.at[rows], buf.at[rows], sems, k, sib)


def head_body(nh, hd, r_ref, ml_ref, wv_ref, wvh_ref, wo_hbm, wup_hbm, wdn_hbm, gain_ref, bu_ref, cb_ref, bo_ref, hg_ref, hb_ref, bup_ref, bdn_ref, og_ref,
              yt_out, gt_t_out, dpre_out, ot_out, da_out, ab_out, mp_out, dot_out, gt_out, aux_out, rf1_out, rb2_out,
              wo_ref, rb1, rc1, wup, wdn, wall, osd, mls, ora, mra, osd2, mls2, orb, mrb, aps, apr, rs, ra, dys, dyr, dos, dor, kps, kpr, dg_s, lsem, sems):
    tp_peer, sib, xp, core = places()
    sp = lax.axis_index('sp')
    nk = 2 * nh
    nb = og_ref.shape[0]
    width = og_ref.shape[1]
    load_up = pltpu.make_async_copy(wup_hbm, wup, lsem.at[0])
    load_dn = pltpu.make_async_copy(wdn_hbm, wdn, lsem.at[1])
    load_o = pltpu.make_async_copy(wo_hbm, wo_ref, lsem.at[2])
    load_dn.start()
    load_o.start()
    load_up.start()
    gain = row_of(gain_ref)
    groups = ml_ref.shape[0]
    for h in range(nh):
        rh = (r_ref[h] * gain).astype(BF16)
        osd[:, h * hd:(h + 1) * hd] = mm(rh, wv_ref[h * hd:(h + 1) * hd, :], NT)
    m0 = jnp.concatenate([ml_ref[g, 0:1] for g in range(groups)], axis=0)
    l0 = jnp.concatenate([ml_ref[g, 1:2] for g in range(groups)], axis=0)
    mls[:groups] = m0
    mls[groups:] = l0
    greet([tp_peer, sib, xp])
    c1 = send(osd, ora, sems, 1, sib)
    c2 = send(mls, mra, sems, 2, sib)
    wall[sp] = wvh_ref[...]
    w1 = send(wvh_ref, wall.at[sp], sems, 0, sib)
    onehot = jnp.where(head_mask(128, nh, hd), 1.0, 0.0).astype(BF16)

    def spread(rows):
        return sum(mm(part, onehot) for part in three(rows))

    def join(oa, ma, la, ob, mb, lb):
        mn = jnp.maximum(ma, mb)
        fa, fb = jnp.exp(ma - mn), jnp.exp(mb - mn)
        o = oa * spread(unpack(fa, nk)) + ob * spread(unpack(fb, nk))
        return o, mn, fa * la + fb * lb

    c1.wait()
    c2.wait()
    o1, m1, l1 = join(osd[...], m0, l0, ora[...], mra[:groups], mra[groups:])
    osd2[...] = o1
    mls2[:groups] = m1
    mls2[groups:] = l1
    c3 = send(osd2, orb, sems, 3, xp)
    c4 = send(mls2, mrb, sems, 4, xp)
    w2 = send(wvh_ref, wall.at[sp], sems, 8, xp)
    load_dn.wait()
    dg_s[...] = mm(og_ref[...], wdn[...], NT)
    c3.wait()
    c4.wait()
    o, m, l = join(o1, m1, l1, orb[...], mrb[:groups], mrb[groups:])
    inv_l = 1.0 / l
    o = o * spread(unpack(inv_l, nk)) + cb_ref[...]
    o_bf = o.astype(BF16)
    load_o.wait()
    ap = mm(o_bf, wo_ref[...])
    aps[...] = ap
    c5 = swap_halves(aps, apr, sems, 5, tp_peer, core)
    wr = unpack(jnp.exp(m0 - m) * inv_l, nk)
    for h in range(nh):
        rs[h] = r_ref[h] * wr[:, h:h + 1]
    nq = nh // 2
    mine = pl.ds(core * nq, nq)
    theirs = pl.ds((1 - core) * nq, nq)
    r1 = send(rs.at[theirs], ra, sems, 6, sib)
    c5.wait()
    c6 = pass_on(apr, sems, 7, sib, core)
    r1.wait()
    rb = rs[mine] + ra[...]
    rb1[...] = rb[:1]
    rb2_out[...] = rb[1:]
    r2 = send(rb1, rc1, sems, 17, xp)
    c6.wait()
    a = ap + apr[...] + row_of(bo_ref)
    acen, arstd = row_stats(a)
    ahat = acen * arstd
    hgain = row_of(hg_ref)
    y = (ahat * hgain + row_of(hb_ref)).astype(BF16)
    load_up.wait()
    pre = mm(y, wup[...]) + row_of(bup_ref)
    k0 = 0.7978845608028654
    k1 = 0.044715
    sq = pre * pre
    th = jnp.tanh(k0 * (pre + k1 * (pre * sq)))
    half = 0.5 * (1.0 + th)
    g = (pre * half).astype(BF16)
    dgelu = half + 0.5 * pre * (1.0 - th * th) * (k0 * (1.0 + 3.0 * k1 * sq))
    dpre = (dg_s[...] * dgelu).astype(BF16)
    dpre_out[...] = dpre
    dyp = mm(dpre, wup[...], NT)
    dys[...] = dyp
    c7 = swap_halves(dys, dyr, sems, 9, tp_peer, core)
    mp_out[...] = mm(g, wdn[...])
    ab_out[...] = a + row_of(bdn_ref)
    yt_out[...] = jnp.transpose(y)
    gt_t_out[...] = jnp.transpose(g)
    ot_out[...] = jnp.transpose(o_bf)
    c7.wait()
    c9 = pass_on(dyr, sems, 11, sib, core)
    c9.wait()
    dah = (dyp + dyr[...]) * hgain
    da = arstd * (dah - jnp.mean(dah, axis=1, keepdims=True) - ahat * jnp.mean(dah * ahat, axis=1, keepdims=True))
    da = (og_ref[...].astype(F32) + da).astype(BF16)
    da_out[...] = da
    do_bf = mm(da, wo_ref[...], NT).astype(BF16)
    do = do_bf.astype(F32)
    dos[...] = do
    kap = sum(mm(part, onehot, NT) for part in two(do * (cb_ref[...] - o)))
    kps[...] = kap
    c10 = swap_halves(dos, dor, sems, 12, tp_peer, core)
    c11 = send(kps, kpr, sems, 13, tp_peer)

    def back(k, h, d, w):
        t = mm(d, w) * gain
        t = t - jnp.mean(t, axis=1, keepdims=True)
        gt_out[k * nh + h] = t.astype(BF16)

    dot_out[...] = jnp.transpose(do_bf)
    for h in range(nh):
        back(0, h, do_bf[:, h * hd:(h + 1) * hd], wv_ref[h * hd:(h + 1) * hd, :])
    c10.wait()
    c12 = pass_on(dor, sems, 14, sib, core)
    w1.wait()
    w2.wait()
    from_x = lax.rem(sp + 2, 4)
    w3 = send(wall.at[from_x], wall.at[from_x], sems, 16, sib)
    c11.wait()
    kall = kap + pltpu.roll(kpr[...], nh, 1)
    kpk = pack(kall, nk)
    mb = m - bu_ref[...]
    for g_ in range(groups):
        aux_out[g_, 0:1] = mb[g_:g_ + 1]
        aux_out[g_, 1:2] = inv_l[g_:g_ + 1]
        aux_out[g_, 2:3] = kpk[g_:g_ + 1]
    c12.wait()
    dob = dor[...].astype(BF16)
    w3.wait()
    for h in range(nh):
        lo = (h % 2) * hd
        back(1, h, dob[:, h * hd:(h + 1) * hd], wall[h // 2, lo:lo + hd, :].astype(BF16))
    r2.wait()
    rf1_out[...] = rb1[...] + rc1[...]


def run_head(nh, hd, r_raw, ml, wv, wvh, wo, w_up, w_down, gain, bu, cb, b_out, hgain, hbias, b_up, b_down, out_grad):
    nb, width = out_grad.shape
    ff = w_up.shape[1]
    nd = nh * hd
    groups = ml.shape[0]
    full = pltpu.VMEM((nb, width), F32)
    heads = pltpu.VMEM((nb, nd), F32)
    stat = pltpu.VMEM((2 * groups, 128), F32)
    rhalf = pltpu.VMEM((nh // 2, nb, width), F32)
    return pl.pallas_call(
        functools.partial(head_body, nh, hd),
        in_specs=[VM] * 4 + [ANY] * 3 + [VM] * 9,
        out_specs=[VM] * 12,
        out_shape=[
            jax.ShapeDtypeStruct((width, nb), BF16),
            jax.ShapeDtypeStruct((ff, nb), BF16),
            jax.ShapeDtypeStruct((nb, ff), BF16),
            jax.ShapeDtypeStruct((nd, nb), BF16),
            jax.ShapeDtypeStruct((nb, width), BF16),
            jax.ShapeDtypeStruct((nb, width), F32),
            jax.ShapeDtypeStruct((nb, width), F32),
            jax.ShapeDtypeStruct((nd, nb), BF16),
            jax.ShapeDtypeStruct((2 * nh, nb, width), BF16),
            jax.ShapeDtypeStruct((groups, 8, 128), F32),
            jax.ShapeDtypeStruct((1, nb, width), F32),
            jax.ShapeDtypeStruct((nh // 2 - 1, nb, width), F32),
        ],
        scratch_shapes=[
            pltpu.VMEM(wo.shape, BF16), pltpu.VMEM((1, nb, width), F32), pltpu.VMEM((1, nb, width), F32), pltpu.VMEM(w_up.shape, BF16), pltpu.VMEM(w_down.shape, BF16), pltpu.VMEM((4,) + wvh.shape, F32),
            heads, stat, heads, stat, heads, stat, heads, stat,
            full, full, pltpu.VMEM((nh, nb, width), F32), rhalf,
            full, full, heads, heads, pltpu.VMEM((nb, 128), F32), pltpu.VMEM((nb, 128), F32),
            pltpu.VMEM((nb, ff), F32),
            pltpu.SemaphoreType.DMA((3,)), pltpu.SemaphoreType.DMA((2, 18)),
        ],
        compiler_params=pltpu.CompilerParams(collective_id=1, has_side_effects=True, vmem_limit_bytes=60 * 1024 * 1024),
        cost_estimate=pl.CostEstimate(flops=3_000_000_000, bytes_accessed=30_000_000, transcendentals=0),
        name='pool_head',
    )(r_raw, ml, wv, wvh, wo, w_up, w_down, gain, bu, cb, b_out, hgain, hbias, b_up, b_down, out_grad)


def tail_body(nh, hd, z_ref, dl_ref, rf1_ref, rb_ref, rc_ref, wk_hbm, wq_hbm, gain_ref, probe_ref, z_out, dq_out, pm_out, gp_out, rf_out, zs, za, zs2, zb, ds, da, ds2, db, ps, pr, rd, re, wk, wq, lsem, sems):
    tp_peer, sib, xp, core = places()
    nk = 2 * nh
    groups = dl_ref.shape[0]
    width = z_ref.shape[1]
    nq = nh // 2
    mine = pl.ds(core * nq, nq)
    theirs = pl.ds((1 - core) * nq, nq)
    load_k = pltpu.make_async_copy(wk_hbm, wk, lsem.at[0])
    load_q = pltpu.make_async_copy(wq_hbm, wq, lsem.at[1])
    load_k.start()
    load_q.start()
    ds[...] = jnp.concatenate([dl_ref[g, 0:1] for g in range(groups)], axis=0)
    zs[...] = z_ref[...]
    greet([tp_peer, sib, xp])
    c1 = send(zs, za, sems, 0, sib)
    d1 = send(ds, da, sems, 1, sib)
    rd[:1] = rf1_ref[...]
    rd[1:] = rb_ref[...] + rc_ref[...]
    r1 = send(rd, re, sems, 2, sib)
    c1.wait()
    d1.wait()
    zs2[...] = zs[...] + za[...]
    ds2[...] = ds[...] + da[...]
    c2 = send(zs2, zb, sems, 3, xp)
    d2 = send(ds2, db, sems, 4, xp)
    rf_out[mine] = rd[...]
    p1, p2, p3 = three(row_of(probe_ref))
    pm_out[...] = jnp.concatenate([p1, p2, p1, p3, p2, p1, jnp.zeros((2, width), BF16)], axis=0)
    r1.wait()
    rf_out[theirs] = re[...]
    load_k.wait()
    load_q.wait()
    c2.wait()
    d2.wait()
    dl = unpack(ds2[...] + db[...], nk)
    fix = jnp.concatenate([jnp.sum(rf_out[h] * dl[:, h:h + 1], axis=0, keepdims=True) for h in range(nh)], axis=0)
    z = (zs2[...] + zb[...] - fix) * row_of(gain_ref) * (hd ** -0.5)
    dqm = mm(z.astype(BF16), wk[...], NT)
    dq = jnp.sum(jnp.where(head_mask(nh, nh, hd), dqm, 0.0), axis=0, keepdims=True)
    gp = mm(jnp.broadcast_to(dq, (8, nh * hd)).astype(BF16), wq[...])[:1]
    ps[...] = gp
    c3 = send(ps, pr, sems, 5, tp_peer)
    z_out[...] = jnp.concatenate(list(three(z)) + [jnp.zeros((nh, width), BF16)], axis=0)
    d1_, d2_, d3_ = (part.astype(F32) for part in three(dq))
    zero = jnp.zeros_like(dq)
    dq_out[...] = jnp.transpose(jnp.concatenate([d1_, d1_, d2_, d1_, d2_, d3_, zero, zero], axis=0)).astype(BF16)
    c3.wait()
    gp_out[...] = (gp + pr[...]).reshape(width)


def run_tail(nh, hd, z, dl, rf1, rb, rc, wk, wq, gain, probe):
    width = z.shape[1]
    nd = nh * hd
    zz = pltpu.VMEM((nh, width), F32)
    dd = pltpu.VMEM((dl.shape[0], 128), F32)
    pp = pltpu.VMEM((1, width), F32)
    rr = pltpu.VMEM((nh // 2,) + rb.shape[1:], F32)
    return pl.pallas_call(
        functools.partial(tail_body, nh, hd),
        in_specs=[VM] * 5 + [ANY] * 2 + [VM] * 2,
        out_specs=[VM] * 5,
        out_shape=[
            jax.ShapeDtypeStruct((4 * nh, width), BF16),
            jax.ShapeDtypeStruct((nd, 8), BF16),
            jax.ShapeDtypeStruct((8, width), BF16),
            jax.ShapeDtypeStruct((width,), F32),
            jax.ShapeDtypeStruct((nh,) + rb.shape[1:], F32),
        ],
        scratch_shapes=[zz, zz, zz, zz, dd, dd, dd, dd, pp, pp, rr, rr, pltpu.VMEM(wk.shape, BF16), pltpu.VMEM(wq.shape, BF16), pltpu.SemaphoreType.DMA((2,)), pltpu.SemaphoreType.DMA((2, 6))],
        compiler_params=pltpu.CompilerParams(collective_id=2, has_side_effects=True),
        cost_estimate=pl.CostEstimate(flops=50_000_000, bytes_accessed=6_000_000, transcendentals=0),
        name='query_back',
    )(z, dl, rf1, rb, rc, wk, wq, gain, probe)


def outer_body(hd, qt_ref, z_ref, dqt_ref, pm_ref, dot_ref, rf_ref, gain_ref, bias_ref, ab_ref, mp_ref, mpo_ref, gp_ref, gwk_ref, gwq_ref, gwv_ref, pooled_out, gp_out):
    gwk_ref[...] = mm(qt_ref[...], z_ref[...])
    gwq_ref[...] = mm(dqt_ref[...], pm_ref[...])
    gain, bias = row_of(gain_ref), row_of(bias_ref)
    for h in range(rf_ref.shape[0]):
        r = (rf_ref[h] * gain + bias).astype(BF16)
        gwv_ref[h * hd:(h + 1) * hd, :] = mm(dot_ref[h * hd:(h + 1) * hd, :], r)
    pooled_out[...] = (ab_ref[...] + (mp_ref[...] + mpo_ref[...])).astype(BF16)
    gp_out[...] = gp_ref[...]


def run_outer(nh, hd, qt, z, dqt, pm, dot, rf, gain, bias, ab, mp, mpo, gp):
    nb, width = ab.shape
    per = 2
    rows = per * hd
    blk = lambda a: pl.BlockSpec((rows, a.shape[1]), lambda i: (i, 0))
    whole = lambda a: pl.BlockSpec(a.shape, lambda i: (0,) * a.ndim)
    big = jax.ShapeDtypeStruct((nh * hd, width), F32)
    return pl.pallas_call(
        functools.partial(outer_body, hd),
        grid=(nh // per,),
        in_specs=[blk(qt), whole(z), blk(dqt), whole(pm), blk(dot), pl.BlockSpec((per, nb, width), lambda i: (i, 0, 0)), whole(gain), whole(bias), whole(ab), whole(mp), whole(mpo), whole(gp)],
        out_specs=[blk(big), blk(big), blk(big), whole(ab), whole(gp)],
        out_shape=[big, big, big, jax.ShapeDtypeStruct(ab.shape, BF16), jax.ShapeDtypeStruct(gp.shape, F32)],
        cost_estimate=pl.CostEstimate(flops=300_000_000, bytes_accessed=14_000_000, transcendentals=0),
        name='outer_grads',
    )(qt, z, dqt, pm, dot, rf, gain, bias, ab, mp, mpo, gp)


def local_head(encoded, enc_gain, enc_bias, probe, w_query, b_query, w_key, w_value, b_value, w_out, b_out, head_gain, head_bias, w_up, b_up, w_down, b_down, out_grad):
    nh, hd = b_query.shape
    width = probe.shape[0]
    nd = nh * hd

    def flat(w):
        return jnp.transpose(w, (1, 2, 0)).reshape(nd, width)

    def heads(g):
        return jnp.transpose(g.reshape(nh, hd, width), (2, 0, 1))

    wq, wk, wv, wo = flat(w_query), flat(w_key), flat(w_value), w_out.reshape(nd, width)
    gu2, bu, qt, cb, wvq = run_query(nh, hd, probe, wq, b_query, wk, wv, b_value, enc_gain, enc_bias)
    wvq = lax.ppermute(wvq, 'tp', [(0, 1), (1, 0)])
    xh, sx, rs, r_raw, ml = run_fwd(encoded, gu2, bu)
    yt, ht, dpre, ot, da, ab, mp, do_t, gt, aux, rf1, rb = run_head(nh, hd, r_raw, ml, wv, wvq, wo, w_up, w_down, enc_gain, bu, cb, b_out, head_gain, head_bias, b_up, b_down, out_grad)
    mpo = lax.ppermute(mp, 'tp', [(0, 1), (1, 0)])
    rc = lax.ppermute(rb, 'sp', [(i, (i + 2) % 4) for i in range(4)])
    grad_encoded, z, dl, grad_w_up, grad_w_down, grad_w_out = run_bwd(xh, sx, rs, gt, gu2, aux, yt, dpre, ht, out_grad, ot, da)
    z, dqt, pm, grad_probe, rf = run_tail(nh, hd, z, dl, rf1, rb, rc, wk, wq, enc_gain, probe)
    gwk, gwq, gwv, pooled, grad_probe = run_outer(nh, hd, qt, z, dqt, pm, do_t, rf, enc_gain, enc_bias, ab, mp, mpo, grad_probe)
    grad_w_query, grad_w_key, grad_w_value = heads(gwq), heads(gwk), heads(gwv)
    return (pooled, grad_encoded, grad_probe, grad_w_query, grad_w_key, grad_w_value, grad_w_out.reshape(nh, hd, width), grad_w_up, grad_w_down)


def solution(mesh):
    return jax.shard_map(local_head, mesh=mesh, in_specs=IN_SPECS, out_specs=OUT_SPECS, check_vma=False)
```

```python
import functools
import jax
import jax.numpy as jnp
from jax import lax
from jax.experimental import pallas as pl
from jax.experimental.pallas import tpu as pltpu
from jax.sharding import PartitionSpec as P

NORM_EPS = 1e-6
F32 = jnp.float32
BF16 = jnp.bfloat16
IN_SPECS = (P('dp', 'sp', None), P(), P(), P(), P(None, 'tp', None), P('tp', None), P(None, 'tp', None), P(None, 'tp', None), P('tp', None), P('tp', None, None), P(), P(), P(), P(None, 'tp'), P('tp'), P('tp', None), P(), P('dp', None))
OUT_SPECS = (P('dp', None), P('dp', 'sp', None), P('dp'), P('dp', 'tp', None), P('dp', 'tp', None), P('dp', 'tp', None), P(('dp', 'tp'), None, None), P('dp', 'tp'), P(('dp', 'tp'), None))
NN = (((1,), (0,)), ((), ()))
NT = (((1,), (1,)), ((), ()))
TN = (((0,), (0,)), ((), ()))


def mm(a, b, dims=NN):
    return lax.dot_general(a, b, dims, preferred_element_type=F32)


def dot(spec, a, b):
    return jnp.einsum(spec, a, b, preferred_element_type=F32)


def row_stats(xs):
    mean = jnp.mean(xs, axis=-1, keepdims=True)
    cen = xs - mean
    return cen, lax.rsqrt(jnp.mean(cen * cen, axis=-1, keepdims=True) + NORM_EPS)


def fwd_body(nk, x_ref, gu_ref, bu_ref, xh_ref, sx_ref, rs_ref, r_ref, ml_ref):
    images, tokens, width = x_ref.shape
    nh = nk // 2
    strip = 16
    for i in range(images):
        for j in range(0, tokens, strip):
            cen, rstd = row_stats(x_ref[i, j:j + strip, :].astype(F32))
            xh_ref[i, j:j + strip, :] = (cen * rstd).astype(BF16)
            rs_ref[0, j:j + strip, i * nk:(i + 1) * nk] = jnp.broadcast_to(rstd, (strip, nk))
    parts = []
    for i in range(images):
        s2 = mm(xh_ref[i], gu_ref[...], NT)
        parts.append(s2[:, :nk] + s2[:, nk:])
    sx = jnp.concatenate(parts, axis=1)
    sx_ref[0] = sx
    s = sx + bu_ref[...]
    m = jnp.max(s, axis=0, keepdims=True)
    e = jnp.exp(s - m)
    l = jnp.sum(e, axis=0, keepdims=True)
    row = lax.broadcasted_iota(jnp.int32, (8, m.shape[1]), 0)
    ml_ref[0] = jnp.where(row == 0, m, l)
    et = jnp.transpose(e.astype(BF16))
    for i in range(images):
        r_ref[:, i, :] = mm(et[i * nk:i * nk + nh], xh_ref[i])


def run_fwd(x, gu2, bu):
    nb, tokens, width = x.shape
    nk = gu2.shape[0] // 2
    bi = 128 // nk
    ng = nb // bi
    return pl.pallas_call(
        functools.partial(fwd_body, nk),
        grid=(ng,),
        in_specs=[
            pl.BlockSpec((bi, tokens, width), lambda i: (i, 0, 0)),
            pl.BlockSpec(gu2.shape, lambda i: (0, 0)),
            pl.BlockSpec(bu.shape, lambda i: (0, 0)),
        ],
        out_specs=[
            pl.BlockSpec((bi, tokens, width), lambda i: (i, 0, 0)),
            pl.BlockSpec((1, tokens, 128), lambda i: (i, 0, 0)),
            pl.BlockSpec((1, tokens, 128), lambda i: (i, 0, 0)),
            pl.BlockSpec((nk // 2, bi, width), lambda i: (0, i, 0)),
            pl.BlockSpec((1, 8, 128), lambda i: (i, 0, 0)),
        ],
        out_shape=[
            jax.ShapeDtypeStruct((nb, tokens, width), BF16),
            jax.ShapeDtypeStruct((ng, tokens, 128), F32),
            jax.ShapeDtypeStruct((ng, tokens, 128), F32),
            jax.ShapeDtypeStruct((nk // 2, nb, width), F32),
            jax.ShapeDtypeStruct((ng, 8, 128), F32),
        ],
        compiler_params=pltpu.CompilerParams(vmem_limit_bytes=67043328),
        cost_estimate=pl.CostEstimate(flops=8_000_000_000, bytes_accessed=40_000_000, transcendentals=0),
        name='fwd_tokens',
    )(x, gu2, bu)


def bwd_body(nk, xh_ref, sx_ref, rs_ref, gt_ref, gu_ref, aux_ref, yt_ref, dpre_ref, ht_ref, og_ref, ot_ref, da_ref, dx_ref, z_ref, dl_ref, gup_ref, gdn_ref, gwo_ref, zacc_ref):
    step = pl.program_id(0)
    images, tokens, width = xh_ref.shape
    nh = nk // 2

    @pl.when(step == 0)
    def _():
        zacc_ref[...] = jnp.zeros_like(zacc_ref)

    gup_ref[...] = mm(yt_ref[...], dpre_ref[...])
    gdn_ref[...] = mm(ht_ref[...], og_ref[...])
    gwo_ref[...] = mm(ot_ref[...], da_ref[...])
    sx = sx_ref[0]
    rstd = rs_ref[0]
    gts = [gt_ref[:, i, :] for i in range(images)]
    dpx = jnp.concatenate([mm(xh_ref[i], gts[i], NT) for i in range(images)], axis=1)
    p = jnp.exp(sx - aux_ref[0, 0:1]) * aux_ref[0, 1:2]
    ds = p * (dpx + aux_ref[0, 2:3])
    dl_ref[0] = jnp.broadcast_to(jnp.sum(ds, axis=0, keepdims=True), dl_ref.shape[1:])
    prod = (ds * sx + p * dpx) * rstd * (1.0 / width)
    ph = prod.astype(BF16)
    po = (prod - ph.astype(F32)).astype(BF16)
    g0 = lax.broadcasted_iota(jnp.int32, (128, 128), 0) // nk
    g1 = lax.broadcasted_iota(jnp.int32, (128, 128), 1) // nk
    ind = jnp.where(g0 == g1, 1.0, 0.0).astype(BF16)
    c2 = mm(ph, ind) + mm(po, ind)
    dst = jnp.transpose(ds.astype(BF16))
    ca = (ds * rstd).astype(BF16)
    cb = (p * rstd).astype(BF16)
    z = zacc_ref[...]
    for i in range(images):
        xh = xh_ref[i]
        z = z + mm(dst[i * nk:i * nk + nh], xh)
        coef = jnp.concatenate([ca[:, i * nk:(i + 1) * nk], cb[:, i * nk:(i + 1) * nk]], axis=1)
        dxh = mm(coef, jnp.concatenate([gu_ref[...], gts[i]], axis=0))
        dx_ref[i] = (dxh - c2[:, i * nk:i * nk + 1] * xh.astype(F32)).astype(BF16)
    zacc_ref[...] = z
    z_ref[...] = z


def run_bwd(xh, sx, rs, gt, gu2, aux, yt, dpre, ht, out_grad, ot, da):
    nb, tokens, width = xh.shape
    nk = gu2.shape[0] // 2
    bi = 128 // nk
    ng = nb // bi
    ff, nd = ht.shape[0], ot.shape[0]
    return pl.pallas_call(
        functools.partial(bwd_body, nk),
        grid=(ng,),
        in_specs=[
            pl.BlockSpec((bi, tokens, width), lambda i: (i, 0, 0)),
            pl.BlockSpec((1, tokens, 128), lambda i: (i, 0, 0)),
            pl.BlockSpec((1, tokens, 128), lambda i: (i, 0, 0)),
            pl.BlockSpec((nk, bi, width), lambda i: (0, i, 0)),
            pl.BlockSpec((nk, width), lambda i: (0, 0)),
            pl.BlockSpec((1, 8, 128), lambda i: (i, 0, 0)),
            pl.BlockSpec((width // ng, nb), lambda i: (i, 0)),
            pl.BlockSpec((nb, ff), lambda i: (0, 0)),
            pl.BlockSpec((ff // ng, nb), lambda i: (i, 0)),
            pl.BlockSpec((nb, width), lambda i: (0, 0)),
            pl.BlockSpec((nd // ng, nb), lambda i: (i, 0)),
            pl.BlockSpec((nb, width), lambda i: (0, 0)),
        ],
        out_specs=[
            pl.BlockSpec((bi, tokens, width), lambda i: (i, 0, 0)),
            pl.BlockSpec((nk // 2, width), lambda i: (0, 0)),
            pl.BlockSpec((1, 8, 128), lambda i: (i, 0, 0)),
            pl.BlockSpec((width // ng, ff), lambda i: (i, 0)),
            pl.BlockSpec((ff // ng, width), lambda i: (i, 0)),
            pl.BlockSpec((nd // ng, width), lambda i: (i, 0)),
        ],
        out_shape=[
            jax.ShapeDtypeStruct((nb, tokens, width), BF16),
            jax.ShapeDtypeStruct((nk // 2, width), F32),
            jax.ShapeDtypeStruct((ng, 8, 128), F32),
            jax.ShapeDtypeStruct((width, ff), F32),
            jax.ShapeDtypeStruct((ff, width), F32),
            jax.ShapeDtypeStruct((nd, width), F32),
        ],
        scratch_shapes=[pltpu.VMEM((nk // 2, width), F32)],
        compiler_params=pltpu.CompilerParams(vmem_limit_bytes=67043328),
        cost_estimate=pl.CostEstimate(flops=12_000_000_000, bytes_accessed=40_000_000, transcendentals=0),
        name='bwd_tokens',
    )(xh, sx, rs, gt, gu2, aux, yt, dpre, ht, out_grad, ot, da)


MESH = pl.DeviceIdType.MESH
VM = pl.BlockSpec(memory_space=pltpu.VMEM)
ANY = pl.BlockSpec(memory_space=pl.ANY)


def send(src, dst, sems, k, where):
    copy = pltpu.make_async_remote_copy(src_ref=src, dst_ref=dst, send_sem=sems.at[0, k], recv_sem=sems.at[1, k], device_id=where, device_id_type=MESH)
    copy.start()
    return copy


def greet(places):
    barrier = pltpu.get_barrier_semaphore()
    for where in places:
        pl.semaphore_signal(barrier, inc=1, device_id=where, device_id_type=MESH)
    pl.semaphore_wait(barrier, len(places))


def places():
    tp = lax.axis_index('tp')
    sp = lax.axis_index('sp')
    core = lax.rem(sp, 2)
    return {'tp': 1 - tp}, {'sp': sp + 1 - 2 * core}, {'sp': lax.rem(sp + 2, 4)}, core


def two(a):
    hi = a.astype(BF16)
    return hi, (a - hi.astype(F32)).astype(BF16)


def three(a):
    hi, rest = a.astype(BF16), a
    rest = rest - hi.astype(F32)
    mid = rest.astype(BF16)
    return hi, mid, (rest - mid.astype(F32)).astype(BF16)


def head_mask(rows, nh, hd):
    lane = lax.broadcasted_iota(jnp.int32, (rows, nh * hd), 1)
    row = lax.broadcasted_iota(jnp.int32, (rows, nh * hd), 0)
    return jnp.logical_and(lane >= row * hd, lane < (row + 1) * hd)


def unpack(packed, nk):
    groups, lanes = packed.shape
    per = lanes // nk
    rows = jnp.concatenate([jnp.broadcast_to(packed[g:g + 1], (per, lanes)) for g in range(groups)], axis=0)
    keep = own_lanes(rows.shape, nk, per)
    rows = jnp.where(keep, rows, 0.0)
    shift = nk
    while shift < lanes:
        rows = rows + pltpu.roll(rows, shift, 1)
        shift *= 2
    return rows


def own_lanes(shape, nk, per):
    lane = lax.broadcasted_iota(jnp.int32, shape, 1)
    row = lax.rem(lax.broadcasted_iota(jnp.int32, shape, 0), per)
    return jnp.logical_and(lane >= row * nk, lane < (row + 1) * nk)


def pack(rows, nk):
    images, lanes = rows.shape
    per = lanes // nk
    shift = nk
    while shift < lanes:
        rows = rows + pltpu.roll(rows, shift, 1)
        shift *= 2
    rows = jnp.where(own_lanes(rows.shape, nk, per), rows, 0.0)
    return jnp.concatenate([jnp.sum(rows[g * per:(g + 1) * per], axis=0, keepdims=True) for g in range(images // per)], axis=0)


def row_of(ref):
    return ref[...].reshape(1, ref.shape[0])


def flat_heads(ref):
    return jnp.concatenate([ref[h:h + 1, :] for h in range(ref.shape[0])], axis=1)


def query_body(nh, hd, probe_ref, wq_ref, bq_ref, wk_hbm, wv_hbm, bv_ref, gain_ref, bias_ref, gu_ref, bu_ref, q_ref, cb_ref, wvq_ref, us_ref, ur_ref, wk_ref, wv_ref, lsem, sems):
    tp_peer, _, _, _ = places()
    load_k = pltpu.make_async_copy(wk_hbm, wk_ref, lsem.at[0])
    load_v = pltpu.make_async_copy(wv_hbm, wv_ref, lsem.at[1])
    load_k.start()
    load_v.start()
    greet([tp_peer])
    width = probe_ref.shape[0]
    nk = 2 * nh
    q = (mm(jnp.broadcast_to(row_of(probe_ref), (8, width)).astype(BF16), wq_ref[...], NT)[:1] + flat_heads(bq_ref)).astype(BF16)
    qd = jnp.where(head_mask(nh, nh, hd), jnp.broadcast_to(q.astype(F32), (nh, nh * hd)), 0.0).astype(BF16)
    qf = qd.astype(F32)
    q_ref[...] = jnp.transpose(jnp.concatenate([qf, qf, qf, jnp.zeros_like(qf)], axis=0)).astype(BF16)
    load_k.wait()
    u = mm(qd, wk_ref[...])
    us_ref[...] = u
    copy = send(us_ref, ur_ref, sems, 0, tp_peer)
    load_v.wait()
    bias = row_of(bias_ref)
    bh, bl = two(bias)
    row = lax.broadcasted_iota(jnp.int32, (8, width), 0)
    b2 = jnp.where(row == 0, bh.astype(F32), jnp.where(row == 1, bl.astype(F32), 0.0)).astype(BF16)
    cb_ref[...] = jnp.sum(mm(b2, wv_ref[...], NT), axis=0, keepdims=True) + flat_heads(bv_ref)
    quarter = wvq_ref.shape[0]
    wvq_ref[...] = wv_ref[pl.ds(pl.multiple_of(lax.axis_index('sp') * quarter, quarter), quarter), :].astype(F32)
    copy.wait()
    scale = hd ** -0.5
    ua = jnp.concatenate([u, ur_ref[...]], axis=0) * scale
    gu = ua * row_of(gain_ref)
    gu = gu - jnp.mean(gu, axis=1, keepdims=True)
    gh, gl = two(gu)
    gu_ref[:nk] = gh
    gu_ref[nk:] = gl
    bu = jnp.broadcast_to(jnp.sum(ua * bias, axis=1, keepdims=True), (nk, 128))
    bu_ref[...] = jnp.transpose(jnp.concatenate([bu] * (128 // nk), axis=0))[:1]


def run_query(nh, hd, probe, wq, bq, wk, wv, bv, gain, bias):
    width = probe.shape[0]
    return pl.pallas_call(
        functools.partial(query_body, nh, hd),
        in_specs=[VM] * 3 + [ANY] * 2 + [VM] * 3,
        out_specs=[VM] * 5,
        out_shape=[
            jax.ShapeDtypeStruct((4 * nh, width), BF16),
            jax.ShapeDtypeStruct((1, 128), F32),
            jax.ShapeDtypeStruct((nh * hd, 4 * nh), BF16),
            jax.ShapeDtypeStruct((1, nh * hd), F32),
            jax.ShapeDtypeStruct((nh * hd // 4, width), F32),
        ],
        scratch_shapes=[pltpu.VMEM((nh, width), F32), pltpu.VMEM((nh, width), F32), pltpu.VMEM(wk.shape, BF16), pltpu.VMEM(wv.shape, BF16), pltpu.SemaphoreType.DMA((2,)), pltpu.SemaphoreType.DMA((2, 1))],
        compiler_params=pltpu.CompilerParams(collective_id=0, has_side_effects=True, vmem_limit_bytes=67043328),
        cost_estimate=pl.CostEstimate(flops=50_000_000, bytes_accessed=6_000_000, transcendentals=0),
        name='query_fold',
    )(probe, wq, bq, wk, wv, bv, gain, bias)


def swap_halves(src, buf, sems, k, tp_peer, core):
    half = src.shape[0] // 2
    rows = pl.ds(pl.multiple_of(core * half, half), half)
    return send(src.at[rows], buf.at[rows], sems, k, tp_peer)


def pass_on(buf, sems, k, sib, core):
    half = buf.shape[0] // 2
    rows = pl.ds(pl.multiple_of(core * half, half), half)
    return send(buf.at[rows], buf.at[rows], sems, k, sib)


def head_body(nh, hd, r_ref, ml_ref, wv_ref, wvh_ref, wo_hbm, wup_hbm, wdn_hbm, gain_ref, bu_ref, cb_ref, bo_ref, hg_ref, hb_ref, bup_ref, bdn_ref, og_ref,
              yt_out, gt_t_out, dpre_out, ot_out, da_out, ab_out, mp_out, dot_out, gt_out, aux_out, rf1_out, rb2_out,
              wo_ref, rb1, rc1, wup, wdn, wall, osd, mls, ora, mra, osd2, mls2, orb, mrb, aps, apr, rs, ra, dys, dyr, dos, dor, kps, kpr, dg_s, lsem, sems):
    tp_peer, sib, xp, core = places()
    sp = lax.axis_index('sp')
    nk = 2 * nh
    nb = og_ref.shape[0]
    width = og_ref.shape[1]
    load_up = pltpu.make_async_copy(wup_hbm, wup, lsem.at[0])
    load_dn = pltpu.make_async_copy(wdn_hbm, wdn, lsem.at[1])
    load_o = pltpu.make_async_copy(wo_hbm, wo_ref, lsem.at[2])
    load_dn.start()
    load_o.start()
    load_up.start()
    gain = row_of(gain_ref)
    groups = ml_ref.shape[0]
    for h in range(nh):
        rh = (r_ref[h] * gain).astype(BF16)
        osd[:, h * hd:(h + 1) * hd] = mm(rh, wv_ref[h * hd:(h + 1) * hd, :], NT)
    m0 = jnp.concatenate([ml_ref[g, 0:1] for g in range(groups)], axis=0)
    l0 = jnp.concatenate([ml_ref[g, 1:2] for g in range(groups)], axis=0)
    mls[:groups] = m0
    mls[groups:] = l0
    greet([tp_peer, sib, xp])
    c1 = send(osd, ora, sems, 1, sib)
    c2 = send(mls, mra, sems, 2, sib)
    wall[sp] = wvh_ref[...]
    w1 = send(wvh_ref, wall.at[sp], sems, 0, sib)
    onehot = jnp.where(head_mask(128, nh, hd), 1.0, 0.0).astype(BF16)

    def spread(rows):
        return sum(mm(part, onehot) for part in three(rows))

    def join(oa, ma, la, ob, mb, lb):
        mn = jnp.maximum(ma, mb)
        fa, fb = jnp.exp(ma - mn), jnp.exp(mb - mn)
        o = oa * spread(unpack(fa, nk)) + ob * spread(unpack(fb, nk))
        return o, mn, fa * la + fb * lb

    c1.wait()
    c2.wait()
    o1, m1, l1 = join(osd[...], m0, l0, ora[...], mra[:groups], mra[groups:])
    osd2[...] = o1
    mls2[:groups] = m1
    mls2[groups:] = l1
    c3 = send(osd2, orb, sems, 3, xp)
    c4 = send(mls2, mrb, sems, 4, xp)
    w2 = send(wvh_ref, wall.at[sp], sems, 8, xp)
    load_dn.wait()
    dg_s[...] = mm(og_ref[...], wdn[...], NT)
    c3.wait()
    c4.wait()
    o, m, l = join(o1, m1, l1, orb[...], mrb[:groups], mrb[groups:])
    inv_l = 1.0 / l
    o = o * spread(unpack(inv_l, nk)) + cb_ref[...]
    o_bf = o.astype(BF16)
    load_o.wait()
    ap = mm(o_bf, wo_ref[...])
    aps[...] = ap
    c5 = swap_halves(aps, apr, sems, 5, tp_peer, core)
    wr = unpack(jnp.exp(m0 - m) * inv_l, nk)
    for h in range(nh):
        rs[h] = r_ref[h] * wr[:, h:h + 1]
    nq = nh // 2
    mine = pl.ds(core * nq, nq)
    theirs = pl.ds((1 - core) * nq, nq)
    r1 = send(rs.at[theirs], ra, sems, 6, sib)
    c5.wait()
    c6 = pass_on(apr, sems, 7, sib, core)
    r1.wait()
    rb = rs[mine] + ra[...]
    rb1[...] = rb[:1]
    rb2_out[...] = rb[1:]
    r2 = send(rb1, rc1, sems, 17, xp)
    c6.wait()
    a = ap + apr[...] + row_of(bo_ref)
    acen, arstd = row_stats(a)
    ahat = acen * arstd
    hgain = row_of(hg_ref)
    y = (ahat * hgain + row_of(hb_ref)).astype(BF16)
    load_up.wait()
    pre = mm(y, wup[...]) + row_of(bup_ref)
    k0 = 0.7978845608028654
    k1 = 0.044715
    sq = pre * pre
    th = jnp.tanh(k0 * (pre + k1 * (pre * sq)))
    half = 0.5 * (1.0 + th)
    g = (pre * half).astype(BF16)
    dgelu = half + 0.5 * pre * (1.0 - th * th) * (k0 * (1.0 + 3.0 * k1 * sq))
    dpre = (dg_s[...] * dgelu).astype(BF16)
    dpre_out[...] = dpre
    dyp = mm(dpre, wup[...], NT)
    dys[...] = dyp
    c7 = swap_halves(dys, dyr, sems, 9, tp_peer, core)
    mp_out[...] = mm(g, wdn[...])
    ab_out[...] = a + row_of(bdn_ref)
    yt_out[...] = jnp.transpose(y)
    gt_t_out[...] = jnp.transpose(g)
    ot_out[...] = jnp.transpose(o_bf)
    c7.wait()
    c9 = pass_on(dyr, sems, 11, sib, core)
    c9.wait()
    dah = (dyp + dyr[...]) * hgain
    da = arstd * (dah - jnp.mean(dah, axis=1, keepdims=True) - ahat * jnp.mean(dah * ahat, axis=1, keepdims=True))
    da = (og_ref[...].astype(F32) + da).astype(BF16)
    da_out[...] = da
    do_bf = mm(da, wo_ref[...], NT).astype(BF16)
    do = do_bf.astype(F32)
    dos[...] = do
    kap = sum(mm(part, onehot, NT) for part in two(do * (cb_ref[...] - o)))
    kps[...] = kap
    c10 = swap_halves(dos, dor, sems, 12, tp_peer, core)
    c11 = send(kps, kpr, sems, 13, tp_peer)

    def back(k, h, d, w):
        t = mm(d, w) * gain
        t = t - jnp.mean(t, axis=1, keepdims=True)
        gt_out[k * nh + h] = t.astype(BF16)

    dot_out[...] = jnp.transpose(do_bf)
    for h in range(nh):
        back(0, h, do_bf[:, h * hd:(h + 1) * hd], wv_ref[h * hd:(h + 1) * hd, :])
    c10.wait()
    c12 = pass_on(dor, sems, 14, sib, core)
    w1.wait()
    w2.wait()
    from_x = lax.rem(sp + 2, 4)
    w3 = send(wall.at[from_x], wall.at[from_x], sems, 16, sib)
    c11.wait()
    kall = kap + pltpu.roll(kpr[...], nh, 1)
    kpk = pack(kall, nk)
    mb = m - bu_ref[...]
    for g_ in range(groups):
        aux_out[g_, 0:1] = mb[g_:g_ + 1]
        aux_out[g_, 1:2] = inv_l[g_:g_ + 1]
        aux_out[g_, 2:3] = kpk[g_:g_ + 1]
    c12.wait()
    dob = dor[...].astype(BF16)
    w3.wait()
    for h in range(nh):
        lo = (h % 2) * hd
        back(1, h, dob[:, h * hd:(h + 1) * hd], wall[h // 2, lo:lo + hd, :].astype(BF16))
    r2.wait()
    rf1_out[...] = rb1[...] + rc1[...]


def run_head(nh, hd, r_raw, ml, wv, wvh, wo, w_up, w_down, gain, bu, cb, b_out, hgain, hbias, b_up, b_down, out_grad):
    nb, width = out_grad.shape
    ff = w_up.shape[1]
    nd = nh * hd
    groups = ml.shape[0]
    full = pltpu.VMEM((nb, width), F32)
    heads = pltpu.VMEM((nb, nd), F32)
    stat = pltpu.VMEM((2 * groups, 128), F32)
    rhalf = pltpu.VMEM((nh // 2, nb, width), F32)
    return pl.pallas_call(
        functools.partial(head_body, nh, hd),
        in_specs=[VM] * 4 + [ANY] * 3 + [VM] * 9,
        out_specs=[VM] * 12,
        out_shape=[
            jax.ShapeDtypeStruct((width, nb), BF16),
            jax.ShapeDtypeStruct((ff, nb), BF16),
            jax.ShapeDtypeStruct((nb, ff), BF16),
            jax.ShapeDtypeStruct((nd, nb), BF16),
            jax.ShapeDtypeStruct((nb, width), BF16),
            jax.ShapeDtypeStruct((nb, width), F32),
            jax.ShapeDtypeStruct((nb, width), F32),
            jax.ShapeDtypeStruct((nd, nb), BF16),
            jax.ShapeDtypeStruct((2 * nh, nb, width), BF16),
            jax.ShapeDtypeStruct((groups, 8, 128), F32),
            jax.ShapeDtypeStruct((1, nb, width), F32),
            jax.ShapeDtypeStruct((nh // 2 - 1, nb, width), F32),
        ],
        scratch_shapes=[
            pltpu.VMEM(wo.shape, BF16), pltpu.VMEM((1, nb, width), F32), pltpu.VMEM((1, nb, width), F32), pltpu.VMEM(w_up.shape, BF16), pltpu.VMEM(w_down.shape, BF16), pltpu.VMEM((4,) + wvh.shape, F32),
            heads, stat, heads, stat, heads, stat, heads, stat,
            full, full, pltpu.VMEM((nh, nb, width), F32), rhalf,
            full, full, heads, heads, pltpu.VMEM((nb, 128), F32), pltpu.VMEM((nb, 128), F32),
            pltpu.VMEM((nb, ff), F32),
            pltpu.SemaphoreType.DMA((3,)), pltpu.SemaphoreType.DMA((2, 18)),
        ],
        compiler_params=pltpu.CompilerParams(collective_id=1, has_side_effects=True, vmem_limit_bytes=67043328),
        cost_estimate=pl.CostEstimate(flops=3_000_000_000, bytes_accessed=30_000_000, transcendentals=0),
        name='pool_head',
    )(r_raw, ml, wv, wvh, wo, w_up, w_down, gain, bu, cb, b_out, hgain, hbias, b_up, b_down, out_grad)


def tail_body(nh, hd, z_ref, dl_ref, rf1_ref, rb_ref, rc_ref, wk_hbm, wq_hbm, gain_ref, probe_ref, z_out, dq_out, pm_out, gp_out, rf_out, zs, za, zs2, zb, ds, da, ds2, db, ps, pr, rd, re, wk, wq, lsem, sems):
    tp_peer, sib, xp, core = places()
    nk = 2 * nh
    groups = dl_ref.shape[0]
    width = z_ref.shape[1]
    nq = nh // 2
    mine = pl.ds(core * nq, nq)
    theirs = pl.ds((1 - core) * nq, nq)
    load_k = pltpu.make_async_copy(wk_hbm, wk, lsem.at[0])
    load_q = pltpu.make_async_copy(wq_hbm, wq, lsem.at[1])
    load_k.start()
    load_q.start()
    ds[...] = jnp.concatenate([dl_ref[g, 0:1] for g in range(groups)], axis=0)
    zs[...] = z_ref[...]
    greet([tp_peer, sib, xp])
    c1 = send(zs, za, sems, 0, sib)
    d1 = send(ds, da, sems, 1, sib)
    rd[:1] = rf1_ref[...]
    rd[1:] = rb_ref[...] + rc_ref[...]
    r1 = send(rd, re, sems, 2, sib)
    c1.wait()
    d1.wait()
    zs2[...] = zs[...] + za[...]
    ds2[...] = ds[...] + da[...]
    c2 = send(zs2, zb, sems, 3, xp)
    d2 = send(ds2, db, sems, 4, xp)
    rf_out[mine] = rd[...]
    p1, p2, p3 = three(row_of(probe_ref))
    pm_out[...] = jnp.concatenate([p1, p2, p1, p3, p2, p1, jnp.zeros((2, width), BF16)], axis=0)
    r1.wait()
    rf_out[theirs] = re[...]
    load_k.wait()
    load_q.wait()
    c2.wait()
    d2.wait()
    dl = unpack(ds2[...] + db[...], nk)
    fix = jnp.concatenate([jnp.sum(rf_out[h] * dl[:, h:h + 1], axis=0, keepdims=True) for h in range(nh)], axis=0)
    z = (zs2[...] + zb[...] - fix) * row_of(gain_ref) * (hd ** -0.5)
    dqm = mm(z.astype(BF16), wk[...], NT)
    dq = jnp.sum(jnp.where(head_mask(nh, nh, hd), dqm, 0.0), axis=0, keepdims=True)
    gp = mm(jnp.broadcast_to(dq, (8, nh * hd)).astype(BF16), wq[...])[:1]
    ps[...] = gp
    c3 = send(ps, pr, sems, 5, tp_peer)
    z_out[...] = jnp.concatenate(list(three(z)) + [jnp.zeros((nh, width), BF16)], axis=0)
    d1_, d2_, d3_ = (part.astype(F32) for part in three(dq))
    zero = jnp.zeros_like(dq)
    dq_out[...] = jnp.transpose(jnp.concatenate([d1_, d1_, d2_, d1_, d2_, d3_, zero, zero], axis=0)).astype(BF16)
    c3.wait()
    gp_out[...] = (gp + pr[...]).reshape(width)


def run_tail(nh, hd, z, dl, rf1, rb, rc, wk, wq, gain, probe):
    width = z.shape[1]
    nd = nh * hd
    zz = pltpu.VMEM((nh, width), F32)
    dd = pltpu.VMEM((dl.shape[0], 128), F32)
    pp = pltpu.VMEM((1, width), F32)
    rr = pltpu.VMEM((nh // 2,) + rb.shape[1:], F32)
    return pl.pallas_call(
        functools.partial(tail_body, nh, hd),
        in_specs=[VM] * 5 + [ANY] * 2 + [VM] * 2,
        out_specs=[VM] * 5,
        out_shape=[
            jax.ShapeDtypeStruct((4 * nh, width), BF16),
            jax.ShapeDtypeStruct((nd, 8), BF16),
            jax.ShapeDtypeStruct((8, width), BF16),
            jax.ShapeDtypeStruct((width,), F32),
            jax.ShapeDtypeStruct((nh,) + rb.shape[1:], F32),
        ],
        scratch_shapes=[zz, zz, zz, zz, dd, dd, dd, dd, pp, pp, rr, rr, pltpu.VMEM(wk.shape, BF16), pltpu.VMEM(wq.shape, BF16), pltpu.SemaphoreType.DMA((2,)), pltpu.SemaphoreType.DMA((2, 6))],
        compiler_params=pltpu.CompilerParams(collective_id=2, has_side_effects=True, vmem_limit_bytes=67043328),
        cost_estimate=pl.CostEstimate(flops=50_000_000, bytes_accessed=6_000_000, transcendentals=0),
        name='query_back',
    )(z, dl, rf1, rb, rc, wk, wq, gain, probe)


def outer_body(hd, qt_ref, z_ref, dqt_ref, pm_ref, dot_ref, rf_ref, gain_ref, bias_ref, ab_ref, mp_ref, mpo_ref, gp_ref, gwk_ref, gwq_ref, gwv_ref, pooled_out, gp_out):
    gwk_ref[...] = mm(qt_ref[...], z_ref[...])
    gwq_ref[...] = mm(dqt_ref[...], pm_ref[...])
    gain, bias = row_of(gain_ref), row_of(bias_ref)
    for h in range(rf_ref.shape[0]):
        r = (rf_ref[h] * gain + bias).astype(BF16)
        gwv_ref[h * hd:(h + 1) * hd, :] = mm(dot_ref[h * hd:(h + 1) * hd, :], r)
    pooled_out[...] = (ab_ref[...] + (mp_ref[...] + mpo_ref[...])).astype(BF16)
    gp_out[...] = gp_ref[...]


def run_outer(nh, hd, qt, z, dqt, pm, dot, rf, gain, bias, ab, mp, mpo, gp):
    nb, width = ab.shape
    per = 2
    rows = per * hd
    blk = lambda a: pl.BlockSpec((rows, a.shape[1]), lambda i: (i, 0))
    whole = lambda a: pl.BlockSpec(a.shape, lambda i: (0,) * a.ndim)
    big = jax.ShapeDtypeStruct((nh * hd, width), F32)
    return pl.pallas_call(
        functools.partial(outer_body, hd),
        grid=(nh // per,),
        in_specs=[blk(qt), whole(z), blk(dqt), whole(pm), blk(dot), pl.BlockSpec((per, nb, width), lambda i: (i, 0, 0)), whole(gain), whole(bias), whole(ab), whole(mp), whole(mpo), whole(gp)],
        out_specs=[blk(big), blk(big), blk(big), whole(ab), whole(gp)],
        out_shape=[big, big, big, jax.ShapeDtypeStruct(ab.shape, BF16), jax.ShapeDtypeStruct(gp.shape, F32)],
        compiler_params=pltpu.CompilerParams(vmem_limit_bytes=67043328),
        cost_estimate=pl.CostEstimate(flops=300_000_000, bytes_accessed=14_000_000, transcendentals=0),
        name='outer_grads',
    )(qt, z, dqt, pm, dot, rf, gain, bias, ab, mp, mpo, gp)


def local_head(encoded, enc_gain, enc_bias, probe, w_query, b_query, w_key, w_value, b_value, w_out, b_out, head_gain, head_bias, w_up, b_up, w_down, b_down, out_grad):
    nh, hd = b_query.shape
    width = probe.shape[0]
    nd = nh * hd

    def flat(w):
        return jnp.transpose(w, (1, 2, 0)).reshape(nd, width)

    def heads(g):
        return jnp.transpose(g.reshape(nh, hd, width), (2, 0, 1))

    wq, wk, wv, wo = flat(w_query), flat(w_key), flat(w_value), w_out.reshape(nd, width)
    gu2, bu, qt, cb, wvq = run_query(nh, hd, probe, wq, b_query, wk, wv, b_value, enc_gain, enc_bias)
    wvq = lax.ppermute(wvq, 'tp', [(0, 1), (1, 0)])
    xh, sx, rs, r_raw, ml = run_fwd(encoded, gu2, bu)
    yt, ht, dpre, ot, da, ab, mp, do_t, gt, aux, rf1, rb = run_head(nh, hd, r_raw, ml, wv, wvq, wo, w_up, w_down, enc_gain, bu, cb, b_out, head_gain, head_bias, b_up, b_down, out_grad)
    mpo = lax.ppermute(mp, 'tp', [(0, 1), (1, 0)])
    rc = lax.ppermute(rb, 'sp', [(i, (i + 2) % 4) for i in range(4)])
    grad_encoded, z, dl, grad_w_up, grad_w_down, grad_w_out = run_bwd(xh, sx, rs, gt, gu2, aux, yt, dpre, ht, out_grad, ot, da)
    z, dqt, pm, grad_probe, rf = run_tail(nh, hd, z, dl, rf1, rb, rc, wk, wq, enc_gain, probe)
    gwk, gwq, gwv, pooled, grad_probe = run_outer(nh, hd, qt, z, dqt, pm, do_t, rf, enc_gain, enc_bias, ab, mp, mpo, grad_probe)
    grad_w_query, grad_w_key, grad_w_value = heads(gwq), heads(gwk), heads(gwv)
    return (pooled, grad_encoded, grad_probe, grad_w_query, grad_w_key, grad_w_value, grad_w_out.reshape(nh, hd, width), grad_w_up, grad_w_down)


def solution(mesh):
    return jax.shard_map(local_head, mesh=mesh, in_specs=IN_SPECS, out_specs=OUT_SPECS, check_vma=False)
```
